32 devices in a mesh: fsdp: 2 (over x), heads: 4 (over y, core), tensor: 4 (over z).
Axes of the slice: x: 2, y: 2, z: 4, core: 2. Of those that a mesh axis runs over, the one named last changes fastest.
Arguments:
- inputs: bfloat16 [16, 1024, 1024], P(('fsdp', 'tensor'), 'heads')
- slot_flag: int32 [16], P(('fsdp', 'tensor')), may hold values from 0 to 1, as said below
- cotangent: bfloat16 [16, 1024, 1024], P(('fsdp', 'tensor'), 'heads'), may hold values from -6 to 6
- first_gain: bfloat16 [1024], P(('fsdp', 'heads', 'tensor')), may hold values from 0.5 to 1.5
- first_shift: bfloat16 [1024], P(('fsdp', 'heads', 'tensor')), may hold values from -1.25 to 1.25
- query_weight: bfloat16 [1024, 1024], P(('fsdp', 'heads', 'tensor')), may hold values from -0.25 to 0.25
- query_bias: bfloat16 [1024], P(('fsdp', 'heads', 'tensor')), may hold values from -1.75 to 1.75
- key_weight: bfloat16 [1024, 1024], P(('fsdp', 'heads', 'tensor')), may hold values from -0.1875 to 0.1875
- value_weight: bfloat16 [1024, 1024], P(('fsdp', 'heads', 'tensor')), may hold values from -0.1875 to 0.1875
- value_bias: bfloat16 [1024], P(('fsdp', 'heads', 'tensor')), may hold values from -0.3125 to 0.3125
- out_weight: bfloat16 [1024, 1024], P(('fsdp', 'heads', 'tensor')), may hold values from -1.5 to 1.5
- out_bias: bfloat16 [1024], P(('fsdp', 'heads', 'tensor')), may hold values from -0.625 to 0.625
- second_gain: bfloat16 [1024], P(('fsdp', 'heads', 'tensor')), may hold values from 0.5 to 1.5
- second_shift: bfloat16 [1024], P(('fsdp', 'heads', 'tensor')), may hold values from -1.25 to 1.25
- gate_weight: bfloat16 [1024, 2736], P(('fsdp', 'heads'), 'tensor'), may hold values from -0.1875 to 0.1875
- gate_bias: bfloat16 [2736], P('tensor'), may hold values from -1.75 to 1.75
- up_weight: bfloat16 [1024, 2736], P(('fsdp', 'heads'), 'tensor'), may hold values from -0.1875 to 0.1875
- up_bias: bfloat16 [2736], P('tensor'), may hold values from -1.75 to 1.75
- inner_gain: bfloat16 [2736], P('tensor'), may hold values from 0.5 to 1.5
- inner_shift: bfloat16 [2736], P('tensor'), may hold values from -1.25 to 1.25
- down_weight: bfloat16 [2736, 1024], P('tensor', ('fsdp', 'heads')), may hold values from -0.109375 to 0.109375
- down_bias: bfloat16 [1024], P(('fsdp', 'heads', 'tensor')), may hold values from -0.625 to 0.625
Outputs:
- output: bfloat16 [16, 1024, 1024], P(('fsdp', 'tensor'), 'heads')
- input_grad: bfloat16 [16, 1024, 1024], P(('fsdp', 'tensor'), 'heads')
- first_gain_grad: float32 [1024], P(('fsdp', 'heads', 'tensor'))
- first_shift_grad: float32 [1024], P(('fsdp', 'heads', 'tensor'))
- query_weight_grad: float32 [1024, 1024], P(('fsdp', 'heads', 'tensor'))
- query_bias_grad: float32 [1024], P(('fsdp', 'heads', 'tensor'))
- key_weight_grad: float32 [1024, 1024], P(('fsdp', 'heads', 'tensor'))
- value_weight_grad: float32 [1024, 1024], P(('fsdp', 'heads', 'tensor'))
- value_bias_grad: float32 [1024], P(('fsdp', 'heads', 'tensor'))
- out_weight_grad: float32 [1024, 1024], P(('fsdp', 'heads', 'tensor'))
- out_bias_grad: float32 [1024], P(('fsdp', 'heads', 'tensor'))
- second_gain_grad: float32 [1024], P(('fsdp', 'heads', 'tensor'))
- second_shift_grad: float32 [1024], P(('fsdp', 'heads', 'tensor'))
- gate_weight_grad: float32 [1024, 2736], P(('fsdp', 'heads'), 'tensor')
- gate_bias_grad: float32 [2736], P('tensor')
- up_weight_grad: float32 [1024, 2736], P(('fsdp', 'heads'), 'tensor')
- up_bias_grad: float32 [2736], P('tensor')
- inner_gain_grad: float32 [2736], P('tensor')
- inner_shift_grad: float32 [2736], P('tensor')
- down_weight_grad: float32 [2736, 1024], P('tensor', ('fsdp', 'heads'))
- down_bias_grad: float32 [1024], P(('fsdp', 'heads', 'tensor'))
The draws below stay inside these ranges and needn't reach their ends.
Inputs may be any that keep to these rules, and one draw needn't show every extreme that they name: `slot_flag`: exactly one of the 16 image slots has flag 0; all others have flag 1.
All inputs are finite; a program needn't handle non-finite values.
Results may differ from the reference program's by a relative error of at most 0.017.
Values may be sent and summed in bfloat16 or wider, within the bound.
A program may use at most 192 MiB of HBM per device.

```python
import math
import jax
import jax.numpy as jnp
from jax import lax

D = 1024
H = 16
HD = 64
FF_REAL = 2730
FF = 2736
GRID = 32
LEN = 1024
SEQS = 16


def draw_inputs(key, part):
    key_one, key_two, key_three = jax.random.split(key, 3)
    row_scale = jnp.exp(jax.random.uniform(key_two, (SEQS, LEN, 1), jnp.float32, math.log(0.4), math.log(3.0)))
    col_scale = jnp.exp(jax.random.uniform(key_three, (1, 1, D), jnp.float32, math.log(0.7), math.log(1.4)))
    values = jax.random.normal(key_one, (SEQS, LEN, D), jnp.float32) * row_scale * col_scale
    return values.astype(jnp.bfloat16)


def draw_slot_flag(key, part):
    empty_slot = jax.random.randint(key, (), 0, SEQS)
    return (jnp.arange(SEQS, dtype=jnp.int32) != empty_slot).astype(jnp.int32)


def levels(own_key, dims, cuts, smallest, high):
    def one(axis_at, parts):
        heights = jax.random.uniform(jax.random.fold_in(jax.random.fold_in(own_key, 6), axis_at), (parts,), jnp.float32, smallest / len(cuts), high / len(cuts))
        return jnp.repeat(jnp.exp(heights), dims[axis_at] // parts).reshape((-1,) + (1,) * (len(dims) - axis_at - 1))

    gain = one(*cuts[0])
    for cut in cuts[1:]:
        gain = gain * one(*cut)
    return gain


def bell_draw(own_key, dims, spread, bound, cuts=(), held_as=jnp.bfloat16):
    values = jax.random.normal(own_key, dims, jnp.float32) * spread
    if len(cuts) > 0:
        values = levels(own_key, dims, cuts, -0.22, 0.18) * values
    return jnp.clip(values, min=-bound, max=bound).astype(held_as)


def setup_inputs(seed: int = 0) -> dict:
    arg_keys = jax.random.split(jax.random.key(seed), 23)
    return {
        "inputs": draw_inputs(jax.random.fold_in(arg_keys[22], 71), 0),
        "slot_flag": draw_slot_flag(jax.random.fold_in(arg_keys[22], 71), 0),
        "cotangent": bell_draw(arg_keys[2], (SEQS, LEN, D), 1.0, 6.0, ((0, 8), (1, 4))),
        "first_gain": jnp.clip(1.0 + 0.1 * jax.random.normal(arg_keys[3], (D,), jnp.float32), 0.5, 1.5).astype(jnp.bfloat16),
        "first_shift": bell_draw(arg_keys[4], (D,), 0.2, 1.25, ((0, 32),)),
        "query_weight": bell_draw(arg_keys[5], (D, D), (D // 2) ** -0.5, 0.25, ((0, 32),)),
        "query_bias": bell_draw(arg_keys[6], (D,), 0.3, 1.75, ((0, 32),)),
        "key_weight": bell_draw(arg_keys[7], (D, D), D ** -0.5, 0.1875, ((0, 32),)),
        "value_weight": bell_draw(arg_keys[8], (D, D), D ** -0.5, 0.1875, ((0, 32),)),
        "value_bias": bell_draw(arg_keys[9], (D,), 0.05, 0.3125, ((0, 32),)),
        "out_weight": bell_draw(arg_keys[10], (D, D), (D // 64) ** -0.5, 1.5, ((0, 32),)),
        "out_bias": bell_draw(arg_keys[11], (D,), 0.1, 0.625, ((0, 32),)),
        "second_gain": jnp.clip(1.0 + 0.1 * jax.random.normal(arg_keys[12], (D,), jnp.float32), 0.5, 1.5).astype(jnp.bfloat16),
        "second_shift": bell_draw(arg_keys[13], (D,), 0.2, 1.25, ((0, 32),)),
        "gate_weight": bell_draw(arg_keys[14], (D, FF), D ** -0.5, 0.1875, ((0, 8), (1, 4))),
        "gate_bias": bell_draw(arg_keys[15], (FF,), 0.3, 1.75, ((0, 4),)),
        "up_weight": bell_draw(arg_keys[16], (D, FF), D ** -0.5, 0.1875, ((0, 8), (1, 4))),
        "up_bias": bell_draw(arg_keys[17], (FF,), 0.3, 1.75, ((0, 4),)),
        "inner_gain": jnp.clip(1.0 + 0.1 * jax.random.normal(arg_keys[18], (FF,), jnp.float32), 0.5, 1.5).astype(jnp.bfloat16),
        "inner_shift": bell_draw(arg_keys[19], (FF,), 0.2, 1.25, ((0, 4),)),
        "down_weight": bell_draw(arg_keys[20], (FF, D), FF ** -0.5, 0.109375, ((0, 4), (1, 8))),
        "down_bias": bell_draw(arg_keys[21], (D,), 0.1, 0.625, ((0, 32),)),
    }


norm_eps = 1e-06

@jax.custom_vjp
def low(v):
    return lax.optimization_barrier(v.astype(jnp.bfloat16)).astype(jnp.float32)

@jax.custom_vjp
def low_back(v):
    return v

def low_keep(v):
    return (low(v), None)

def low_pass(kept, grad):
    return (grad,)

def back_keep(v):
    return (v, None)

def back_low(kept, grad):
    return (low(grad),)
low.defvjp(low_keep, low_pass)
low_back.defvjp(back_keep, back_low)

def layer_norm(values, gain_vec, shift_vec):
    row_mean = lax.optimization_barrier(jnp.mean(values, axis=-1, keepdims=True))
    centered = values - row_mean
    row_var = lax.optimization_barrier(jnp.mean(centered * centered, axis=-1, keepdims=True))
    return centered * lax.rsqrt(row_var + norm_eps) * gain_vec + shift_vec

def rope_tables():
    positions = jnp.arange(GRID * GRID, dtype=jnp.int32)
    row_place = (positions // GRID).astype(jnp.float32)
    col_place = (positions % GRID).astype(jnp.float32)
    quarter = HD // 4
    frequency = jnp.power(10000.0, -jnp.arange(quarter, dtype=jnp.float32) / quarter)
    angles = jnp.concatenate([row_place[:, None] * frequency[None, :], col_place[:, None] * frequency[None, :]], axis=1)
    angles = jnp.repeat(angles, 2, axis=1)
    return (jnp.cos(angles), jnp.sin(angles))

def pair_swap(values):
    paired = values.reshape(values.shape[:-1] + (values.shape[-1] // 2, 2))
    return jnp.stack([-paired[..., 1], paired[..., 0]], axis=-1).reshape(values.shape)

def rotate(values, cosine_table, sine_table):
    return values * cosine_table[:, None, :] + pair_swap(values) * sine_table[:, None, :]

def project(left_rows, right_rows):
    return jnp.dot(left_rows, right_rows, precision=lax.Precision.HIGHEST, preferred_element_type=jnp.float32)

def block_forward(inputs_f, params, flags, cosine_table, sine_table, unit_mask):
    gain_one, shift_one, query_full, query_shift, key_full, value_full, value_shift, out_full, out_shift, gain_two, shift_two, gate_full, gate_shift, up_full, up_shift, inner_scale, inner_offset, down_full, down_shift = params
    low_one = low(layer_norm(inputs_f, gain_one, shift_one))
    query_lin = low(low_back(project(low_one, query_full) + query_shift))
    key_lin = low(low_back(project(low_one, key_full)))
    value_lin = low(low_back(project(low_one, value_full) + value_shift))
    head_shape = inputs_f.shape[:2] + (H, HD)
    query_rot = low(rotate(query_lin.reshape(head_shape), cosine_table, sine_table))
    key_rot = low(rotate(key_lin.reshape(head_shape), cosine_table, sine_table))
    scores = jnp.einsum('bqhd,bkhd->bhqk', query_rot, key_rot, precision=lax.Precision.HIGHEST)
    scores = low_back(scores * (1.0 / math.sqrt(HD)))
    top_score = lax.optimization_barrier(jnp.max(scores, axis=-1, keepdims=True))
    weights_exp = jnp.exp(scores - top_score)
    attn_probs = weights_exp / lax.optimization_barrier(jnp.sum(weights_exp, axis=-1, keepdims=True))
    mixed_heads = jnp.einsum('bhqk,bkhd->bqhd', low(attn_probs), value_lin.reshape(head_shape), precision=lax.Precision.HIGHEST)
    mixed_heads = low(low_back(mixed_heads))
    residual = inputs_f + low_back(project(mixed_heads.reshape(inputs_f.shape), out_full) + out_shift)
    low_two = low(layer_norm(residual, gain_two, shift_two))
    gate_pre = low_back(project(low_two, gate_full) + gate_shift)
    up_pre = low_back(project(low_two, up_full) + up_shift)
    hidden = jax.nn.silu(gate_pre) * up_pre * unit_mask
    unit_mean = lax.optimization_barrier(jnp.sum(hidden, axis=-1, keepdims=True)) / FF_REAL
    unit_var = lax.optimization_barrier(jnp.sum(hidden * hidden, axis=-1, keepdims=True)) / FF_REAL - unit_mean * unit_mean
    normed_hidden = low(((hidden - unit_mean) * lax.rsqrt(unit_var + norm_eps) * inner_scale + inner_offset) * unit_mask)
    branch_out = low_back(project(normed_hidden, down_full) + down_shift)
    return flags[:, None, None] * (residual + branch_out)

def reference(inputs, slot_flag, cotangent, first_gain, first_shift, query_weight, query_bias, key_weight, value_weight, value_bias, out_weight, out_bias, second_gain, second_shift, gate_weight, gate_bias, up_weight, up_bias, inner_gain, inner_shift, down_weight, down_bias):
    params = tuple((member.astype(jnp.float32) for member in (first_gain, first_shift, query_weight, query_bias, key_weight, value_weight, value_bias, out_weight, out_bias, second_gain, second_shift, gate_weight, gate_bias, up_weight, up_bias, inner_gain, inner_shift, down_weight, down_bias)))
    cosine_table, sine_table = rope_tables()
    unit_mask = (jnp.arange(FF, dtype=jnp.int32) < FF_REAL).astype(jnp.float32)
    batch_seqs = 2
    steps_count = SEQS // batch_seqs
    inputs_b = inputs.astype(jnp.float32).reshape(steps_count, batch_seqs, LEN, D)
    cotangent_b = cotangent.astype(jnp.float32).reshape(steps_count, batch_seqs, LEN, D)
    flags_b = slot_flag.astype(jnp.float32).reshape(steps_count, batch_seqs)

    def one_step(running, batch_items):
        batch_inputs, batch_cot, batch_flags = batch_items

        def forward(values, weights):
            return block_forward(values, weights, batch_flags, cosine_table, sine_table, unit_mask)
        result, pullback = jax.vjp(forward, batch_inputs, params)
        input_part, weight_parts = pullback(batch_cot)
        running = tuple((total_part + grad_part for total_part, grad_part in zip(running, weight_parts)))
        return (running, (result.astype(jnp.bfloat16), input_part.astype(jnp.bfloat16)))
    initial = tuple((jnp.zeros(member.shape, jnp.float32) for member in params))
    totals, (results, input_grads) = lax.scan(one_step, initial, (inputs_b, cotangent_b, flags_b))
    return (results.reshape(SEQS, LEN, D), input_grads.reshape(SEQS, LEN, D), totals[0], totals[1], totals[2], totals[3], totals[4], totals[5], totals[6], totals[7], totals[8], totals[9], totals[10], totals[11], totals[12], totals[13], totals[14], totals[15], totals[16], totals[17], totals[18])
```

```python
import math

import jax
import jax.numpy as jnp
from jax import lax
from jax.experimental import pallas as pl
from jax.experimental.pallas import tpu as pltpu
from jax.sharding import PartitionSpec as P

HD = 64
PAIR = 2 * HD
FF_REAL = 2730
GRID = 32


norm_eps = 1e-06


def layer_norm(values, gain_vec, shift_vec):
    row_mean = jnp.mean(values, axis=-1, keepdims=True)
    centered = values - row_mean
    row_var = jnp.mean(centered * centered, axis=-1, keepdims=True)
    inv_std = lax.rsqrt(row_var + norm_eps)
    unit_rows = centered * inv_std
    return (unit_rows * gain_vec + shift_vec, unit_rows, inv_std)


def norm_backward(grad_values, unit_rows, inv_std, gain_vec):
    scaled = grad_values * gain_vec
    centered = scaled - jnp.mean(scaled, axis=-1, keepdims=True)
    centered = centered - unit_rows * jnp.mean(scaled * unit_rows, axis=-1, keepdims=True)
    return centered * inv_std


def rope_tables():
    positions = jnp.arange(GRID * GRID, dtype=jnp.int32)
    row_place = (positions // GRID).astype(jnp.float32)
    col_place = (positions % GRID).astype(jnp.float32)
    quarter = HD // 4
    frequency = jnp.power(10000.0, -jnp.arange(quarter, dtype=jnp.float32) / quarter)
    angles = jnp.concatenate(
        [row_place[:, None] * frequency[None, :], col_place[:, None] * frequency[None, :]], axis=1
    )
    angles = jnp.repeat(angles, 2, axis=1)
    return (jnp.cos(angles), jnp.sin(angles))


def pair_swap(values):
    count = values.shape[-1]
    lanes = lax.broadcasted_iota(jnp.int32, values.shape, 1)
    following = pltpu.roll(values, count - 1, 1)
    preceding = pltpu.roll(values, 1, 1)
    return jnp.where(lanes % 2 == 0, -following, preceding)


def rotate(values, cosine_table, sine_table):
    return values * cosine_table + pair_swap(values) * sine_table


def rotate_back(grad_values, cosine_table, sine_table):
    return grad_values * cosine_table - pair_swap(grad_values * sine_table)


def outer_product(left_rows, right_rows):
    return lax.dot_general(
        left_rows, right_rows, (((0,), (0,)), ((), ())), preferred_element_type=jnp.float32
    )


def times_transpose(left_rows, right_rows):
    return lax.dot_general(
        left_rows, right_rows, (((1,), (1,)), ((), ())), preferred_element_type=jnp.float32
    )


def gather_rows(block_values):
    return lax.all_gather(block_values, "tensor", axis=0, tiled=True)


def tensor_sums(first_sum, second_sum):
    both = lax.psum(jnp.stack([first_sum, second_sum]).astype(jnp.bfloat16), "tensor")
    return (both[0].astype(jnp.float32), both[1].astype(jnp.float32))


def scatter_rows(term_fn, row_total):
    return lax.psum_scatter(
        term_fn(jnp.int32(0), row_total * lax.axis_size("tensor")).astype(jnp.bfloat16),
        "tensor",
        scatter_dimension=0,
        tiled=True,
    ).astype(jnp.float32)


def head_masks(axis):
    shape = (1, PAIR) if axis == 1 else (PAIR, 1)
    place = lax.broadcasted_iota(jnp.int32, shape, axis)
    first = (place < HD).astype(jnp.float32)
    return (first, 1.0 - first)


def load_heads(qkv_ref, cosine_ref, sine_ref, query_s, key_s, value_s):
    rows = qkv_ref[...].reshape(query_s.shape[0], 3 * PAIR)
    cosine, sine = cosine_ref[...], sine_ref[...]
    query_rot = rotate(rows[:, :PAIR].astype(jnp.float32), cosine, sine).astype(jnp.bfloat16)
    query_s[...] = (query_rot.astype(jnp.float32) * (1.0 / math.sqrt(HD))).astype(jnp.bfloat16)
    key_rot = rotate(rows[:, PAIR : 2 * PAIR].astype(jnp.float32), cosine, sine)
    key_s[...] = key_rot.astype(jnp.bfloat16)
    value_s[...] = rows[:, 2 * PAIR :]


def forward_kernel(qkv_ref, cosine_ref, sine_ref, mixed_ref, query_s, key_s, value_s):
    load_heads(qkv_ref, cosine_ref, sine_ref, query_s, key_s, value_s)
    pieces, _, piece_len, _ = mixed_ref.shape
    masks = head_masks(1)

    def one_piece(piece, carry):
        start = pl.multiple_of(piece * piece_len, piece_len)
        query_rows = query_s[pl.ds(start, piece_len), :]
        mixed = jnp.zeros((piece_len, PAIR), jnp.float32)
        for mask in masks:
            own_query = query_rows * mask.astype(jnp.bfloat16)
            scores = times_transpose(own_query, key_s[...])
            weights_exp = jnp.exp(scores - jnp.max(scores, axis=-1, keepdims=True))
            inverse = 1.0 / jnp.sum(weights_exp, axis=-1, keepdims=True)
            probs_low = (weights_exp * inverse).astype(jnp.bfloat16)
            part = jnp.dot(probs_low, value_s[...], preferred_element_type=jnp.float32)
            mixed = mixed + part * mask
        mixed_ref[piece, 0] = mixed.astype(jnp.bfloat16)
        return carry

    lax.fori_loop(0, pieces, one_piece, 0)


def backward_kernel(
    qkv_ref, grad_ref, cosine_ref, sine_ref, out_ref,
    query_s, key_s, value_s, turned_s, key_grad_s, value_grad_s,
):
    load_heads(qkv_ref, cosine_ref, sine_ref, query_s, key_s, value_s)
    pieces, _, piece_len, _ = grad_ref.shape
    turned_s[...] = key_s[...].astype(jnp.float32).T.astype(jnp.bfloat16)
    key_grad_s[...] = jnp.zeros_like(key_grad_s)
    value_grad_s[...] = jnp.zeros_like(value_grad_s)
    row_masks = head_masks(1)
    column_masks = head_masks(0)

    def one_piece(piece, carry):
        start = pl.multiple_of(piece * piece_len, piece_len)
        rows = pl.ds(start, piece_len)
        query_rows = query_s[rows, :]
        grad_rows = grad_ref[piece, 0]
        query_grad = jnp.zeros((PAIR, piece_len), jnp.float32)
        for mask, column_mask in zip(row_masks, column_masks):
            own_query = query_rows * mask.astype(jnp.bfloat16)
            own_grad = grad_rows * mask.astype(jnp.bfloat16)
            scores = times_transpose(key_s[...], own_query)
            weights_exp = jnp.exp(scores - jnp.max(scores, axis=0, keepdims=True))
            probs = weights_exp * (1.0 / jnp.sum(weights_exp, axis=0, keepdims=True))
            grad_probs = times_transpose(value_s[...], own_grad)
            row_dot = jnp.sum(grad_probs * probs, axis=0, keepdims=True)
            grad_scores = (probs * (grad_probs - row_dot)).astype(jnp.bfloat16)
            value_grad_s[...] += jnp.dot(
                probs.astype(jnp.bfloat16), own_grad, preferred_element_type=jnp.float32
            )
            key_grad_s[...] += jnp.dot(grad_scores, own_query, preferred_element_type=jnp.float32)
            own_turned = turned_s[...] * column_mask.astype(jnp.bfloat16)
            query_grad = query_grad + jnp.dot(
                own_turned, grad_scores, preferred_element_type=jnp.float32
            )
        query_grad = query_grad.T * (1.0 / math.sqrt(HD))
        turned = rotate_back(query_grad, cosine_ref[rows, :], sine_ref[rows, :])
        out_ref[piece, 0, :, :PAIR] = turned.astype(jnp.bfloat16)
        return carry

    lax.fori_loop(0, pieces, one_piece, 0)
    piece_shape = (pieces, 1, piece_len, PAIR)
    key_grad = rotate_back(key_grad_s[...], cosine_ref[...], sine_ref[...])
    out_ref[:, :, :, PAIR : 2 * PAIR] = key_grad.astype(jnp.bfloat16).reshape(piece_shape)
    out_ref[:, :, :, 2 * PAIR :] = value_grad_s[...].astype(jnp.bfloat16).reshape(piece_shape)


def attention_call(kernel, name, qkv, extra, tables, out_lanes, more_scratch, products):
    pieces, seq_count, piece_len, lanes = qkv.shape
    pair_count = lanes // (3 * PAIR)
    length = pieces * piece_len

    def per_pair(wide):
        return pl.BlockSpec((pieces, 1, piece_len, wide), lambda seq, pair: (0, seq, 0, pair))

    table_spec = pl.BlockSpec((length, PAIR), lambda seq, pair: (0, 0))
    blocks = seq_count * pair_count
    return pl.pallas_call(
        kernel,
        name=name,
        grid=(seq_count, pair_count),
        in_specs=[per_pair(3 * PAIR)] + [per_pair(PAIR)] * len(extra) + [table_spec] * 2,
        out_specs=per_pair(out_lanes),
        out_shape=jax.ShapeDtypeStruct(
            (pieces, seq_count, piece_len, pair_count * out_lanes), jnp.bfloat16
        ),
        scratch_shapes=[pltpu.VMEM((length, PAIR), jnp.bfloat16)] * 3 + more_scratch,
        compiler_params=pltpu.CompilerParams(vmem_limit_bytes=48 << 20),
        cost_estimate=pl.CostEstimate(
            flops=blocks * products * 4 * length * length * PAIR,
            bytes_accessed=blocks * length * PAIR * 16,
            transcendentals=blocks * 2 * length * length,
        ),
    )(qkv, *extra, *tables)


def attend_forward(qkv, tables):
    return attention_call(forward_kernel, "attend_forward", qkv, (), tables, PAIR, [], 2)


def attend_backward(qkv, grad_mixed, tables):
    length = qkv.shape[0] * qkv.shape[2]
    more = [
        pltpu.VMEM((PAIR, length), jnp.bfloat16),
        pltpu.VMEM((length, PAIR), jnp.float32),
        pltpu.VMEM((length, PAIR), jnp.float32),
    ]
    return attention_call(
        backward_kernel, "attend_backward", qkv, (grad_mixed,), tables, 3 * PAIR, more, 5
    )


def hidden_forward(token_rows, gate_part, up_part, gate_shift, up_shift, unit_mask):
    gate_pre = jnp.dot(token_rows, gate_part, preferred_element_type=jnp.float32) + gate_shift
    up_pre = jnp.dot(token_rows, up_part, preferred_element_type=jnp.float32) + up_shift
    return (gate_pre, up_pre, jax.nn.silu(gate_pre) * up_pre * unit_mask)


def inner_normalize(hidden, first_sum, second_sum, inner_scale, inner_offset, unit_mask):
    unit_mean = first_sum[:, None] / FF_REAL
    unit_var = second_sum[:, None] / FF_REAL - unit_mean * unit_mean
    inv_std = lax.rsqrt(unit_var + norm_eps)
    unit_hidden = (hidden - unit_mean) * inv_std
    normed = ((unit_hidden * inner_scale + inner_offset) * unit_mask).astype(jnp.bfloat16)
    return (normed, unit_hidden, inv_std)


def hidden_backward_terms(grad_normed, unit_hidden, inner_scale, unit_mask):
    scaled = grad_normed * unit_mask * inner_scale
    return (scaled, jnp.sum(scaled, axis=-1), jnp.sum(scaled * unit_hidden, axis=-1))


def gate_grads(scaled, scaled_sum, cross_sum, unit_hidden, inv_std, gate_pre, up_pre, unit_mask):
    grad_hidden = (
        unit_mask
        * (scaled - scaled_sum[:, None] / FF_REAL - unit_hidden * cross_sum[:, None] / FF_REAL)
        * inv_std
    )
    sigmoid_gate = jax.nn.sigmoid(gate_pre)
    grad_gate = (
        grad_hidden * up_pre * sigmoid_gate * (1.0 + gate_pre * (1.0 - sigmoid_gate))
    ).astype(jnp.bfloat16)
    grad_up = (grad_hidden * gate_pre * sigmoid_gate).astype(jnp.bfloat16)
    return (grad_gate, grad_up)


def vector_sums(grad_gate, grad_up, grad_normed, unit_hidden, unit_mask):
    return (
        jnp.sum(grad_gate, axis=0, dtype=jnp.float32),
        jnp.sum(grad_up, axis=0, dtype=jnp.float32),
        jnp.sum(grad_normed * unit_mask * unit_hidden, axis=0),
        jnp.sum(grad_normed * unit_mask, axis=0),
    )


def on_device(
    inputs,
    slot_flag,
    cotangent,
    first_gain,
    first_shift,
    query_weight,
    query_bias,
    key_weight,
    value_weight,
    value_bias,
    out_weight,
    out_bias,
    second_gain,
    second_shift,
    gate_weight,
    gate_bias,
    up_weight,
    up_bias,
    inner_gain,
    inner_shift,
    down_weight,
    down_bias,
):
    seq_local, piece_len, width = inputs.shape
    head_ways = lax.axis_size("heads")
    seq_len = piece_len * head_ways
    group_width = width // head_ways
    group_pairs = group_width // PAIR
    token_count = seq_local * piece_len
    fsdp_ways, tensor_ways = lax.axis_size("fsdp"), lax.axis_size("tensor")
    row_part = query_weight.shape[0]
    group_index = lax.axis_index("heads")
    inputs_group = lax.all_gather(inputs, "heads", axis=0, tiled=True)
    stacked = jnp.stack(
        [
            member.reshape(row_part, head_ways, group_pairs, PAIR)
            for member in (query_weight, key_weight, value_weight)
        ],
        axis=3,
    ).reshape(row_part, head_ways, 3 * group_width)
    own_columns = lax.all_to_all(
        stacked.transpose(1, 0, 2), "heads", split_axis=0, concat_axis=0, tiled=True
    )
    qkv_part = lax.all_gather(
        own_columns.reshape(head_ways * row_part, 3 * group_width),
        ("fsdp", "tensor"),
        axis=0,
        tiled=True,
    )
    qkv_part = (
        qkv_part.reshape(fsdp_ways, tensor_ways, head_ways, row_part, 3 * group_width)
        .transpose(0, 2, 1, 3, 4)
        .reshape(width, 3 * group_width)
    )
    out_full = lax.all_gather(out_weight, ("fsdp", "heads", "tensor"), axis=0, tiled=True)
    gathered = tuple(
        lax.all_gather(member, ("fsdp", "heads", "tensor"), axis=0, tiled=True)
        for member in (
            first_gain,
            first_shift,
            query_bias,
            value_bias,
            out_bias,
            second_gain,
            second_shift,
            down_bias,
        )
    )
    gain_one, shift_one, query_shift, value_shift, out_shift, gain_two, shift_two, down_shift = [
        member.astype(jnp.float32) for member in gathered
    ]
    gate_part, up_part, down_part = (
        lax.all_gather(gate_weight, ("fsdp", "heads"), axis=0, tiled=True),
        lax.all_gather(up_weight, ("fsdp", "heads"), axis=0, tiled=True),
        lax.all_gather(down_weight, ("fsdp", "heads"), axis=1, tiled=True),
    )
    inputs_f = inputs.astype(jnp.float32)
    _, unit_one, inv_one = layer_norm(inputs_f, gain_one, shift_one)
    normed_group, _, _ = layer_norm(
        inputs_group.reshape(-1, width).astype(jnp.float32), gain_one, shift_one
    )
    low_one = normed_group.astype(jnp.bfloat16)

    def group_lanes(full_vec):
        own = lax.dynamic_slice_in_dim(full_vec, group_index * group_width, group_width, 0)
        return own.reshape(group_pairs, PAIR)

    query_lanes, value_lanes = group_lanes(query_shift), group_lanes(value_shift)
    qkv_shift = jnp.stack([query_lanes, jnp.zeros_like(query_lanes), value_lanes], axis=1)
    qkv_lin = (
        (jnp.dot(low_one, qkv_part, preferred_element_type=jnp.float32) + qkv_shift.reshape(-1))
        .astype(jnp.bfloat16)
        .reshape(head_ways, seq_local, piece_len, 3 * group_width)
    )
    tables = tuple(jnp.tile(table, (1, PAIR // HD)) for table in rope_tables())
    mixed_heads = attend_forward(qkv_lin, tables)
    mixed_parts = lax.all_to_all(mixed_heads, "heads", split_axis=0, concat_axis=0, tiled=True)
    mixed_flat = mixed_parts.transpose(1, 2, 0, 3).reshape(token_count, width)
    residual = inputs_f + (
        jnp.dot(mixed_flat, out_full, preferred_element_type=jnp.float32) + out_shift
    ).reshape(inputs.shape)
    normed_two, unit_two, inv_two = layer_norm(residual, gain_two, shift_two)
    low_two = normed_two.astype(jnp.bfloat16)
    flag_rows = slot_flag.astype(jnp.float32)[:, None, None]
    grad_total = flag_rows * cotangent.astype(jnp.float32)
    grad_branch = grad_total.astype(jnp.bfloat16)
    down_shift_grad = jnp.sum(grad_branch.reshape(token_count, width), axis=0, dtype=jnp.float32)
    ffn_local = gate_part.shape[1]
    token_rows3 = gather_rows(low_two)
    token_rows = token_rows3.reshape(-1, width)
    col_index = lax.axis_index("tensor") * ffn_local + jnp.arange(ffn_local, dtype=jnp.int32)
    unit_mask = (col_index < FF_REAL).astype(jnp.float32)
    gate_pre, up_pre, hidden = hidden_forward(
        token_rows,
        gate_part,
        up_part,
        gate_bias.astype(jnp.float32),
        up_bias.astype(jnp.float32),
        unit_mask,
    )
    first_sum, second_sum = tensor_sums(jnp.sum(hidden, axis=-1), jnp.sum(hidden * hidden, axis=-1))
    inner_scale = inner_gain.astype(jnp.float32)
    normed_hidden, unit_hidden, inv_hidden = inner_normalize(
        hidden, first_sum, second_sum, inner_scale, inner_shift.astype(jnp.float32), unit_mask
    )
    hidden_seqs = normed_hidden.reshape(token_rows3.shape[0], piece_len, ffn_local)

    def down_term(row_start, row_count):
        picked = hidden_seqs.reshape(-1, ffn_local)
        return jnp.dot(picked, down_part, preferred_element_type=jnp.float32).reshape(
            row_count, piece_len, width
        )

    branch_out = scatter_rows(down_term, seq_local)
    grad_rows = gather_rows(grad_branch).reshape(-1, width)
    down_grad = outer_product(normed_hidden, grad_rows)
    grad_normed = times_transpose(grad_rows, down_part)
    scaled, scaled_sum, cross_sum = hidden_backward_terms(
        grad_normed, unit_hidden, inner_scale, unit_mask
    )
    scaled_sum, cross_sum = tensor_sums(scaled_sum, cross_sum)
    grad_gate, grad_up = gate_grads(
        scaled, scaled_sum, cross_sum, unit_hidden, inv_hidden, gate_pre, up_pre, unit_mask
    )
    gate_grad = outer_product(token_rows, grad_gate)
    up_grad = outer_product(token_rows, grad_up)
    vector_grads = vector_sums(grad_gate, grad_up, grad_normed, unit_hidden, unit_mask)
    gate_seqs = grad_gate.reshape(-1, piece_len, ffn_local)
    up_seqs = grad_up.reshape(-1, piece_len, ffn_local)

    def input_term(row_start, row_count):
        picked_gate = gate_seqs.reshape(-1, ffn_local)
        picked_up = up_seqs.reshape(-1, ffn_local)
        summed = times_transpose(picked_gate, gate_part) + times_transpose(picked_up, up_part)
        return summed.reshape(row_count, piece_len, width)

    grad_normed_two = scatter_rows(input_term, seq_local)
    output = (flag_rows * (residual + branch_out + down_shift)).astype(jnp.bfloat16)
    gate_weight_grad, up_weight_grad, down_weight_grad = (
        lax.psum_scatter(
            gate_grad.astype(jnp.bfloat16), ("fsdp", "heads"), scatter_dimension=0, tiled=True
        ).astype(jnp.float32),
        lax.psum_scatter(
            up_grad.astype(jnp.bfloat16), ("fsdp", "heads"), scatter_dimension=0, tiled=True
        ).astype(jnp.float32),
        lax.psum_scatter(
            down_grad.astype(jnp.bfloat16), ("fsdp", "heads"), scatter_dimension=1, tiled=True
        ).astype(jnp.float32),
    )
    gate_bias_grad, up_bias_grad, inner_gain_grad, inner_shift_grad = lax.psum(
        (vector_grads[0], vector_grads[1], vector_grads[2], vector_grads[3]), ("fsdp", "heads")
    )
    grad_residual = grad_total + norm_backward(grad_normed_two, unit_two, inv_two, gain_two)
    gain_two_grad = jnp.sum((grad_normed_two * unit_two).reshape(token_count, width), axis=0)
    shift_two_grad = jnp.sum(grad_normed_two.reshape(token_count, width), axis=0)
    grad_attn = grad_residual.astype(jnp.bfloat16).reshape(token_count, width)
    out_weight_part = outer_product(mixed_flat, grad_attn)
    out_shift_grad = jnp.sum(grad_attn, axis=0, dtype=jnp.float32)
    grad_mixed = times_transpose(grad_attn, out_full).astype(jnp.bfloat16)
    grad_parts = grad_mixed.reshape(seq_local, piece_len, head_ways, group_width)
    grad_heads = lax.all_to_all(
        grad_parts.transpose(2, 0, 1, 3), "heads", split_axis=0, concat_axis=0, tiled=True
    )
    qkv_grad = attend_backward(qkv_lin, grad_heads, tables)
    qkv_grad = qkv_grad.reshape(head_ways * token_count, 3 * group_width)
    grad_normed_one = (
        lax.psum_scatter(
            times_transpose(qkv_grad, qkv_part).astype(jnp.bfloat16),
            "heads",
            scatter_dimension=0,
            tiled=True,
        )
        .astype(jnp.float32)
        .reshape(inputs.shape)
    )
    qkv_weight_part = (
        outer_product(low_one, qkv_grad)
        .astype(jnp.bfloat16)
        .reshape(fsdp_ways, head_ways, tensor_ways, row_part, 3 * group_width)
        .transpose(0, 2, 1, 3, 4)
        .reshape(width, 3 * group_width)
    )
    qkv_rows = lax.psum_scatter(
        qkv_weight_part, ("fsdp", "tensor"), scatter_dimension=0, tiled=True
    )
    qkv_columns = lax.all_to_all(qkv_rows, "heads", split_axis=0, concat_axis=0, tiled=True)
    qkv_weight_grads = (
        qkv_columns.reshape(head_ways, row_part, group_pairs, 3, PAIR)
        .transpose(3, 1, 0, 2, 4)
        .reshape(3, row_part, width)
        .astype(jnp.float32)
    )
    qkv_shift_grad = jnp.sum(qkv_grad, axis=0, dtype=jnp.float32).reshape(group_pairs, 3, PAIR)

    def place_lanes(own_lanes):
        return lax.dynamic_update_slice_in_dim(
            jnp.zeros((width,), jnp.float32), own_lanes.reshape(-1), group_index * group_width, 0
        )

    query_shift_grad = place_lanes(qkv_shift_grad[:, 0])
    value_shift_grad = place_lanes(qkv_shift_grad[:, 2])
    input_grad = (
        grad_residual + norm_backward(grad_normed_one, unit_one, inv_one, gain_one)
    ).astype(jnp.bfloat16)
    gain_one_grad = jnp.sum((grad_normed_one * unit_one).reshape(token_count, width), axis=0)
    shift_one_grad = jnp.sum(grad_normed_one.reshape(token_count, width), axis=0)
    attn_sums = (
        qkv_weight_grads[0],
        qkv_weight_grads[1],
        qkv_weight_grads[2],
        lax.psum_scatter(
            out_weight_part.astype(jnp.bfloat16),
            ("fsdp", "heads", "tensor"),
            scatter_dimension=0,
            tiled=True,
        ).astype(jnp.float32),
        lax.psum_scatter(
            gain_one_grad, ("fsdp", "heads", "tensor"), scatter_dimension=0, tiled=True
        ),
        lax.psum_scatter(
            shift_one_grad, ("fsdp", "heads", "tensor"), scatter_dimension=0, tiled=True
        ),
        lax.psum_scatter(
            query_shift_grad, ("fsdp", "heads", "tensor"), scatter_dimension=0, tiled=True
        ),
        lax.psum_scatter(
            value_shift_grad, ("fsdp", "heads", "tensor"), scatter_dimension=0, tiled=True
        ),
        lax.psum_scatter(
            out_shift_grad, ("fsdp", "heads", "tensor"), scatter_dimension=0, tiled=True
        ),
        lax.psum_scatter(
            gain_two_grad, ("fsdp", "heads", "tensor"), scatter_dimension=0, tiled=True
        ),
        lax.psum_scatter(
            shift_two_grad, ("fsdp", "heads", "tensor"), scatter_dimension=0, tiled=True
        ),
        lax.psum_scatter(
            down_shift_grad, ("fsdp", "heads", "tensor"), scatter_dimension=0, tiled=True
        ),
    )
    return (
        output,
        input_grad,
        attn_sums[4],
        attn_sums[5],
        attn_sums[0],
        attn_sums[6],
        attn_sums[1],
        attn_sums[2],
        attn_sums[7],
        attn_sums[3],
        attn_sums[8],
        attn_sums[9],
        attn_sums[10],
        gate_weight_grad,
        gate_bias_grad,
        up_weight_grad,
        up_bias_grad,
        inner_gain_grad,
        inner_shift_grad,
        down_weight_grad,
        attn_sums[11],
    )


def solution(mesh):
    return jax.shard_map(
        on_device,
        mesh=mesh,
        in_specs=(
            P(("fsdp", "tensor"), "heads", None),
            P(("fsdp", "tensor")),
            P(("fsdp", "tensor"), "heads", None),
            P(("fsdp", "heads", "tensor")),
            P(("fsdp", "heads", "tensor")),
            P(("fsdp", "heads", "tensor"), None),
            P(("fsdp", "heads", "tensor")),
            P(("fsdp", "heads", "tensor"), None),
            P(("fsdp", "heads", "tensor"), None),
            P(("fsdp", "heads", "tensor")),
            P(("fsdp", "heads", "tensor"), None),
            P(("fsdp", "heads", "tensor")),
            P(("fsdp", "heads", "tensor")),
            P(("fsdp", "heads", "tensor")),
            P(("fsdp", "heads"), "tensor"),
            P("tensor"),
            P(("fsdp", "heads"), "tensor"),
            P("tensor"),
            P("tensor"),
            P("tensor"),
            P("tensor", ("fsdp", "heads")),
            P(("fsdp", "heads", "tensor")),
        ),
        out_specs=(
            P(("fsdp", "tensor"), "heads", None),
            P(("fsdp", "tensor"), "heads", None),
            P(("fsdp", "heads", "tensor")),
            P(("fsdp", "heads", "tensor")),
            P(("fsdp", "heads", "tensor"), None),
            P(("fsdp", "heads", "tensor")),
            P(("fsdp", "heads", "tensor"), None),
            P(("fsdp", "heads", "tensor"), None),
            P(("fsdp", "heads", "tensor")),
            P(("fsdp", "heads", "tensor"), None),
            P(("fsdp", "heads", "tensor")),
            P(("fsdp", "heads", "tensor")),
            P(("fsdp", "heads", "tensor")),
            P(("fsdp", "heads"), "tensor"),
            P("tensor"),
            P(("fsdp", "heads"), "tensor"),
            P("tensor"),
            P("tensor"),
            P("tensor"),
            P("tensor", ("fsdp", "heads")),
            P(("fsdp", "heads", "tensor")),
        ),
        check_vma=False,
    )
```

```python
import math

import jax
import jax.numpy as jnp
from jax import lax
from jax.experimental import pallas as pl
from jax.experimental.pallas import tpu as pltpu
from jax.sharding import PartitionSpec as P

HD = 64
PAIR = 2 * HD
FF_REAL = 2730
GRID = 32


norm_eps = 1e-06


def layer_norm(values, gain_vec, shift_vec):
    row_mean = jnp.mean(values, axis=-1, keepdims=True)
    centered = values - row_mean
    row_var = jnp.mean(centered * centered, axis=-1, keepdims=True)
    inv_std = lax.rsqrt(row_var + norm_eps)
    unit_rows = centered * inv_std
    return (unit_rows * gain_vec + shift_vec, unit_rows, inv_std)


def norm_backward(grad_values, unit_rows, inv_std, gain_vec):
    scaled = grad_values * gain_vec
    centered = scaled - jnp.mean(scaled, axis=-1, keepdims=True)
    centered = centered - unit_rows * jnp.mean(scaled * unit_rows, axis=-1, keepdims=True)
    return centered * inv_std


def rope_tables():
    positions = jnp.arange(GRID * GRID, dtype=jnp.int32)
    row_place = (positions // GRID).astype(jnp.float32)
    col_place = (positions % GRID).astype(jnp.float32)
    quarter = HD // 4
    frequency = jnp.power(10000.0, -jnp.arange(quarter, dtype=jnp.float32) / quarter)
    angles = jnp.concatenate(
        [row_place[:, None] * frequency[None, :], col_place[:, None] * frequency[None, :]], axis=1
    )
    angles = jnp.repeat(angles, 2, axis=1)
    return (jnp.cos(angles), jnp.sin(angles))


def pair_swap(values):
    count = values.shape[-1]
    lanes = lax.broadcasted_iota(jnp.int32, values.shape, 1)
    following = pltpu.roll(values, count - 1, 1)
    preceding = pltpu.roll(values, 1, 1)
    return jnp.where(lanes % 2 == 0, -following, preceding)


def rotate(values, cosine_table, sine_table):
    return values * cosine_table + pair_swap(values) * sine_table


def rotate_back(grad_values, cosine_table, sine_table):
    return grad_values * cosine_table - pair_swap(grad_values * sine_table)


def outer_product(left_rows, right_rows):
    return lax.dot_general(
        left_rows, right_rows, (((0,), (0,)), ((), ())), preferred_element_type=jnp.float32
    )


def times_transpose(left_rows, right_rows):
    return lax.dot_general(
        left_rows, right_rows, (((1,), (1,)), ((), ())), preferred_element_type=jnp.float32
    )


def gather_rows(block_values):
    return lax.all_gather(block_values, "tensor", axis=0, tiled=True)


def tensor_sums(first_sum, second_sum):
    both = lax.psum(jnp.stack([first_sum, second_sum]).astype(jnp.bfloat16), "tensor")
    return (both[0].astype(jnp.float32), both[1].astype(jnp.float32))


def cube_pairs(ways, bit):
    return [(place, place ^ (1 << bit)) for place in range(ways)]


def cube_gather(block, axis_name):
    ways = lax.axis_size(axis_name)
    bits = ways.bit_length() - 1
    index = lax.axis_index(axis_name)
    held = block.reshape((1,) * bits + block.shape)
    for bit in reversed(range(bits)):
        place = bits - 1 - bit
        other = lax.ppermute(held, axis_name, cube_pairs(ways, bit))
        held = jnp.where(
            (index >> bit) % 2 == 0,
            jnp.concatenate([held, other], axis=place),
            jnp.concatenate([other, held], axis=place),
        )
    return held.reshape((ways * block.shape[0],) + block.shape[1:])


def cube_scatter(terms, axis_name):
    ways = lax.axis_size(axis_name)
    bits = ways.bit_length() - 1
    index = lax.axis_index(axis_name)
    held = terms.reshape((2,) * bits + terms.shape[1:])
    for bit in range(bits):
        place = bits - 1 - bit
        mine = (index >> bit) % 2
        kept = lax.dynamic_index_in_dim(held, mine, place, keepdims=False)
        sent = lax.dynamic_index_in_dim(held, 1 - mine, place, keepdims=False)
        other = lax.ppermute(sent.astype(jnp.bfloat16), axis_name, cube_pairs(ways, bit))
        held = kept.astype(jnp.float32) + other.astype(jnp.float32)
    return held


def line_pairs(ways):
    upward = [(place, place + 1) for place in range(ways - 1)]
    return (upward, [(target, source) for source, target in upward])


def line_gather(block, axis_name):
    ways = lax.axis_size(axis_name)
    upward, downward = line_pairs(ways)
    below, above = [block], [block]
    for _ in range(ways - 1):
        below.append(lax.ppermute(below[-1], axis_name, upward))
        above.append(lax.ppermute(above[-1], axis_name, downward))
    around = jnp.stack(below[:0:-1] + [block] + above[1:])
    picked = lax.dynamic_slice_in_dim(around, ways - 1 - lax.axis_index(axis_name), ways, 0)
    return picked.reshape((ways * block.shape[0],) + block.shape[1:])


def line_scatter(terms, axis_name):
    ways = lax.axis_size(axis_name)
    upward, downward = line_pairs(ways)
    index = lax.axis_index(axis_name)

    def term(offset):
        place = jnp.clip(index + offset, 0, ways - 1)
        return lax.dynamic_index_in_dim(terms, place, 0, keepdims=False).astype(jnp.float32)

    total = term(0)
    for sign, pairs in ((1, upward), (-1, downward)):
        running = term(sign * (ways - 1))
        for distance in range(ways - 1, 0, -1):
            if distance < ways - 1:
                running = term(sign * distance) + running.astype(jnp.float32)
            running = lax.ppermute(running.astype(jnp.bfloat16), axis_name, pairs)
        total = total + running.astype(jnp.float32)
    return total


def scatter_rows(term_fn, row_total):
    return lax.psum_scatter(
        term_fn(jnp.int32(0), row_total * lax.axis_size("tensor")).astype(jnp.bfloat16),
        "tensor",
        scatter_dimension=0,
        tiled=True,
    ).astype(jnp.float32)


def head_masks(axis):
    shape = (1, PAIR) if axis == 1 else (PAIR, 1)
    place = lax.broadcasted_iota(jnp.int32, shape, axis)
    first = (place < HD).astype(jnp.float32)
    return (first, 1.0 - first)


def load_heads(qkv_ref, cosine_ref, sine_ref, query_s, key_s, value_s):
    rows = qkv_ref[...].reshape(query_s.shape[0], 3 * PAIR)
    cosine, sine = cosine_ref[...], sine_ref[...]
    query_rot = rotate(rows[:, :PAIR].astype(jnp.float32), cosine, sine).astype(jnp.bfloat16)
    query_s[...] = (query_rot.astype(jnp.float32) * (1.0 / math.sqrt(HD))).astype(jnp.bfloat16)
    key_rot = rotate(rows[:, PAIR : 2 * PAIR].astype(jnp.float32), cosine, sine)
    key_s[...] = key_rot.astype(jnp.bfloat16)
    value_s[...] = rows[:, 2 * PAIR :]


def forward_kernel(qkv_ref, cosine_ref, sine_ref, mixed_ref, query_s, key_s, value_s):
    load_heads(qkv_ref, cosine_ref, sine_ref, query_s, key_s, value_s)
    pieces, _, piece_len, _ = mixed_ref.shape
    masks = head_masks(1)

    def one_piece(piece, carry):
        start = pl.multiple_of(piece * piece_len, piece_len)
        query_rows = query_s[pl.ds(start, piece_len), :]
        mixed = jnp.zeros((piece_len, PAIR), jnp.float32)
        for mask in masks:
            own_query = query_rows * mask.astype(jnp.bfloat16)
            scores = times_transpose(own_query, key_s[...])
            weights_exp = jnp.exp(scores - jnp.max(scores, axis=-1, keepdims=True))
            inverse = 1.0 / jnp.sum(weights_exp, axis=-1, keepdims=True)
            probs_low = (weights_exp * inverse).astype(jnp.bfloat16)
            part = jnp.dot(probs_low, value_s[...], preferred_element_type=jnp.float32)
            mixed = mixed + part * mask
        mixed_ref[piece, 0] = mixed.astype(jnp.bfloat16)
        return carry

    lax.fori_loop(0, pieces, one_piece, 0)


def backward_kernel(
    qkv_ref, grad_ref, cosine_ref, sine_ref, out_ref,
    query_s, key_s, value_s, turned_s, key_grad_s, value_grad_s,
):
    load_heads(qkv_ref, cosine_ref, sine_ref, query_s, key_s, value_s)
    pieces, _, piece_len, _ = grad_ref.shape
    turned_s[...] = key_s[...].astype(jnp.float32).T.astype(jnp.bfloat16)
    key_grad_s[...] = jnp.zeros_like(key_grad_s)
    value_grad_s[...] = jnp.zeros_like(value_grad_s)
    row_masks = head_masks(1)
    column_masks = head_masks(0)

    def one_piece(piece, carry):
        start = pl.multiple_of(piece * piece_len, piece_len)
        rows = pl.ds(start, piece_len)
        query_rows = query_s[rows, :]
        grad_rows = grad_ref[piece, 0]
        query_grad = jnp.zeros((PAIR, piece_len), jnp.float32)
        for mask, column_mask in zip(row_masks, column_masks):
            own_query = query_rows * mask.astype(jnp.bfloat16)
            own_grad = grad_rows * mask.astype(jnp.bfloat16)
            scores = times_transpose(key_s[...], own_query)
            weights_exp = jnp.exp(scores - jnp.max(scores, axis=0, keepdims=True))
            probs = weights_exp * (1.0 / jnp.sum(weights_exp, axis=0, keepdims=True))
            grad_probs = times_transpose(value_s[...], own_grad)
            row_dot = jnp.sum(grad_probs * probs, axis=0, keepdims=True)
            grad_scores = (probs * (grad_probs - row_dot)).astype(jnp.bfloat16)
            value_grad_s[...] += jnp.dot(
                probs.astype(jnp.bfloat16), own_grad, preferred_element_type=jnp.float32
            )
            key_grad_s[...] += jnp.dot(grad_scores, own_query, preferred_element_type=jnp.float32)
            own_turned = turned_s[...] * column_mask.astype(jnp.bfloat16)
            query_grad = query_grad + jnp.dot(
                own_turned, grad_scores, preferred_element_type=jnp.float32
            )
        query_grad = query_grad.T * (1.0 / math.sqrt(HD))
        turned = rotate_back(query_grad, cosine_ref[rows, :], sine_ref[rows, :])
        out_ref[piece, 0, :, :PAIR] = turned.astype(jnp.bfloat16)
        return carry

    lax.fori_loop(0, pieces, one_piece, 0)
    piece_shape = (pieces, 1, piece_len, PAIR)
    key_grad = rotate_back(key_grad_s[...], cosine_ref[...], sine_ref[...])
    out_ref[:, :, :, PAIR : 2 * PAIR] = key_grad.astype(jnp.bfloat16).reshape(piece_shape)
    out_ref[:, :, :, 2 * PAIR :] = value_grad_s[...].astype(jnp.bfloat16).reshape(piece_shape)


def attention_call(kernel, name, qkv, extra, tables, out_lanes, more_scratch, products):
    pieces, seq_count, piece_len, lanes = qkv.shape
    pair_count = lanes // (3 * PAIR)
    length = pieces * piece_len

    def per_pair(wide):
        return pl.BlockSpec((pieces, 1, piece_len, wide), lambda seq, pair: (0, seq, 0, pair))

    table_spec = pl.BlockSpec((length, PAIR), lambda seq, pair: (0, 0))
    blocks = seq_count * pair_count
    return pl.pallas_call(
        kernel,
        name=name,
        grid=(seq_count, pair_count),
        in_specs=[per_pair(3 * PAIR)] + [per_pair(PAIR)] * len(extra) + [table_spec] * 2,
        out_specs=per_pair(out_lanes),
        out_shape=jax.ShapeDtypeStruct(
            (pieces, seq_count, piece_len, pair_count * out_lanes), jnp.bfloat16
        ),
        scratch_shapes=[pltpu.VMEM((length, PAIR), jnp.bfloat16)] * 3 + more_scratch,
        compiler_params=pltpu.CompilerParams(vmem_limit_bytes=48 << 20),
        cost_estimate=pl.CostEstimate(
            flops=blocks * products * 4 * length * length * PAIR,
            bytes_accessed=blocks * length * PAIR * 16,
            transcendentals=blocks * 2 * length * length,
        ),
    )(qkv, *extra, *tables)


def attend_forward(qkv, tables):
    return attention_call(forward_kernel, "attend_forward", qkv, (), tables, PAIR, [], 2)


def attend_backward(qkv, grad_mixed, tables):
    length = qkv.shape[0] * qkv.shape[2]
    more = [
        pltpu.VMEM((PAIR, length), jnp.bfloat16),
        pltpu.VMEM((length, PAIR), jnp.float32),
        pltpu.VMEM((length, PAIR), jnp.float32),
    ]
    return attention_call(
        backward_kernel, "attend_backward", qkv, (grad_mixed,), tables, 3 * PAIR, more, 5
    )


def hidden_forward(token_rows, gate_part, up_part, gate_shift, up_shift, unit_mask):
    gate_pre = jnp.dot(token_rows, gate_part, preferred_element_type=jnp.float32) + gate_shift
    up_pre = jnp.dot(token_rows, up_part, preferred_element_type=jnp.float32) + up_shift
    return (gate_pre, up_pre, jax.nn.silu(gate_pre) * up_pre * unit_mask)


def inner_normalize(hidden, first_sum, second_sum, inner_scale, inner_offset, unit_mask):
    unit_mean = first_sum[:, None] / FF_REAL
    unit_var = second_sum[:, None] / FF_REAL - unit_mean * unit_mean
    inv_std = lax.rsqrt(unit_var + norm_eps)
    unit_hidden = (hidden - unit_mean) * inv_std
    normed = ((unit_hidden * inner_scale + inner_offset) * unit_mask).astype(jnp.bfloat16)
    return (normed, unit_hidden, inv_std)


def hidden_backward_terms(grad_normed, unit_hidden, inner_scale, unit_mask):
    scaled = grad_normed * unit_mask * inner_scale
    return (scaled, jnp.sum(scaled, axis=-1), jnp.sum(scaled * unit_hidden, axis=-1))


def gate_grads(scaled, scaled_sum, cross_sum, unit_hidden, inv_std, gate_pre, up_pre, unit_mask):
    grad_hidden = (
        unit_mask
        * (scaled - scaled_sum[:, None] / FF_REAL - unit_hidden * cross_sum[:, None] / FF_REAL)
        * inv_std
    )
    sigmoid_gate = jax.nn.sigmoid(gate_pre)
    grad_gate = (
        grad_hidden * up_pre * sigmoid_gate * (1.0 + gate_pre * (1.0 - sigmoid_gate))
    ).astype(jnp.bfloat16)
    grad_up = (grad_hidden * gate_pre * sigmoid_gate).astype(jnp.bfloat16)
    return (grad_gate, grad_up)


def vector_sums(grad_gate, grad_up, grad_normed, unit_hidden, unit_mask):
    return (
        jnp.sum(grad_gate, axis=0, dtype=jnp.float32),
        jnp.sum(grad_up, axis=0, dtype=jnp.float32),
        jnp.sum(grad_normed * unit_mask * unit_hidden, axis=0),
        jnp.sum(grad_normed * unit_mask, axis=0),
    )


def on_device(
    inputs,
    slot_flag,
    cotangent,
    first_gain,
    first_shift,
    query_weight,
    query_bias,
    key_weight,
    value_weight,
    value_bias,
    out_weight,
    out_bias,
    second_gain,
    second_shift,
    gate_weight,
    gate_bias,
    up_weight,
    up_bias,
    inner_gain,
    inner_shift,
    down_weight,
    down_bias,
):
    seq_local, piece_len, width = inputs.shape
    head_ways = lax.axis_size("heads")
    seq_len = piece_len * head_ways
    group_width = width // head_ways
    group_pairs = group_width // PAIR
    token_count = seq_local * piece_len
    fsdp_ways, tensor_ways = lax.axis_size("fsdp"), lax.axis_size("tensor")
    row_part = query_weight.shape[0]
    group_index = lax.axis_index("heads")
    inputs_group = cube_gather(inputs, "heads")
    grad_flags = slot_flag.astype(jnp.float32)[:, None, None]
    grad_total = grad_flags * cotangent.astype(jnp.float32)
    grad_branch = grad_total.astype(jnp.bfloat16)
    grad_rows = line_gather(grad_branch, "tensor").reshape(-1, width)
    stacked = jnp.stack(
        [
            member.reshape(row_part, head_ways, group_pairs, PAIR)
            for member in (query_weight, key_weight, value_weight)
        ],
        axis=3,
    ).reshape(row_part, head_ways, 3 * group_width)
    vectors = jnp.concatenate(
        [
            first_gain,
            first_shift,
            query_bias,
            value_bias,
            out_bias,
            second_gain,
            second_shift,
            down_bias,
        ]
    )
    vector_row = jnp.pad(vectors, (0, 3 * group_width - vectors.shape[0]))
    sent_columns = jnp.concatenate(
        [
            stacked.transpose(1, 0, 2),
            jnp.broadcast_to(vector_row, (head_ways, 1, 3 * group_width)),
        ],
        axis=1,
    )
    own_columns = lax.all_to_all(
        sent_columns, "heads", split_axis=0, concat_axis=0, tiled=True
    )
    columns = lax.all_gather(
        own_columns.reshape(-1, 3 * group_width), ("fsdp", "tensor"), axis=0, tiled=True
    )
    columns = columns.reshape(
        fsdp_ways, tensor_ways, head_ways, row_part + 1, 3 * group_width
    ).transpose(0, 2, 1, 3, 4)
    qkv_part = columns[:, :, :, :row_part].reshape(width, 3 * group_width)
    gathered = (
        columns[:, :, :, row_part, : vectors.shape[0]]
        .reshape(-1, 8, row_part)
        .transpose(1, 0, 2)
        .reshape(8, width)
    )
    out_full = lax.all_gather(out_weight, ("fsdp", "heads", "tensor"), axis=0, tiled=True)
    gain_one, shift_one, query_shift, value_shift, out_shift, gain_two, shift_two, down_shift = [
        member.astype(jnp.float32) for member in gathered
    ]
    gate_part, up_part, down_part = (
        lax.all_gather(gate_weight, ("fsdp", "heads"), axis=0, tiled=True),
        lax.all_gather(up_weight, ("fsdp", "heads"), axis=0, tiled=True),
        lax.all_gather(down_weight, ("fsdp", "heads"), axis=1, tiled=True),
    )
    inputs_f = inputs.astype(jnp.float32)
    _, unit_one, inv_one = layer_norm(inputs_f, gain_one, shift_one)
    normed_group, _, _ = layer_norm(
        inputs_group.reshape(-1, width).astype(jnp.float32), gain_one, shift_one
    )
    low_one = normed_group.astype(jnp.bfloat16)

    def group_lanes(full_vec):
        own = lax.dynamic_slice_in_dim(full_vec, group_index * group_width, group_width, 0)
        return own.reshape(group_pairs, PAIR)

    query_lanes, value_lanes = group_lanes(query_shift), group_lanes(value_shift)
    qkv_shift = jnp.stack([query_lanes, jnp.zeros_like(query_lanes), value_lanes], axis=1)
    qkv_lin = (
        (jnp.dot(low_one, qkv_part, preferred_element_type=jnp.float32) + qkv_shift.reshape(-1))
        .astype(jnp.bfloat16)
        .reshape(head_ways, seq_local, piece_len, 3 * group_width)
    )
    tables = tuple(jnp.tile(table, (1, PAIR // HD)) for table in rope_tables())
    mixed_heads = attend_forward(qkv_lin, tables)
    mixed_parts = lax.all_to_all(mixed_heads, "heads", split_axis=0, concat_axis=0, tiled=True)
    mixed_flat = mixed_parts.transpose(1, 2, 0, 3).reshape(token_count, width)
    residual = inputs_f + (
        jnp.dot(mixed_flat, out_full, preferred_element_type=jnp.float32) + out_shift
    ).reshape(inputs.shape)
    normed_two, unit_two, inv_two = layer_norm(residual, gain_two, shift_two)
    low_two = normed_two.astype(jnp.bfloat16)
    flag_rows = slot_flag.astype(jnp.float32)[:, None, None]
    down_shift_grad = jnp.sum(grad_branch.reshape(token_count, width), axis=0, dtype=jnp.float32)
    ffn_local = gate_part.shape[1]
    token_rows3 = gather_rows(low_two)
    token_rows = token_rows3.reshape(-1, width)
    col_index = lax.axis_index("tensor") * ffn_local + jnp.arange(ffn_local, dtype=jnp.int32)
    unit_mask = (col_index < FF_REAL).astype(jnp.float32)
    gate_pre, up_pre, hidden = hidden_forward(
        token_rows,
        gate_part,
        up_part,
        gate_bias.astype(jnp.float32),
        up_bias.astype(jnp.float32),
        unit_mask,
    )
    first_sum, second_sum = tensor_sums(jnp.sum(hidden, axis=-1), jnp.sum(hidden * hidden, axis=-1))
    inner_scale = inner_gain.astype(jnp.float32)
    normed_hidden, unit_hidden, inv_hidden = inner_normalize(
        hidden, first_sum, second_sum, inner_scale, inner_shift.astype(jnp.float32), unit_mask
    )
    hidden_seqs = normed_hidden.reshape(token_rows3.shape[0], piece_len, ffn_local)

    def down_term(row_start, row_count):
        picked = hidden_seqs.reshape(-1, ffn_local)
        return jnp.dot(picked, down_part, preferred_element_type=jnp.float32).reshape(
            row_count, piece_len, width
        )

    branch_terms = down_term(0, seq_local * tensor_ways).astype(jnp.bfloat16)
    branch_out = line_scatter(
        branch_terms.reshape((tensor_ways,) + inputs.shape), "tensor"
    )
    down_grad = outer_product(normed_hidden, grad_rows)
    grad_normed = times_transpose(grad_rows, down_part)
    scaled, scaled_sum, cross_sum = hidden_backward_terms(
        grad_normed, unit_hidden, inner_scale, unit_mask
    )
    scaled_sum, cross_sum = tensor_sums(scaled_sum, cross_sum)
    grad_gate, grad_up = gate_grads(
        scaled, scaled_sum, cross_sum, unit_hidden, inv_hidden, gate_pre, up_pre, unit_mask
    )
    gate_grad = outer_product(token_rows, grad_gate)
    up_grad = outer_product(token_rows, grad_up)
    vector_grads = vector_sums(grad_gate, grad_up, grad_normed, unit_hidden, unit_mask)
    gate_seqs = grad_gate.reshape(-1, piece_len, ffn_local)
    up_seqs = grad_up.reshape(-1, piece_len, ffn_local)

    def input_term(row_start, row_count):
        picked_gate = gate_seqs.reshape(-1, ffn_local)
        picked_up = up_seqs.reshape(-1, ffn_local)
        summed = times_transpose(picked_gate, gate_part) + times_transpose(picked_up, up_part)
        return summed.reshape(row_count, piece_len, width)

    grad_normed_two = scatter_rows(input_term, seq_local)
    output = (flag_rows * (residual + branch_out + down_shift)).astype(jnp.bfloat16)
    gate_weight_grad, up_weight_grad, down_weight_grad = (
        lax.psum_scatter(
            gate_grad.astype(jnp.bfloat16), ("fsdp", "heads"), scatter_dimension=0, tiled=True
        ).astype(jnp.float32),
        lax.psum_scatter(
            up_grad.astype(jnp.bfloat16), ("fsdp", "heads"), scatter_dimension=0, tiled=True
        ).astype(jnp.float32),
        lax.psum_scatter(
            down_grad.astype(jnp.bfloat16), ("fsdp", "heads"), scatter_dimension=1, tiled=True
        ).astype(jnp.float32),
    )
    gate_bias_grad, up_bias_grad, inner_gain_grad, inner_shift_grad = lax.psum(
        (vector_grads[0], vector_grads[1], vector_grads[2], vector_grads[3]), ("fsdp", "heads")
    )
    grad_residual = grad_total + norm_backward(grad_normed_two, unit_two, inv_two, gain_two)
    gain_two_grad = jnp.sum((grad_normed_two * unit_two).reshape(token_count, width), axis=0)
    shift_two_grad = jnp.sum(grad_normed_two.reshape(token_count, width), axis=0)
    grad_attn = grad_residual.astype(jnp.bfloat16).reshape(token_count, width)
    out_weight_part = outer_product(mixed_flat, grad_attn)
    out_shift_grad = jnp.sum(grad_attn, axis=0, dtype=jnp.float32)
    grad_mixed = times_transpose(grad_attn, out_full).astype(jnp.bfloat16)
    grad_parts = grad_mixed.reshape(seq_local, piece_len, head_ways, group_width)
    grad_heads = lax.all_to_all(
        grad_parts.transpose(2, 0, 1, 3), "heads", split_axis=0, concat_axis=0, tiled=True
    )
    qkv_grad = attend_backward(qkv_lin, grad_heads, tables)
    qkv_grad = qkv_grad.reshape(head_ways * token_count, 3 * group_width)
    group_terms = times_transpose(qkv_grad, qkv_part).astype(jnp.bfloat16)
    grad_normed_one = cube_scatter(
        group_terms.reshape((head_ways,) + inputs.shape), "heads"
    )
    qkv_weight_part = (
        outer_product(low_one, qkv_grad)
        .astype(jnp.bfloat16)
        .reshape(fsdp_ways, head_ways, tensor_ways, row_part, 3 * group_width)
        .transpose(0, 2, 1, 3, 4)
        .reshape(width, 3 * group_width)
    )
    qkv_rows = lax.psum_scatter(
        qkv_weight_part, ("fsdp", "tensor"), scatter_dimension=0, tiled=True
    )
    qkv_columns = lax.all_to_all(qkv_rows, "heads", split_axis=0, concat_axis=0, tiled=True)
    qkv_weight_grads = (
        qkv_columns.reshape(head_ways, row_part, group_pairs, 3, PAIR)
        .transpose(3, 1, 0, 2, 4)
        .reshape(3, row_part, width)
        .astype(jnp.float32)
    )
    qkv_shift_grad = jnp.sum(qkv_grad, axis=0, dtype=jnp.float32).reshape(group_pairs, 3, PAIR)

    def place_lanes(own_lanes):
        return lax.dynamic_update_slice_in_dim(
            jnp.zeros((width,), jnp.float32), own_lanes.reshape(-1), group_index * group_width, 0
        )

    query_shift_grad = place_lanes(qkv_shift_grad[:, 0])
    value_shift_grad = place_lanes(qkv_shift_grad[:, 2])
    input_grad = (
        grad_residual + norm_backward(grad_normed_one, unit_one, inv_one, gain_one)
    ).astype(jnp.bfloat16)
    gain_one_grad = jnp.sum((grad_normed_one * unit_one).reshape(token_count, width), axis=0)
    shift_one_grad = jnp.sum(grad_normed_one.reshape(token_count, width), axis=0)
    attn_sums = (
        qkv_weight_grads[0],
        qkv_weight_grads[1],
        qkv_weight_grads[2],
        lax.psum_scatter(
            lax.psum_scatter(
                out_weight_part.astype(jnp.bfloat16),
                ("fsdp", "heads"),
                scatter_dimension=0,
                tiled=True,
            ),
            "tensor",
            scatter_dimension=0,
            tiled=True,
        ).astype(jnp.float32),
        lax.psum_scatter(
            gain_one_grad, ("fsdp", "heads", "tensor"), scatter_dimension=0, tiled=True
        ),
        lax.psum_scatter(
            shift_one_grad, ("fsdp", "heads", "tensor"), scatter_dimension=0, tiled=True
        ),
        lax.psum_scatter(
            query_shift_grad, ("fsdp", "heads", "tensor"), scatter_dimension=0, tiled=True
        ),
        lax.psum_scatter(
            value_shift_grad, ("fsdp", "heads", "tensor"), scatter_dimension=0, tiled=True
        ),
        lax.psum_scatter(
            out_shift_grad, ("fsdp", "heads", "tensor"), scatter_dimension=0, tiled=True
        ),
        lax.psum_scatter(
            gain_two_grad, ("fsdp", "heads", "tensor"), scatter_dimension=0, tiled=True
        ),
        lax.psum_scatter(
            shift_two_grad, ("fsdp", "heads", "tensor"), scatter_dimension=0, tiled=True
        ),
        lax.psum_scatter(
            down_shift_grad, ("fsdp", "heads", "tensor"), scatter_dimension=0, tiled=True
        ),
    )
    return (
        output,
        input_grad,
        attn_sums[4],
        attn_sums[5],
        attn_sums[0],
        attn_sums[6],
        attn_sums[1],
        attn_sums[2],
        attn_sums[7],
        attn_sums[3],
        attn_sums[8],
        attn_sums[9],
        attn_sums[10],
        gate_weight_grad,
        gate_bias_grad,
        up_weight_grad,
        up_bias_grad,
        inner_gain_grad,
        inner_shift_grad,
        down_weight_grad,
        attn_sums[11],
    )


def solution(mesh):
    return jax.shard_map(
        on_device,
        mesh=mesh,
        in_specs=(
            P(("fsdp", "tensor"), "heads", None),
            P(("fsdp", "tensor")),
            P(("fsdp", "tensor"), "heads", None),
            P(("fsdp", "heads", "tensor")),
            P(("fsdp", "heads", "tensor")),
            P(("fsdp", "heads", "tensor"), None),
            P(("fsdp", "heads", "tensor")),
            P(("fsdp", "heads", "tensor"), None),
            P(("fsdp", "heads", "tensor"), None),
            P(("fsdp", "heads", "tensor")),
            P(("fsdp", "heads", "tensor"), None),
            P(("fsdp", "heads", "tensor")),
            P(("fsdp", "heads", "tensor")),
            P(("fsdp", "heads", "tensor")),
            P(("fsdp", "heads"), "tensor"),
            P("tensor"),
            P(("fsdp", "heads"), "tensor"),
            P("tensor"),
            P("tensor"),
            P("tensor"),
            P("tensor", ("fsdp", "heads")),
            P(("fsdp", "heads", "tensor")),
        ),
        out_specs=(
            P(("fsdp", "tensor"), "heads", None),
            P(("fsdp", "tensor"), "heads", None),
            P(("fsdp", "heads", "tensor")),
            P(("fsdp", "heads", "tensor")),
            P(("fsdp", "heads", "tensor"), None),
            P(("fsdp", "heads", "tensor")),
            P(("fsdp", "heads", "tensor"), None),
            P(("fsdp", "heads", "tensor"), None),
            P(("fsdp", "heads", "tensor")),
            P(("fsdp", "heads", "tensor"), None),
            P(("fsdp", "heads", "tensor")),
            P(("fsdp", "heads", "tensor")),
            P(("fsdp", "heads", "tensor")),
            P(("fsdp", "heads"), "tensor"),
            P("tensor"),
            P(("fsdp", "heads"), "tensor"),
            P("tensor"),
            P("tensor"),
            P("tensor"),
            P("tensor", ("fsdp", "heads")),
            P(("fsdp", "heads", "tensor")),
        ),
        check_vma=False,
    )
```

```python
import math

import jax
import jax.numpy as jnp
from jax import lax
from jax.experimental import pallas as pl
from jax.experimental.pallas import tpu as pltpu
from jax.sharding import PartitionSpec as P

HD = 64
PAIR = 2 * HD
FF_REAL = 2730
GRID = 32


norm_eps = 1e-06


def layer_norm(values, gain_vec, shift_vec):
    row_mean = jnp.mean(values, axis=-1, keepdims=True)
    centered = values - row_mean
    row_var = jnp.mean(centered * centered, axis=-1, keepdims=True)
    inv_std = lax.rsqrt(row_var + norm_eps)
    unit_rows = centered * inv_std
    return (unit_rows * gain_vec + shift_vec, unit_rows, inv_std)


def norm_backward(grad_values, unit_rows, inv_std, gain_vec):
    scaled = grad_values * gain_vec
    centered = scaled - jnp.mean(scaled, axis=-1, keepdims=True)
    centered = centered - unit_rows * jnp.mean(scaled * unit_rows, axis=-1, keepdims=True)
    return centered * inv_std


def rope_tables():
    positions = jnp.arange(GRID * GRID, dtype=jnp.int32)
    row_place = (positions // GRID).astype(jnp.float32)
    col_place = (positions % GRID).astype(jnp.float32)
    quarter = HD // 4
    frequency = jnp.power(10000.0, -jnp.arange(quarter, dtype=jnp.float32) / quarter)
    angles = jnp.concatenate(
        [row_place[:, None] * frequency[None, :], col_place[:, None] * frequency[None, :]], axis=1
    )
    angles = jnp.repeat(angles, 2, axis=1)
    return (jnp.cos(angles), jnp.sin(angles))


def pair_swap(values):
    count = values.shape[-1]
    lanes = lax.broadcasted_iota(jnp.int32, values.shape, 1)
    following = pltpu.roll(values, count - 1, 1)
    preceding = pltpu.roll(values, 1, 1)
    return jnp.where(lanes % 2 == 0, -following, preceding)


def rotate(values, cosine_table, sine_table):
    return values * cosine_table + pair_swap(values) * sine_table


def rotate_back(grad_values, cosine_table, sine_table):
    return grad_values * cosine_table - pair_swap(grad_values * sine_table)


def outer_product(left_rows, right_rows):
    return lax.dot_general(
        left_rows, right_rows, (((0,), (0,)), ((), ())), preferred_element_type=jnp.float32
    )


def times_transpose(left_rows, right_rows):
    return lax.dot_general(
        left_rows, right_rows, (((1,), (1,)), ((), ())), preferred_element_type=jnp.float32
    )


def gather_rows(block_values):
    return lax.all_gather(block_values, "tensor", axis=0, tiled=True)


def tensor_sums(first_sum, second_sum):
    both = lax.psum(jnp.stack([first_sum, second_sum]).astype(jnp.bfloat16), "tensor")
    return (both[0].astype(jnp.float32), both[1].astype(jnp.float32))


def cube_pairs(ways, bit):
    return [(place, place ^ (1 << bit)) for place in range(ways)]


def cube_gather(block, axis_name):
    ways = lax.axis_size(axis_name)
    bits = ways.bit_length() - 1
    index = lax.axis_index(axis_name)
    held = block.reshape((1,) * bits + block.shape)
    for bit in reversed(range(bits)):
        place = bits - 1 - bit
        other = lax.ppermute(held, axis_name, cube_pairs(ways, bit))
        held = jnp.where(
            (index >> bit) % 2 == 0,
            jnp.concatenate([held, other], axis=place),
            jnp.concatenate([other, held], axis=place),
        )
    return held.reshape((ways * block.shape[0],) + block.shape[1:])


def cube_scatter(terms, axis_name):
    ways = lax.axis_size(axis_name)
    bits = ways.bit_length() - 1
    index = lax.axis_index(axis_name)
    held = terms.reshape((2,) * bits + terms.shape[1:])
    for bit in range(bits):
        place = bits - 1 - bit
        mine = (index >> bit) % 2
        kept = lax.dynamic_index_in_dim(held, mine, place, keepdims=False)
        sent = lax.dynamic_index_in_dim(held, 1 - mine, place, keepdims=False)
        other = lax.ppermute(sent.astype(jnp.bfloat16), axis_name, cube_pairs(ways, bit))
        held = kept.astype(jnp.float32) + other.astype(jnp.float32)
    return held


def line_pairs(ways):
    upward = [(place, place + 1) for place in range(ways - 1)]
    return (upward, [(target, source) for source, target in upward])


def line_step(below, above, axis_name):
    upward, downward = line_pairs(lax.axis_size(axis_name))
    below.append(lax.ppermute(below[-1], axis_name, upward))
    above.append(lax.ppermute(above[-1], axis_name, downward))


def line_pick(below, above, axis_name):
    ways = lax.axis_size(axis_name)
    block = below[0]
    around = jnp.stack(below[:0:-1] + [block] + above[1:])
    picked = lax.dynamic_slice_in_dim(around, ways - 1 - lax.axis_index(axis_name), ways, 0)
    return picked.reshape((ways * block.shape[0],) + block.shape[1:])


def after(value, *others):
    return lax.optimization_barrier((value,) + others)[0]


def line_scatter(terms, axis_name, gates):
    ways = lax.axis_size(axis_name)
    pairs = line_pairs(ways)
    index = lax.axis_index(axis_name)

    def term(offset):
        place = jnp.clip(index + offset, 0, ways - 1)
        return lax.dynamic_index_in_dim(terms, place, 0, keepdims=False).astype(jnp.float32)

    running = [None, None]
    for step, distance in enumerate(range(ways - 1, 0, -1)):
        for side, sign in ((0, 1), (1, -1)):
            total = term(sign * distance)
            if step > 0:
                total = total + running[side].astype(jnp.float32)
            gated = after(total.astype(jnp.bfloat16), gates[min(step, len(gates) - 1)])
            running[side] = lax.ppermute(gated, axis_name, pairs[side])
    return term(0) + running[0].astype(jnp.float32) + running[1].astype(jnp.float32)


def scatter_rows(term_fn, row_total):
    return lax.psum_scatter(
        term_fn(jnp.int32(0), row_total * lax.axis_size("tensor")).astype(jnp.bfloat16),
        "tensor",
        scatter_dimension=0,
        tiled=True,
    ).astype(jnp.float32)


def head_masks(axis):
    shape = (1, PAIR) if axis == 1 else (PAIR, 1)
    place = lax.broadcasted_iota(jnp.int32, shape, axis)
    first = (place < HD).astype(jnp.float32)
    return (first, 1.0 - first)


def load_heads(qkv_ref, cosine_ref, sine_ref, query_s, key_s, value_s):
    rows = qkv_ref[...].reshape(query_s.shape[0], 3 * PAIR)
    cosine, sine = cosine_ref[...], sine_ref[...]
    query_rot = rotate(rows[:, :PAIR].astype(jnp.float32), cosine, sine).astype(jnp.bfloat16)
    query_s[...] = (query_rot.astype(jnp.float32) * (1.0 / math.sqrt(HD))).astype(jnp.bfloat16)
    key_rot = rotate(rows[:, PAIR : 2 * PAIR].astype(jnp.float32), cosine, sine)
    key_s[...] = key_rot.astype(jnp.bfloat16)
    value_s[...] = rows[:, 2 * PAIR :]


def forward_kernel(qkv_ref, cosine_ref, sine_ref, mixed_ref, query_s, key_s, value_s):
    load_heads(qkv_ref, cosine_ref, sine_ref, query_s, key_s, value_s)
    pieces, _, piece_len, _ = mixed_ref.shape
    masks = head_masks(1)

    def one_piece(piece, carry):
        start = pl.multiple_of(piece * piece_len, piece_len)
        query_rows = query_s[pl.ds(start, piece_len), :]
        mixed = jnp.zeros((piece_len, PAIR), jnp.float32)
        for mask in masks:
            own_query = query_rows * mask.astype(jnp.bfloat16)
            scores = times_transpose(own_query, key_s[...])
            weights_exp = jnp.exp(scores - jnp.max(scores, axis=-1, keepdims=True))
            inverse = 1.0 / jnp.sum(weights_exp, axis=-1, keepdims=True)
            probs_low = (weights_exp * inverse).astype(jnp.bfloat16)
            part = jnp.dot(probs_low, value_s[...], preferred_element_type=jnp.float32)
            mixed = mixed + part * mask
        mixed_ref[piece, 0] = mixed.astype(jnp.bfloat16)
        return carry

    lax.fori_loop(0, pieces, one_piece, 0)


def backward_kernel(
    qkv_ref, grad_ref, cosine_ref, sine_ref, out_ref,
    query_s, key_s, value_s, turned_s, key_grad_s, value_grad_s,
):
    load_heads(qkv_ref, cosine_ref, sine_ref, query_s, key_s, value_s)
    pieces, _, piece_len, _ = grad_ref.shape
    turned_s[...] = key_s[...].astype(jnp.float32).T.astype(jnp.bfloat16)
    key_grad_s[...] = jnp.zeros_like(key_grad_s)
    value_grad_s[...] = jnp.zeros_like(value_grad_s)
    row_masks = head_masks(1)
    column_masks = head_masks(0)

    def one_piece(piece, carry):
        start = pl.multiple_of(piece * piece_len, piece_len)
        rows = pl.ds(start, piece_len)
        query_rows = query_s[rows, :]
        grad_rows = grad_ref[piece, 0]
        query_grad = jnp.zeros((PAIR, piece_len), jnp.float32)
        for mask, column_mask in zip(row_masks, column_masks):
            own_query = query_rows * mask.astype(jnp.bfloat16)
            own_grad = grad_rows * mask.astype(jnp.bfloat16)
            scores = times_transpose(key_s[...], own_query)
            weights_exp = jnp.exp(scores - jnp.max(scores, axis=0, keepdims=True))
            probs = weights_exp * (1.0 / jnp.sum(weights_exp, axis=0, keepdims=True))
            grad_probs = times_transpose(value_s[...], own_grad)
            row_dot = jnp.sum(grad_probs * probs, axis=0, keepdims=True)
            grad_scores = (probs * (grad_probs - row_dot)).astype(jnp.bfloat16)
            value_grad_s[...] += jnp.dot(
                probs.astype(jnp.bfloat16), own_grad, preferred_element_type=jnp.float32
            )
            key_grad_s[...] += jnp.dot(grad_scores, own_query, preferred_element_type=jnp.float32)
            own_turned = turned_s[...] * column_mask.astype(jnp.bfloat16)
            query_grad = query_grad + jnp.dot(
                own_turned, grad_scores, preferred_element_type=jnp.float32
            )
        query_grad = query_grad.T * (1.0 / math.sqrt(HD))
        turned = rotate_back(query_grad, cosine_ref[rows, :], sine_ref[rows, :])
        out_ref[piece, 0, :, :PAIR] = turned.astype(jnp.bfloat16)
        return carry

    lax.fori_loop(0, pieces, one_piece, 0)
    piece_shape = (pieces, 1, piece_len, PAIR)
    key_grad = rotate_back(key_grad_s[...], cosine_ref[...], sine_ref[...])
    out_ref[:, :, :, PAIR : 2 * PAIR] = key_grad.astype(jnp.bfloat16).reshape(piece_shape)
    out_ref[:, :, :, 2 * PAIR :] = value_grad_s[...].astype(jnp.bfloat16).reshape(piece_shape)


def attention_call(kernel, name, qkv, extra, tables, out_lanes, more_scratch, products):
    pieces, seq_count, piece_len, lanes = qkv.shape
    pair_count = lanes // (3 * PAIR)
    length = pieces * piece_len

    def per_pair(wide):
        return pl.BlockSpec((pieces, 1, piece_len, wide), lambda seq, pair: (0, seq, 0, pair))

    table_spec = pl.BlockSpec((length, PAIR), lambda seq, pair: (0, 0))
    blocks = seq_count * pair_count
    return pl.pallas_call(
        kernel,
        name=name,
        grid=(seq_count, pair_count),
        in_specs=[per_pair(3 * PAIR)] + [per_pair(PAIR)] * len(extra) + [table_spec] * 2,
        out_specs=per_pair(out_lanes),
        out_shape=jax.ShapeDtypeStruct(
            (pieces, seq_count, piece_len, pair_count * out_lanes), jnp.bfloat16
        ),
        scratch_shapes=[pltpu.VMEM((length, PAIR), jnp.bfloat16)] * 3 + more_scratch,
        compiler_params=pltpu.CompilerParams(vmem_limit_bytes=48 << 20),
        cost_estimate=pl.CostEstimate(
            flops=blocks * products * 4 * length * length * PAIR,
            bytes_accessed=blocks * length * PAIR * 16,
            transcendentals=blocks * 2 * length * length,
        ),
    )(qkv, *extra, *tables)


def attend_forward(qkv, tables):
    return attention_call(forward_kernel, "attend_forward", qkv, (), tables, PAIR, [], 2)


def attend_backward(qkv, grad_mixed, tables):
    length = qkv.shape[0] * qkv.shape[2]
    more = [
        pltpu.VMEM((PAIR, length), jnp.bfloat16),
        pltpu.VMEM((length, PAIR), jnp.float32),
        pltpu.VMEM((length, PAIR), jnp.float32),
    ]
    return attention_call(
        backward_kernel, "attend_backward", qkv, (grad_mixed,), tables, 3 * PAIR, more, 5
    )


def hidden_forward(token_rows, gate_part, up_part, gate_shift, up_shift, unit_mask):
    gate_pre = jnp.dot(token_rows, gate_part, preferred_element_type=jnp.float32) + gate_shift
    up_pre = jnp.dot(token_rows, up_part, preferred_element_type=jnp.float32) + up_shift
    return (gate_pre, up_pre, jax.nn.silu(gate_pre) * up_pre * unit_mask)


def inner_normalize(hidden, first_sum, second_sum, inner_scale, inner_offset, unit_mask):
    unit_mean = first_sum[:, None] / FF_REAL
    unit_var = second_sum[:, None] / FF_REAL - unit_mean * unit_mean
    inv_std = lax.rsqrt(unit_var + norm_eps)
    unit_hidden = (hidden - unit_mean) * inv_std
    normed = ((unit_hidden * inner_scale + inner_offset) * unit_mask).astype(jnp.bfloat16)
    return (normed, unit_hidden, inv_std)


def hidden_backward_terms(grad_normed, unit_hidden, inner_scale, unit_mask):
    scaled = grad_normed * unit_mask * inner_scale
    return (scaled, jnp.sum(scaled, axis=-1), jnp.sum(scaled * unit_hidden, axis=-1))


def gate_grads(scaled, scaled_sum, cross_sum, unit_hidden, inv_std, gate_pre, up_pre, unit_mask):
    grad_hidden = (
        unit_mask
        * (scaled - scaled_sum[:, None] / FF_REAL - unit_hidden * cross_sum[:, None] / FF_REAL)
        * inv_std
    )
    sigmoid_gate = jax.nn.sigmoid(gate_pre)
    grad_gate = (
        grad_hidden * up_pre * sigmoid_gate * (1.0 + gate_pre * (1.0 - sigmoid_gate))
    ).astype(jnp.bfloat16)
    grad_up = (grad_hidden * gate_pre * sigmoid_gate).astype(jnp.bfloat16)
    return (grad_gate, grad_up)


def vector_sums(grad_gate, grad_up, grad_normed, unit_hidden, unit_mask):
    return (
        jnp.sum(grad_gate, axis=0, dtype=jnp.float32),
        jnp.sum(grad_up, axis=0, dtype=jnp.float32),
        jnp.sum(grad_normed * unit_mask * unit_hidden, axis=0),
        jnp.sum(grad_normed * unit_mask, axis=0),
    )


def on_device(
    inputs,
    slot_flag,
    cotangent,
    first_gain,
    first_shift,
    query_weight,
    query_bias,
    key_weight,
    value_weight,
    value_bias,
    out_weight,
    out_bias,
    second_gain,
    second_shift,
    gate_weight,
    gate_bias,
    up_weight,
    up_bias,
    inner_gain,
    inner_shift,
    down_weight,
    down_bias,
):
    seq_local, piece_len, width = inputs.shape
    head_ways = lax.axis_size("heads")
    seq_len = piece_len * head_ways
    group_width = width // head_ways
    group_pairs = group_width // PAIR
    token_count = seq_local * piece_len
    fsdp_ways, tensor_ways = lax.axis_size("fsdp"), lax.axis_size("tensor")
    row_part = query_weight.shape[0]
    group_index = lax.axis_index("heads")
    inputs_group = cube_gather(inputs, "heads")
    grad_flags = slot_flag.astype(jnp.float32)[:, None, None]
    grad_total = grad_flags * cotangent.astype(jnp.float32)
    grad_branch = grad_total.astype(jnp.bfloat16)
    below, above = [grad_branch], [grad_branch]
    line_step(below, above, "tensor")
    stacked = jnp.stack(
        [
            member.reshape(row_part, head_ways, group_pairs, PAIR)
            for member in (query_weight, key_weight, value_weight)
        ],
        axis=3,
    ).reshape(row_part, head_ways, 3 * group_width)
    vectors = jnp.concatenate(
        [
            first_gain,
            first_shift,
            query_bias,
            value_bias,
            out_bias,
            second_gain,
            second_shift,
            down_bias,
        ]
    )
    vector_row = jnp.pad(vectors, (0, 3 * group_width - vectors.shape[0]))
    sent_columns = jnp.concatenate(
        [
            stacked.transpose(1, 0, 2),
            jnp.broadcast_to(vector_row, (head_ways, 1, 3 * group_width)),
        ],
        axis=1,
    )
    own_columns = lax.all_to_all(
        sent_columns, "heads", split_axis=0, concat_axis=0, tiled=True
    )
    columns = lax.all_gather(
        own_columns.reshape(-1, 3 * group_width), ("fsdp", "tensor"), axis=0, tiled=True
    )
    columns = columns.reshape(
        fsdp_ways, tensor_ways, head_ways, row_part + 1, 3 * group_width
    ).transpose(0, 2, 1, 3, 4)
    qkv_part = columns[:, :, :, :row_part].reshape(width, 3 * group_width)
    gathered = (
        columns[:, :, :, row_part, : vectors.shape[0]]
        .reshape(-1, 8, row_part)
        .transpose(1, 0, 2)
        .reshape(8, width)
    )
    out_full = lax.all_gather(
        lax.all_gather(out_weight, "tensor", axis=0, tiled=True),
        ("fsdp", "heads"),
        axis=0,
        tiled=True,
    )
    gain_one, shift_one, query_shift, value_shift, out_shift, gain_two, shift_two, down_shift = [
        member.astype(jnp.float32) for member in gathered
    ]
    gate_part, up_part, down_part = (
        lax.all_gather(gate_weight, ("fsdp", "heads"), axis=0, tiled=True),
        lax.all_gather(up_weight, ("fsdp", "heads"), axis=0, tiled=True),
        lax.all_gather(down_weight, ("fsdp", "heads"), axis=1, tiled=True),
    )
    inputs_f = inputs.astype(jnp.float32)
    _, unit_one, inv_one = layer_norm(inputs_f, gain_one, shift_one)
    normed_group, _, _ = layer_norm(
        inputs_group.reshape(-1, width).astype(jnp.float32), gain_one, shift_one
    )
    low_one = normed_group.astype(jnp.bfloat16)

    def group_lanes(full_vec):
        own = lax.dynamic_slice_in_dim(full_vec, group_index * group_width, group_width, 0)
        return own.reshape(group_pairs, PAIR)

    query_lanes, value_lanes = group_lanes(query_shift), group_lanes(value_shift)
    qkv_shift = jnp.stack([query_lanes, jnp.zeros_like(query_lanes), value_lanes], axis=1)
    low_one = after(low_one, below[-1], above[-1])
    line_step(below, above, "tensor")
    qkv_lin = (
        (jnp.dot(low_one, qkv_part, preferred_element_type=jnp.float32) + qkv_shift.reshape(-1))
        .astype(jnp.bfloat16)
        .reshape(head_ways, seq_local, piece_len, 3 * group_width)
    )
    tables = tuple(jnp.tile(table, (1, PAIR // HD)) for table in rope_tables())
    attended = after(qkv_lin, below[-1], above[-1])
    for _ in range(tensor_ways - 3):
        line_step(below, above, "tensor")
    mixed_heads = attend_forward(attended, tables)
    mixed_parts = lax.all_to_all(mixed_heads, "heads", split_axis=0, concat_axis=0, tiled=True)
    mixed_parts = after(mixed_parts, below[-1], above[-1])
    grad_rows = line_pick(below, above, "tensor").reshape(-1, width)
    mixed_flat = mixed_parts.transpose(1, 2, 0, 3).reshape(token_count, width)
    residual = inputs_f + (
        jnp.dot(mixed_flat, out_full, preferred_element_type=jnp.float32) + out_shift
    ).reshape(inputs.shape)
    normed_two, unit_two, inv_two = layer_norm(residual, gain_two, shift_two)
    low_two = normed_two.astype(jnp.bfloat16)
    flag_rows = slot_flag.astype(jnp.float32)[:, None, None]
    down_shift_grad = jnp.sum(grad_branch.reshape(token_count, width), axis=0, dtype=jnp.float32)
    ffn_local = gate_part.shape[1]
    token_rows3 = gather_rows(after(low_two, gate_part, up_part))
    token_rows = token_rows3.reshape(-1, width)
    col_index = lax.axis_index("tensor") * ffn_local + jnp.arange(ffn_local, dtype=jnp.int32)
    unit_mask = (col_index < FF_REAL).astype(jnp.float32)
    gate_pre, up_pre, hidden = hidden_forward(
        token_rows,
        gate_part,
        up_part,
        gate_bias.astype(jnp.float32),
        up_bias.astype(jnp.float32),
        unit_mask,
    )
    first_sum, second_sum = tensor_sums(jnp.sum(hidden, axis=-1), jnp.sum(hidden * hidden, axis=-1))
    inner_scale = inner_gain.astype(jnp.float32)
    normed_hidden, unit_hidden, inv_hidden = inner_normalize(
        hidden, first_sum, second_sum, inner_scale, inner_shift.astype(jnp.float32), unit_mask
    )
    hidden_seqs = normed_hidden.reshape(token_rows3.shape[0], piece_len, ffn_local)

    def down_term(row_start, row_count):
        picked = hidden_seqs.reshape(-1, ffn_local)
        return jnp.dot(picked, down_part, preferred_element_type=jnp.float32).reshape(
            row_count, piece_len, width
        )

    down_grad = outer_product(normed_hidden, grad_rows)
    down_weight_grad = lax.psum_scatter(
        down_grad.astype(jnp.bfloat16), ("fsdp", "heads"), scatter_dimension=1, tiled=True
    )
    grad_normed = times_transpose(grad_rows, down_part)
    scaled, scaled_sum, cross_sum = hidden_backward_terms(
        grad_normed, unit_hidden, inner_scale, unit_mask
    )
    scaled_sum, cross_sum = tensor_sums(scaled_sum, cross_sum)
    grad_gate, grad_up = gate_grads(
        scaled, scaled_sum, cross_sum, unit_hidden, inv_hidden, gate_pre, up_pre, unit_mask
    )
    gate_grad = outer_product(token_rows, grad_gate)
    up_grad = outer_product(token_rows, grad_up)
    vector_grads = vector_sums(grad_gate, grad_up, grad_normed, unit_hidden, unit_mask)
    gate_seqs = after(grad_gate, down_weight_grad).reshape(-1, piece_len, ffn_local)
    up_seqs = grad_up.reshape(-1, piece_len, ffn_local)

    def input_term(row_start, row_count):
        picked_gate = gate_seqs.reshape(-1, ffn_local)
        picked_up = up_seqs.reshape(-1, ffn_local)
        summed = times_transpose(picked_gate, gate_part) + times_transpose(picked_up, up_part)
        return summed.reshape(row_count, piece_len, width)

    grad_normed_two = scatter_rows(input_term, seq_local)
    gate_weight_grad, up_weight_grad = (
        lax.psum_scatter(
            gate_grad.astype(jnp.bfloat16), ("fsdp", "heads"), scatter_dimension=0, tiled=True
        ).astype(jnp.float32),
        lax.psum_scatter(
            up_grad.astype(jnp.bfloat16), ("fsdp", "heads"), scatter_dimension=0, tiled=True
        ).astype(jnp.float32),
    )
    down_weight_grad = down_weight_grad.astype(jnp.float32)
    gate_bias_grad, up_bias_grad, inner_gain_grad, inner_shift_grad = lax.psum(
        (vector_grads[0], vector_grads[1], vector_grads[2], vector_grads[3]), ("fsdp", "heads")
    )
    grad_residual = grad_total + norm_backward(grad_normed_two, unit_two, inv_two, gain_two)
    gain_two_grad = jnp.sum((grad_normed_two * unit_two).reshape(token_count, width), axis=0)
    shift_two_grad = jnp.sum(grad_normed_two.reshape(token_count, width), axis=0)
    grad_attn = grad_residual.astype(jnp.bfloat16).reshape(token_count, width)
    out_weight_part = outer_product(mixed_flat, grad_attn)
    out_shift_grad = jnp.sum(grad_attn, axis=0, dtype=jnp.float32)
    grad_mixed = times_transpose(grad_attn, out_full).astype(jnp.bfloat16)
    grad_parts = grad_mixed.reshape(seq_local, piece_len, head_ways, group_width)
    grad_heads = lax.all_to_all(
        grad_parts.transpose(2, 0, 1, 3), "heads", split_axis=0, concat_axis=0, tiled=True
    )
    qkv_grad = attend_backward(qkv_lin, grad_heads, tables)
    branch_terms = down_term(0, seq_local * tensor_ways).astype(jnp.bfloat16)
    branch_out = line_scatter(
        branch_terms.reshape((tensor_ways,) + inputs.shape),
        "tensor",
        (grad_mixed, grad_heads, qkv_grad),
    )
    output = (flag_rows * (residual + branch_out + down_shift)).astype(jnp.bfloat16)
    qkv_grad = qkv_grad.reshape(head_ways * token_count, 3 * group_width)
    group_terms = times_transpose(qkv_grad, qkv_part).astype(jnp.bfloat16)
    grad_normed_one = cube_scatter(
        group_terms.reshape((head_ways,) + inputs.shape), "heads"
    )
    qkv_weight_part = (
        outer_product(low_one, qkv_grad)
        .astype(jnp.bfloat16)
        .reshape(fsdp_ways, head_ways, tensor_ways, row_part, 3 * group_width)
        .transpose(0, 2, 1, 3, 4)
        .reshape(width, 3 * group_width)
    )
    qkv_half = cube_scatter(
        qkv_weight_part.reshape(fsdp_ways, -1, 3 * group_width), "fsdp"
    ).astype(jnp.bfloat16)
    qkv_rows = lax.psum_scatter(qkv_half, "tensor", scatter_dimension=0, tiled=True)
    qkv_shift_grad = jnp.sum(qkv_grad, axis=0, dtype=jnp.float32).reshape(group_pairs, 3, PAIR)

    def place_lanes(own_lanes):
        return lax.dynamic_update_slice_in_dim(
            jnp.zeros((width,), jnp.float32), own_lanes.reshape(-1), group_index * group_width, 0
        )

    query_shift_grad = place_lanes(qkv_shift_grad[:, 0])
    value_shift_grad = place_lanes(qkv_shift_grad[:, 2])
    input_grad = (
        grad_residual + norm_backward(grad_normed_one, unit_one, inv_one, gain_one)
    ).astype(jnp.bfloat16)
    gain_one_grad = jnp.sum((grad_normed_one * unit_one).reshape(token_count, width), axis=0)
    shift_one_grad = jnp.sum(grad_normed_one.reshape(token_count, width), axis=0)
    vector_sums_all = lax.psum(
        jnp.stack(
            [
                gain_one_grad,
                shift_one_grad,
                query_shift_grad,
                value_shift_grad,
                out_shift_grad,
                gain_two_grad,
                shift_two_grad,
                down_shift_grad,
            ]
        ),
        ("fsdp", "heads", "tensor"),
    )
    device_place = (
        lax.axis_index("fsdp") * head_ways + group_index
    ) * tensor_ways + lax.axis_index("tensor")
    own_sums = lax.dynamic_slice_in_dim(vector_sums_all, device_place * row_part, row_part, 1)
    qkv_rows = after(qkv_rows, own_sums)
    qkv_columns = lax.all_to_all(qkv_rows, "heads", split_axis=0, concat_axis=0, tiled=True)
    qkv_weight_grads = (
        qkv_columns.reshape(head_ways, row_part, group_pairs, 3, PAIR)
        .transpose(3, 1, 0, 2, 4)
        .reshape(3, row_part, width)
        .astype(jnp.float32)
    )
    out_weight_grad = lax.psum_scatter(
        lax.psum_scatter(
            out_weight_part.astype(jnp.bfloat16),
            ("fsdp", "heads"),
            scatter_dimension=0,
            tiled=True,
        ),
        "tensor",
        scatter_dimension=0,
        tiled=True,
    ).astype(jnp.float32)
    attn_sums = tuple(qkv_weight_grads) + (out_weight_grad,) + tuple(own_sums)
    return (
        output,
        input_grad,
        attn_sums[4],
        attn_sums[5],
        attn_sums[0],
        attn_sums[6],
        attn_sums[1],
        attn_sums[2],
        attn_sums[7],
        attn_sums[3],
        attn_sums[8],
        attn_sums[9],
        attn_sums[10],
        gate_weight_grad,
        gate_bias_grad,
        up_weight_grad,
        up_bias_grad,
        inner_gain_grad,
        inner_shift_grad,
        down_weight_grad,
        attn_sums[11],
    )


def solution(mesh):
    return jax.shard_map(
        on_device,
        mesh=mesh,
        in_specs=(
            P(("fsdp", "tensor"), "heads", None),
            P(("fsdp", "tensor")),
            P(("fsdp", "tensor"), "heads", None),
            P(("fsdp", "heads", "tensor")),
            P(("fsdp", "heads", "tensor")),
            P(("fsdp", "heads", "tensor"), None),
            P(("fsdp", "heads", "tensor")),
            P(("fsdp", "heads", "tensor"), None),
            P(("fsdp", "heads", "tensor"), None),
            P(("fsdp", "heads", "tensor")),
            P(("fsdp", "heads", "tensor"), None),
            P(("fsdp", "heads", "tensor")),
            P(("fsdp", "heads", "tensor")),
            P(("fsdp", "heads", "tensor")),
            P(("fsdp", "heads"), "tensor"),
            P("tensor"),
            P(("fsdp", "heads"), "tensor"),
            P("tensor"),
            P("tensor"),
            P("tensor"),
            P("tensor", ("fsdp", "heads")),
            P(("fsdp", "heads", "tensor")),
        ),
        out_specs=(
            P(("fsdp", "tensor"), "heads", None),
            P(("fsdp", "tensor"), "heads", None),
            P(("fsdp", "heads", "tensor")),
            P(("fsdp", "heads", "tensor")),
            P(("fsdp", "heads", "tensor"), None),
            P(("fsdp", "heads", "tensor")),
            P(("fsdp", "heads", "tensor"), None),
            P(("fsdp", "heads", "tensor"), None),
            P(("fsdp", "heads", "tensor")),
            P(("fsdp", "heads", "tensor"), None),
            P(("fsdp", "heads", "tensor")),
            P(("fsdp", "heads", "tensor")),
            P(("fsdp", "heads", "tensor")),
            P(("fsdp", "heads"), "tensor"),
            P("tensor"),
            P(("fsdp", "heads"), "tensor"),
            P("tensor"),
            P("tensor"),
            P("tensor"),
            P("tensor", ("fsdp", "heads")),
            P(("fsdp", "heads", "tensor")),
        ),
        check_vma=False,
    )
```

```python
import math

import jax
import jax.numpy as jnp
from jax import lax
from jax.experimental import pallas as pl
from jax.experimental.pallas import tpu as pltpu
from jax.sharding import PartitionSpec as P

HD = 64
PAIR = 2 * HD
FF_REAL = 2730
GRID = 32


norm_eps = 1e-06


def layer_norm(values, gain_vec, shift_vec):
    row_mean = jnp.mean(values, axis=-1, keepdims=True)
    centered = values - row_mean
    row_var = jnp.mean(centered * centered, axis=-1, keepdims=True)
    inv_std = lax.rsqrt(row_var + norm_eps)
    unit_rows = centered * inv_std
    return (unit_rows * gain_vec + shift_vec, unit_rows, inv_std)


def norm_backward(grad_values, unit_rows, inv_std, gain_vec):
    scaled = grad_values * gain_vec
    centered = scaled - jnp.mean(scaled, axis=-1, keepdims=True)
    centered = centered - unit_rows * jnp.mean(scaled * unit_rows, axis=-1, keepdims=True)
    return centered * inv_std


def rope_tables():
    positions = jnp.arange(GRID * GRID, dtype=jnp.int32)
    row_place = (positions // GRID).astype(jnp.float32)
    col_place = (positions % GRID).astype(jnp.float32)
    quarter = HD // 4
    frequency = jnp.power(10000.0, -jnp.arange(quarter, dtype=jnp.float32) / quarter)
    angles = jnp.concatenate(
        [row_place[:, None] * frequency[None, :], col_place[:, None] * frequency[None, :]], axis=1
    )
    angles = jnp.repeat(angles, 2, axis=1)
    return (jnp.cos(angles), jnp.sin(angles))


def pair_swap(values):
    count = values.shape[-1]
    lanes = lax.broadcasted_iota(jnp.int32, values.shape, 1)
    following = pltpu.roll(values, count - 1, 1)
    preceding = pltpu.roll(values, 1, 1)
    return jnp.where(lanes % 2 == 0, -following, preceding)


def rotate(values, cosine_table, sine_table):
    return values * cosine_table + pair_swap(values) * sine_table


def rotate_back(grad_values, cosine_table, sine_table):
    return grad_values * cosine_table - pair_swap(grad_values * sine_table)


def outer_product(left_rows, right_rows):
    return lax.dot_general(
        left_rows, right_rows, (((0,), (0,)), ((), ())), preferred_element_type=jnp.float32
    )


def times_transpose(left_rows, right_rows):
    return lax.dot_general(
        left_rows, right_rows, (((1,), (1,)), ((), ())), preferred_element_type=jnp.float32
    )


def gather_rows(block_values):
    return lax.all_gather(block_values, "tensor", axis=0, tiled=True)


def tensor_sums(first_sum, second_sum):
    both = lax.psum(jnp.stack([first_sum, second_sum]).astype(jnp.bfloat16), "tensor")
    return (both[0].astype(jnp.float32), both[1].astype(jnp.float32))


def cube_pairs(ways, bit):
    return [(place, place ^ (1 << bit)) for place in range(ways)]


def cube_gather(block, axis_name):
    ways = lax.axis_size(axis_name)
    bits = ways.bit_length() - 1
    index = lax.axis_index(axis_name)
    held = block.reshape((1,) * bits + block.shape)
    for bit in reversed(range(bits)):
        place = bits - 1 - bit
        other = lax.ppermute(held, axis_name, cube_pairs(ways, bit))
        held = jnp.where(
            (index >> bit) % 2 == 0,
            jnp.concatenate([held, other], axis=place),
            jnp.concatenate([other, held], axis=place),
        )
    return held.reshape((ways * block.shape[0],) + block.shape[1:])


def cube_scatter(terms, axis_name):
    ways = lax.axis_size(axis_name)
    bits = ways.bit_length() - 1
    index = lax.axis_index(axis_name)
    held = terms.reshape((2,) * bits + terms.shape[1:])
    for bit in range(bits):
        place = bits - 1 - bit
        mine = (index >> bit) % 2
        kept = lax.dynamic_index_in_dim(held, mine, place, keepdims=False)
        sent = lax.dynamic_index_in_dim(held, 1 - mine, place, keepdims=False)
        other = lax.ppermute(sent.astype(jnp.bfloat16), axis_name, cube_pairs(ways, bit))
        held = kept.astype(jnp.float32) + other.astype(jnp.float32)
    return held


def line_pairs(ways):
    upward = [(place, place + 1) for place in range(ways - 1)]
    return (upward, [(target, source) for source, target in upward])


def line_step(below, above, axis_name):
    upward, downward = line_pairs(lax.axis_size(axis_name))
    below.append(lax.ppermute(below[-1], axis_name, upward))
    above.append(lax.ppermute(above[-1], axis_name, downward))


def line_pick(below, above, axis_name):
    ways = lax.axis_size(axis_name)
    block = below[0]
    around = jnp.stack(below[:0:-1] + [block] + above[1:])
    picked = lax.dynamic_slice_in_dim(around, ways - 1 - lax.axis_index(axis_name), ways, 0)
    return picked.reshape((ways * block.shape[0],) + block.shape[1:])


def after(value, *others):
    return lax.optimization_barrier((value,) + others)[0]


def line_scatter(terms, axis_name, gates):
    ways = lax.axis_size(axis_name)
    pairs = line_pairs(ways)
    index = lax.axis_index(axis_name)

    def term(offset):
        place = jnp.clip(index + offset, 0, ways - 1)
        return lax.dynamic_index_in_dim(terms, place, 0, keepdims=False).astype(jnp.float32)

    running = [None, None]
    for step, distance in enumerate(range(ways - 1, 0, -1)):
        for side, sign in ((0, 1), (1, -1)):
            total = term(sign * distance)
            if step > 0:
                total = total + running[side].astype(jnp.float32)
            gated = after(total.astype(jnp.bfloat16), gates[min(step, len(gates) - 1)])
            running[side] = lax.ppermute(gated, axis_name, pairs[side])
    return term(0) + running[0].astype(jnp.float32) + running[1].astype(jnp.float32)


def scatter_rows(term_fn, row_total):
    return lax.psum_scatter(
        term_fn(jnp.int32(0), row_total * lax.axis_size("tensor")).astype(jnp.bfloat16),
        "tensor",
        scatter_dimension=0,
        tiled=True,
    ).astype(jnp.float32)


def head_masks(axis):
    shape = (1, PAIR) if axis == 1 else (PAIR, 1)
    place = lax.broadcasted_iota(jnp.int32, shape, axis)
    first = (place < HD).astype(jnp.float32)
    return (first, 1.0 - first)


def load_heads(qkv_ref, cosine_ref, sine_ref, query_s, key_s, value_s):
    rows = qkv_ref[...].reshape(query_s.shape[0], 3 * PAIR)
    cosine, sine = cosine_ref[...], sine_ref[...]
    query_rot = rotate(rows[:, :PAIR].astype(jnp.float32), cosine, sine).astype(jnp.bfloat16)
    query_s[...] = (query_rot.astype(jnp.float32) * (1.0 / math.sqrt(HD))).astype(jnp.bfloat16)
    key_rot = rotate(rows[:, PAIR : 2 * PAIR].astype(jnp.float32), cosine, sine)
    key_s[...] = key_rot.astype(jnp.bfloat16)
    value_s[...] = rows[:, 2 * PAIR :]


def forward_kernel(qkv_ref, cosine_ref, sine_ref, mixed_ref, query_s, key_s, value_s):
    load_heads(qkv_ref, cosine_ref, sine_ref, query_s, key_s, value_s)
    pieces, _, piece_len, _ = mixed_ref.shape
    masks = head_masks(1)

    def one_piece(piece, carry):
        start = pl.multiple_of(piece * piece_len, piece_len)
        query_rows = query_s[pl.ds(start, piece_len), :]
        mixed = jnp.zeros((piece_len, PAIR), jnp.float32)
        for mask in masks:
            own_query = query_rows * mask.astype(jnp.bfloat16)
            scores = times_transpose(own_query, key_s[...])
            weights_exp = jnp.exp(scores - jnp.max(scores, axis=-1, keepdims=True))
            inverse = 1.0 / jnp.sum(weights_exp, axis=-1, keepdims=True)
            probs_low = (weights_exp * inverse).astype(jnp.bfloat16)
            part = jnp.dot(probs_low, value_s[...], preferred_element_type=jnp.float32)
            mixed = mixed + part * mask
        mixed_ref[piece, 0] = mixed.astype(jnp.bfloat16)
        return carry

    lax.fori_loop(0, pieces, one_piece, 0)


def backward_kernel(
    qkv_ref, grad_ref, cosine_ref, sine_ref, out_ref,
    query_s, key_s, value_s, turned_s, key_grad_s, value_grad_s,
):
    load_heads(qkv_ref, cosine_ref, sine_ref, query_s, key_s, value_s)
    pieces, _, piece_len, _ = grad_ref.shape
    turned_s[...] = key_s[...].astype(jnp.float32).T.astype(jnp.bfloat16)
    key_grad_s[...] = jnp.zeros_like(key_grad_s)
    value_grad_s[...] = jnp.zeros_like(value_grad_s)
    row_masks = head_masks(1)
    column_masks = head_masks(0)

    def one_piece(piece, carry):
        start = pl.multiple_of(piece * piece_len, piece_len)
        rows = pl.ds(start, piece_len)
        query_rows = query_s[rows, :]
        grad_rows = grad_ref[piece, 0]
        query_grad = jnp.zeros((PAIR, piece_len), jnp.float32)
        for mask, column_mask in zip(row_masks, column_masks):
            own_query = query_rows * mask.astype(jnp.bfloat16)
            own_grad = grad_rows * mask.astype(jnp.bfloat16)
            scores = times_transpose(key_s[...], own_query)
            weights_exp = jnp.exp(scores - jnp.max(scores, axis=0, keepdims=True))
            probs = weights_exp * (1.0 / jnp.sum(weights_exp, axis=0, keepdims=True))
            grad_probs = times_transpose(value_s[...], own_grad)
            row_dot = jnp.sum(grad_probs * probs, axis=0, keepdims=True)
            grad_scores = (probs * (grad_probs - row_dot)).astype(jnp.bfloat16)
            value_grad_s[...] += jnp.dot(
                probs.astype(jnp.bfloat16), own_grad, preferred_element_type=jnp.float32
            )
            key_grad_s[...] += jnp.dot(grad_scores, own_query, preferred_element_type=jnp.float32)
            own_turned = turned_s[...] * column_mask.astype(jnp.bfloat16)
            query_grad = query_grad + jnp.dot(
                own_turned, grad_scores, preferred_element_type=jnp.float32
            )
        query_grad = query_grad.T * (1.0 / math.sqrt(HD))
        turned = rotate_back(query_grad, cosine_ref[rows, :], sine_ref[rows, :])
        out_ref[piece, 0, :, :PAIR] = turned.astype(jnp.bfloat16)
        return carry

    lax.fori_loop(0, pieces, one_piece, 0)
    piece_shape = (pieces, 1, piece_len, PAIR)
    key_grad = rotate_back(key_grad_s[...], cosine_ref[...], sine_ref[...])
    out_ref[:, :, :, PAIR : 2 * PAIR] = key_grad.astype(jnp.bfloat16).reshape(piece_shape)
    out_ref[:, :, :, 2 * PAIR :] = value_grad_s[...].astype(jnp.bfloat16).reshape(piece_shape)


def attention_call(kernel, name, qkv, extra, tables, out_lanes, more_scratch, products):
    pieces, seq_count, piece_len, lanes = qkv.shape
    pair_count = lanes // (3 * PAIR)
    length = pieces * piece_len

    def per_pair(wide):
        return pl.BlockSpec((pieces, 1, piece_len, wide), lambda seq, pair: (0, seq, 0, pair))

    table_spec = pl.BlockSpec((length, PAIR), lambda seq, pair: (0, 0))
    blocks = seq_count * pair_count
    return pl.pallas_call(
        kernel,
        name=name,
        grid=(seq_count, pair_count),
        in_specs=[per_pair(3 * PAIR)] + [per_pair(PAIR)] * len(extra) + [table_spec] * 2,
        out_specs=per_pair(out_lanes),
        out_shape=jax.ShapeDtypeStruct(
            (pieces, seq_count, piece_len, pair_count * out_lanes), jnp.bfloat16
        ),
        scratch_shapes=[pltpu.VMEM((length, PAIR), jnp.bfloat16)] * 3 + more_scratch,
        compiler_params=pltpu.CompilerParams(vmem_limit_bytes=48 << 20),
        cost_estimate=pl.CostEstimate(
            flops=blocks * products * 4 * length * length * PAIR,
            bytes_accessed=blocks * length * PAIR * 16,
            transcendentals=blocks * 2 * length * length,
        ),
    )(qkv, *extra, *tables)


def attend_forward(qkv, tables):
    return attention_call(forward_kernel, "attend_forward", qkv, (), tables, PAIR, [], 2)


def attend_backward(qkv, grad_mixed, tables):
    length = qkv.shape[0] * qkv.shape[2]
    more = [
        pltpu.VMEM((PAIR, length), jnp.bfloat16),
        pltpu.VMEM((length, PAIR), jnp.float32),
        pltpu.VMEM((length, PAIR), jnp.float32),
    ]
    return attention_call(
        backward_kernel, "attend_backward", qkv, (grad_mixed,), tables, 3 * PAIR, more, 5
    )


def hidden_forward(token_rows, gate_part, up_part, gate_shift, up_shift, unit_mask):
    gate_pre = jnp.dot(token_rows, gate_part, preferred_element_type=jnp.float32) + gate_shift
    up_pre = jnp.dot(token_rows, up_part, preferred_element_type=jnp.float32) + up_shift
    return (gate_pre, up_pre, jax.nn.silu(gate_pre) * up_pre * unit_mask)


def inner_normalize(hidden, first_sum, second_sum, inner_scale, inner_offset, unit_mask):
    unit_mean = first_sum[:, None] / FF_REAL
    unit_var = second_sum[:, None] / FF_REAL - unit_mean * unit_mean
    inv_std = lax.rsqrt(unit_var + norm_eps)
    unit_hidden = (hidden - unit_mean) * inv_std
    normed = ((unit_hidden * inner_scale + inner_offset) * unit_mask).astype(jnp.bfloat16)
    return (normed, unit_hidden, inv_std)


def hidden_backward_terms(grad_normed, unit_hidden, inner_scale, unit_mask):
    scaled = grad_normed * unit_mask * inner_scale
    return (scaled, jnp.sum(scaled, axis=-1), jnp.sum(scaled * unit_hidden, axis=-1))


def gate_grads(scaled, scaled_sum, cross_sum, unit_hidden, inv_std, gate_pre, up_pre, unit_mask):
    grad_hidden = (
        unit_mask
        * (scaled - scaled_sum[:, None] / FF_REAL - unit_hidden * cross_sum[:, None] / FF_REAL)
        * inv_std
    )
    sigmoid_gate = jax.nn.sigmoid(gate_pre)
    grad_gate = (
        grad_hidden * up_pre * sigmoid_gate * (1.0 + gate_pre * (1.0 - sigmoid_gate))
    ).astype(jnp.bfloat16)
    grad_up = (grad_hidden * gate_pre * sigmoid_gate).astype(jnp.bfloat16)
    return (grad_gate, grad_up)


def vector_sums(grad_gate, grad_up, grad_normed, unit_hidden, unit_mask):
    return (
        jnp.sum(grad_gate, axis=0, dtype=jnp.float32),
        jnp.sum(grad_up, axis=0, dtype=jnp.float32),
        jnp.sum(grad_normed * unit_mask * unit_hidden, axis=0),
        jnp.sum(grad_normed * unit_mask, axis=0),
    )


def on_device(
    inputs,
    slot_flag,
    cotangent,
    first_gain,
    first_shift,
    query_weight,
    query_bias,
    key_weight,
    value_weight,
    value_bias,
    out_weight,
    out_bias,
    second_gain,
    second_shift,
    gate_weight,
    gate_bias,
    up_weight,
    up_bias,
    inner_gain,
    inner_shift,
    down_weight,
    down_bias,
):
    seq_local, piece_len, width = inputs.shape
    head_ways = lax.axis_size("heads")
    seq_len = piece_len * head_ways
    group_width = width // head_ways
    group_pairs = group_width // PAIR
    token_count = seq_local * piece_len
    fsdp_ways, tensor_ways = lax.axis_size("fsdp"), lax.axis_size("tensor")
    row_part = query_weight.shape[0]
    group_index = lax.axis_index("heads")
    inputs_group = cube_gather(inputs, "heads")
    grad_flags = slot_flag.astype(jnp.float32)[:, None, None]
    grad_total = grad_flags * cotangent.astype(jnp.float32)
    grad_branch = grad_total.astype(jnp.bfloat16)
    stacked = jnp.stack(
        [
            member.reshape(row_part, head_ways, group_pairs, PAIR)
            for member in (query_weight, key_weight, value_weight)
        ],
        axis=3,
    ).reshape(row_part, head_ways, 3 * group_width)
    vectors = jnp.concatenate(
        [
            first_gain,
            first_shift,
            query_bias,
            value_bias,
            out_bias,
            second_gain,
            second_shift,
            down_bias,
        ]
    )
    vector_row = jnp.pad(vectors, (0, 3 * group_width - vectors.shape[0]))
    sent_columns = jnp.concatenate(
        [
            stacked.transpose(1, 0, 2),
            jnp.broadcast_to(vector_row, (head_ways, 1, 3 * group_width)),
        ],
        axis=1,
    )
    own_columns = lax.all_to_all(
        sent_columns, "heads", split_axis=0, concat_axis=0, tiled=True
    )
    columns = lax.all_gather(
        own_columns.reshape(-1, 3 * group_width), ("fsdp", "tensor"), axis=0, tiled=True
    )
    columns = columns.reshape(
        fsdp_ways, tensor_ways, head_ways, row_part + 1, 3 * group_width
    ).transpose(0, 2, 1, 3, 4)
    qkv_part = columns[:, :, :, :row_part].reshape(width, 3 * group_width)
    gated_branch = after(grad_branch, columns)
    below, above = [gated_branch], [gated_branch]
    line_step(below, above, "tensor")
    gathered = (
        columns[:, :, :, row_part, : vectors.shape[0]]
        .reshape(-1, 8, row_part)
        .transpose(1, 0, 2)
        .reshape(8, width)
    )
    out_full = lax.all_gather(
        lax.all_gather(out_weight, "tensor", axis=0, tiled=True),
        ("fsdp", "heads"),
        axis=0,
        tiled=True,
    )
    gain_one, shift_one, query_shift, value_shift, out_shift, gain_two, shift_two, down_shift = [
        member.astype(jnp.float32) for member in gathered
    ]
    gate_part, up_part, down_part = (
        lax.all_gather(gate_weight, ("fsdp", "heads"), axis=0, tiled=True),
        lax.all_gather(up_weight, ("fsdp", "heads"), axis=0, tiled=True),
        lax.all_gather(down_weight, ("fsdp", "heads"), axis=1, tiled=True),
    )
    inputs_f = inputs.astype(jnp.float32)
    _, unit_one, inv_one = layer_norm(inputs_f, gain_one, shift_one)
    normed_group, _, _ = layer_norm(
        inputs_group.reshape(-1, width).astype(jnp.float32), gain_one, shift_one
    )
    low_one = normed_group.astype(jnp.bfloat16)

    def group_lanes(full_vec):
        own = lax.dynamic_slice_in_dim(full_vec, group_index * group_width, group_width, 0)
        return own.reshape(group_pairs, PAIR)

    query_lanes, value_lanes = group_lanes(query_shift), group_lanes(value_shift)
    qkv_shift = jnp.stack([query_lanes, jnp.zeros_like(query_lanes), value_lanes], axis=1)
    qkv_lin = (
        (jnp.dot(low_one, qkv_part, preferred_element_type=jnp.float32) + qkv_shift.reshape(-1))
        .astype(jnp.bfloat16)
        .reshape(head_ways, seq_local, piece_len, 3 * group_width)
    )
    tables = tuple(jnp.tile(table, (1, PAIR // HD)) for table in rope_tables())
    attended = after(qkv_lin, below[-1], above[-1])
    for _ in range(tensor_ways - 3):
        line_step(below, above, "tensor")
    mixed_heads = attend_forward(attended, tables)
    below[-1], above[-1] = after(below[-1], mixed_heads), after(above[-1], mixed_heads)
    line_step(below, above, "tensor")
    mixed_parts = lax.all_to_all(mixed_heads, "heads", split_axis=0, concat_axis=0, tiled=True)
    grad_rows = line_pick(below, above, "tensor").reshape(-1, width)
    mixed_flat = mixed_parts.transpose(1, 2, 0, 3).reshape(token_count, width)
    residual = inputs_f + (
        jnp.dot(mixed_flat, out_full, preferred_element_type=jnp.float32) + out_shift
    ).reshape(inputs.shape)
    normed_two, unit_two, inv_two = layer_norm(residual, gain_two, shift_two)
    low_two = normed_two.astype(jnp.bfloat16)
    flag_rows = slot_flag.astype(jnp.float32)[:, None, None]
    down_shift_grad = jnp.sum(grad_branch.reshape(token_count, width), axis=0, dtype=jnp.float32)
    ffn_local = gate_part.shape[1]
    token_rows3 = gather_rows(after(low_two, gate_part, up_part, below[-1], above[-1]))
    token_rows = token_rows3.reshape(-1, width)
    col_index = lax.axis_index("tensor") * ffn_local + jnp.arange(ffn_local, dtype=jnp.int32)
    unit_mask = (col_index < FF_REAL).astype(jnp.float32)
    gate_pre, up_pre, hidden = hidden_forward(
        token_rows,
        gate_part,
        up_part,
        gate_bias.astype(jnp.float32),
        up_bias.astype(jnp.float32),
        unit_mask,
    )
    first_sum, second_sum = tensor_sums(jnp.sum(hidden, axis=-1), jnp.sum(hidden * hidden, axis=-1))
    inner_scale = inner_gain.astype(jnp.float32)
    normed_hidden, unit_hidden, inv_hidden = inner_normalize(
        hidden, first_sum, second_sum, inner_scale, inner_shift.astype(jnp.float32), unit_mask
    )
    hidden_seqs = normed_hidden.reshape(token_rows3.shape[0], piece_len, ffn_local)

    def down_term(row_start, row_count):
        picked = hidden_seqs.reshape(-1, ffn_local)
        return jnp.dot(picked, down_part, preferred_element_type=jnp.float32).reshape(
            row_count, piece_len, width
        )

    down_grad = outer_product(normed_hidden, grad_rows)
    down_weight_grad = lax.psum_scatter(
        down_grad.astype(jnp.bfloat16), ("fsdp", "heads"), scatter_dimension=1, tiled=True
    )
    grad_normed = times_transpose(after(grad_rows, down_grad), down_part)
    scaled, scaled_sum, cross_sum = hidden_backward_terms(
        grad_normed, unit_hidden, inner_scale, unit_mask
    )
    scaled_sum, cross_sum = tensor_sums(scaled_sum, cross_sum)
    grad_gate, grad_up = gate_grads(
        scaled, scaled_sum, cross_sum, unit_hidden, inv_hidden, gate_pre, up_pre, unit_mask
    )
    gate_grad = outer_product(token_rows, grad_gate)
    up_grad = outer_product(token_rows, grad_up)
    vector_grads = vector_sums(grad_gate, grad_up, grad_normed, unit_hidden, unit_mask)
    gate_seqs = after(grad_gate, down_weight_grad).reshape(-1, piece_len, ffn_local)
    up_seqs = grad_up.reshape(-1, piece_len, ffn_local)

    def input_term(row_start, row_count):
        picked_gate = gate_seqs.reshape(-1, ffn_local)
        picked_up = up_seqs.reshape(-1, ffn_local)
        summed = times_transpose(picked_gate, gate_part) + times_transpose(picked_up, up_part)
        return summed.reshape(row_count, piece_len, width)

    grad_normed_two = scatter_rows(input_term, seq_local)
    gate_weight_grad, up_weight_grad = (
        lax.psum_scatter(
            gate_grad.astype(jnp.bfloat16), ("fsdp", "heads"), scatter_dimension=0, tiled=True
        ).astype(jnp.float32),
        lax.psum_scatter(
            up_grad.astype(jnp.bfloat16), ("fsdp", "heads"), scatter_dimension=0, tiled=True
        ).astype(jnp.float32),
    )
    down_weight_grad = down_weight_grad.astype(jnp.float32)
    gate_bias_grad, up_bias_grad, inner_gain_grad, inner_shift_grad = lax.psum(
        (vector_grads[0], vector_grads[1], vector_grads[2], vector_grads[3]), ("fsdp", "heads")
    )
    grad_normed_two = after(grad_normed_two, gate_bias_grad)
    grad_residual = grad_total + norm_backward(grad_normed_two, unit_two, inv_two, gain_two)
    gain_two_grad = jnp.sum((grad_normed_two * unit_two).reshape(token_count, width), axis=0)
    shift_two_grad = jnp.sum(grad_normed_two.reshape(token_count, width), axis=0)
    grad_attn = grad_residual.astype(jnp.bfloat16).reshape(token_count, width)
    out_weight_part = outer_product(mixed_flat, grad_attn)
    out_shift_grad = jnp.sum(grad_attn, axis=0, dtype=jnp.float32)
    grad_mixed = times_transpose(grad_attn, out_full).astype(jnp.bfloat16)
    grad_parts = grad_mixed.reshape(seq_local, piece_len, head_ways, group_width)
    grad_heads = lax.all_to_all(
        grad_parts.transpose(2, 0, 1, 3), "heads", split_axis=0, concat_axis=0, tiled=True
    )
    qkv_grad = attend_backward(qkv_lin, grad_heads, tables)
    branch_terms = down_term(0, seq_local * tensor_ways).astype(jnp.bfloat16)
    branch_out = line_scatter(
        branch_terms.reshape((tensor_ways,) + inputs.shape),
        "tensor",
        (grad_mixed, grad_heads, qkv_grad),
    )
    output = (flag_rows * (residual + branch_out + down_shift)).astype(jnp.bfloat16)
    qkv_grad = qkv_grad.reshape(head_ways * token_count, 3 * group_width)
    group_terms = times_transpose(qkv_grad, qkv_part).astype(jnp.bfloat16)
    grad_normed_one = cube_scatter(
        group_terms.reshape((head_ways,) + inputs.shape), "heads"
    )
    qkv_shift_grad = jnp.sum(qkv_grad, axis=0, dtype=jnp.float32).reshape(group_pairs, 3, PAIR)

    def place_lanes(own_lanes):
        return lax.dynamic_update_slice_in_dim(
            jnp.zeros((width,), jnp.float32), own_lanes.reshape(-1), group_index * group_width, 0
        )

    query_shift_grad = place_lanes(qkv_shift_grad[:, 0])
    value_shift_grad = place_lanes(qkv_shift_grad[:, 2])
    input_grad = (
        grad_residual + norm_backward(grad_normed_one, unit_one, inv_one, gain_one)
    ).astype(jnp.bfloat16)
    gain_one_grad = jnp.sum((grad_normed_one * unit_one).reshape(token_count, width), axis=0)
    shift_one_grad = jnp.sum(grad_normed_one.reshape(token_count, width), axis=0)
    vector_terms = jnp.stack(
        [
            gain_one_grad,
            shift_one_grad,
            query_shift_grad,
            value_shift_grad,
            out_shift_grad,
            gain_two_grad,
            shift_two_grad,
            down_shift_grad,
        ]
    )
    vector_lanes = vector_terms.shape[0] * row_part
    vector_rows = (
        vector_terms.reshape(-1, fsdp_ways, head_ways, tensor_ways, row_part)
        .transpose(1, 3, 2, 0, 4)
        .reshape(fsdp_ways, tensor_ways, head_ways, 1, vector_lanes)
    )
    extra_rows = 1
    while head_ways * (row_part + extra_rows) % 16 != 0:
        extra_rows += 1
    vector_rows = jnp.pad(
        vector_rows,
        ((0, 0),) * 3 + ((0, extra_rows - 1), (0, 3 * group_width - vector_lanes)),
    )
    qkv_terms = outer_product(low_one, qkv_grad).astype(jnp.bfloat16)
    qkv_terms = qkv_terms.reshape(
        fsdp_ways, head_ways, tensor_ways, row_part, 3 * group_width
    ).transpose(0, 2, 1, 3, 4)
    qkv_terms = jnp.concatenate([qkv_terms, vector_rows.astype(jnp.bfloat16)], axis=3)
    qkv_half = cube_scatter(
        qkv_terms.reshape(fsdp_ways, -1, 3 * group_width), "fsdp"
    ).astype(jnp.bfloat16)
    qkv_rows = lax.psum_scatter(qkv_half, "tensor", scatter_dimension=0, tiled=True)
    qkv_columns = lax.all_to_all(
        qkv_rows, "heads", split_axis=0, concat_axis=0, tiled=True
    ).reshape(head_ways, row_part + extra_rows, 3 * group_width)
    qkv_weight_grads = (
        qkv_columns[:, :row_part]
        .reshape(head_ways, row_part, group_pairs, 3, PAIR)
        .transpose(3, 1, 0, 2, 4)
        .reshape(3, row_part, width)
        .astype(jnp.float32)
    )
    own_sums = jnp.sum(
        qkv_columns[:, row_part, :vector_lanes].astype(jnp.float32), axis=0
    ).reshape(-1, row_part)
    out_terms = out_weight_part.astype(jnp.bfloat16).reshape(fsdp_ways, -1, width)
    out_half = cube_scatter(out_terms, "fsdp").astype(jnp.bfloat16)
    out_eighth = cube_scatter(out_half.reshape(head_ways, -1, width), "heads")
    out_weight_grad = lax.psum_scatter(
        out_eighth.astype(jnp.bfloat16), "tensor", scatter_dimension=0, tiled=True
    ).astype(jnp.float32)
    attn_sums = tuple(qkv_weight_grads) + (out_weight_grad,) + tuple(own_sums)
    return (
        output,
        input_grad,
        attn_sums[4],
        attn_sums[5],
        attn_sums[0],
        attn_sums[6],
        attn_sums[1],
        attn_sums[2],
        attn_sums[7],
        attn_sums[3],
        attn_sums[8],
        attn_sums[9],
        attn_sums[10],
        gate_weight_grad,
        gate_bias_grad,
        up_weight_grad,
        up_bias_grad,
        inner_gain_grad,
        inner_shift_grad,
        down_weight_grad,
        attn_sums[11],
    )


def solution(mesh):
    return jax.shard_map(
        on_device,
        mesh=mesh,
        in_specs=(
            P(("fsdp", "tensor"), "heads", None),
            P(("fsdp", "tensor")),
            P(("fsdp", "tensor"), "heads", None),
            P(("fsdp", "heads", "tensor")),
            P(("fsdp", "heads", "tensor")),
            P(("fsdp", "heads", "tensor"), None),
            P(("fsdp", "heads", "tensor")),
            P(("fsdp", "heads", "tensor"), None),
            P(("fsdp", "heads", "tensor"), None),
            P(("fsdp", "heads", "tensor")),
            P(("fsdp", "heads", "tensor"), None),
            P(("fsdp", "heads", "tensor")),
            P(("fsdp", "heads", "tensor")),
            P(("fsdp", "heads", "tensor")),
            P(("fsdp", "heads"), "tensor"),
            P("tensor"),
            P(("fsdp", "heads"), "tensor"),
            P("tensor"),
            P("tensor"),
            P("tensor"),
            P("tensor", ("fsdp", "heads")),
            P(("fsdp", "heads", "tensor")),
        ),
        out_specs=(
            P(("fsdp", "tensor"), "heads", None),
            P(("fsdp", "tensor"), "heads", None),
            P(("fsdp", "heads", "tensor")),
            P(("fsdp", "heads", "tensor")),
            P(("fsdp", "heads", "tensor"), None),
            P(("fsdp", "heads", "tensor")),
            P(("fsdp", "heads", "tensor"), None),
            P(("fsdp", "heads", "tensor"), None),
            P(("fsdp", "heads", "tensor")),
            P(("fsdp", "heads", "tensor"), None),
            P(("fsdp", "heads", "tensor")),
            P(("fsdp", "heads", "tensor")),
            P(("fsdp", "heads", "tensor")),
            P(("fsdp", "heads"), "tensor"),
            P("tensor"),
            P(("fsdp", "heads"), "tensor"),
            P("tensor"),
            P("tensor"),
            P("tensor"),
            P("tensor", ("fsdp", "heads")),
            P(("fsdp", "heads", "tensor")),
        ),
        check_vma=False,
    )
```

```python
import math

import jax
import jax.numpy as jnp
from jax import lax
from jax.experimental import pallas as pl
from jax.experimental.pallas import tpu as pltpu
from jax.sharding import PartitionSpec as P

HD = 64
PAIR = 2 * HD
FF_REAL = 2730
GRID = 32


norm_eps = 1e-06


def layer_norm(values, gain_vec, shift_vec):
    row_mean = jnp.mean(values, axis=-1, keepdims=True)
    centered = values - row_mean
    row_var = jnp.mean(centered * centered, axis=-1, keepdims=True)
    inv_std = lax.rsqrt(row_var + norm_eps)
    unit_rows = centered * inv_std
    return (unit_rows * gain_vec + shift_vec, unit_rows, inv_std)


def norm_backward(grad_values, unit_rows, inv_std, gain_vec):
    scaled = grad_values * gain_vec
    centered = scaled - jnp.mean(scaled, axis=-1, keepdims=True)
    centered = centered - unit_rows * jnp.mean(scaled * unit_rows, axis=-1, keepdims=True)
    return centered * inv_std


def rope_tables():
    positions = jnp.arange(GRID * GRID, dtype=jnp.int32)
    row_place = (positions // GRID).astype(jnp.float32)
    col_place = (positions % GRID).astype(jnp.float32)
    quarter = HD // 4
    frequency = jnp.power(10000.0, -jnp.arange(quarter, dtype=jnp.float32) / quarter)
    angles = jnp.concatenate(
        [row_place[:, None] * frequency[None, :], col_place[:, None] * frequency[None, :]], axis=1
    )
    angles = jnp.repeat(angles, 2, axis=1)
    return (jnp.cos(angles), jnp.sin(angles))


def pair_swap(values):
    count = values.shape[-1]
    lanes = lax.broadcasted_iota(jnp.int32, values.shape, 1)
    following = pltpu.roll(values, count - 1, 1)
    preceding = pltpu.roll(values, 1, 1)
    return jnp.where(lanes % 2 == 0, -following, preceding)


def rotate(values, cosine_table, sine_table):
    return values * cosine_table + pair_swap(values) * sine_table


def rotate_back(grad_values, cosine_table, sine_table):
    return grad_values * cosine_table - pair_swap(grad_values * sine_table)


def outer_product(left_rows, right_rows):
    return lax.dot_general(
        left_rows, right_rows, (((0,), (0,)), ((), ())), preferred_element_type=jnp.float32
    )


def times_transpose(left_rows, right_rows):
    return lax.dot_general(
        left_rows, right_rows, (((1,), (1,)), ((), ())), preferred_element_type=jnp.float32
    )


def gather_rows(block_values):
    return lax.all_gather(block_values, "tensor", axis=0, tiled=True)


def tensor_sums(first_sum, second_sum):
    both = lax.psum(jnp.stack([first_sum, second_sum]).astype(jnp.bfloat16), "tensor")
    return (both[0].astype(jnp.float32), both[1].astype(jnp.float32))


def cube_pairs(ways, bit):
    return [(place, place ^ (1 << bit)) for place in range(ways)]


def cube_gather(block, axis_name):
    ways = lax.axis_size(axis_name)
    bits = ways.bit_length() - 1
    index = lax.axis_index(axis_name)
    held = block.reshape((1,) * bits + block.shape)
    for bit in reversed(range(bits)):
        place = bits - 1 - bit
        other = lax.ppermute(held, axis_name, cube_pairs(ways, bit))
        held = jnp.where(
            (index >> bit) % 2 == 0,
            jnp.concatenate([held, other], axis=place),
            jnp.concatenate([other, held], axis=place),
        )
    return held.reshape((ways * block.shape[0],) + block.shape[1:])


def cube_scatter(terms, axis_name):
    ways = lax.axis_size(axis_name)
    bits = ways.bit_length() - 1
    index = lax.axis_index(axis_name)
    held = terms.reshape((2,) * bits + terms.shape[1:])
    for bit in range(bits):
        place = bits - 1 - bit
        mine = (index >> bit) % 2
        kept = lax.dynamic_index_in_dim(held, mine, place, keepdims=False)
        sent = lax.dynamic_index_in_dim(held, 1 - mine, place, keepdims=False)
        other = lax.ppermute(sent.astype(jnp.bfloat16), axis_name, cube_pairs(ways, bit))
        held = kept.astype(jnp.float32) + other.astype(jnp.float32)
    return held


def line_pairs(ways):
    upward = [(place, place + 1) for place in range(ways - 1)]
    return (upward, [(target, source) for source, target in upward])


def line_step(below, above, axis_name):
    upward, downward = line_pairs(lax.axis_size(axis_name))
    below.append(lax.ppermute(below[-1], axis_name, upward))
    above.append(lax.ppermute(above[-1], axis_name, downward))


def line_pick(below, above, axis_name):
    ways = lax.axis_size(axis_name)
    block = below[0]
    around = jnp.stack(below[:0:-1] + [block] + above[1:])
    picked = lax.dynamic_slice_in_dim(around, ways - 1 - lax.axis_index(axis_name), ways, 0)
    return picked.reshape((ways * block.shape[0],) + block.shape[1:])


def after(value, *others):
    return lax.optimization_barrier((value,) + others)[0]


def line_term(terms, offset, axis_name):
    place = lax.axis_index(axis_name) + offset
    place = jnp.clip(place, 0, lax.axis_size(axis_name) - 1)
    return lax.dynamic_index_in_dim(terms, place, 0, keepdims=False).astype(jnp.float32)


def line_scatter_step(terms, running, distance, axis_name, gate):
    pairs = line_pairs(lax.axis_size(axis_name))
    passed = []
    for side, sign in ((0, 1), (1, -1)):
        total = line_term(terms, sign * distance, axis_name)
        if running is not None:
            total = total + running[side].astype(jnp.float32)
        gated = after(total.astype(jnp.bfloat16), gate)
        passed.append(lax.ppermute(gated, axis_name, pairs[side]))
    return passed


def scatter_rows(term_fn, row_total):
    return lax.psum_scatter(
        term_fn(jnp.int32(0), row_total * lax.axis_size("tensor")).astype(jnp.bfloat16),
        "tensor",
        scatter_dimension=0,
        tiled=True,
    ).astype(jnp.float32)


def head_masks(axis):
    shape = (1, PAIR) if axis == 1 else (PAIR, 1)
    place = lax.broadcasted_iota(jnp.int32, shape, axis)
    first = (place < HD).astype(jnp.float32)
    return (first, 1.0 - first)


def load_heads(qkv_ref, cosine_ref, sine_ref, query_s, key_s, value_s):
    rows = qkv_ref[...].reshape(query_s.shape[0], 3 * PAIR)
    cosine, sine = cosine_ref[...], sine_ref[...]
    query_rot = rotate(rows[:, :PAIR].astype(jnp.float32), cosine, sine).astype(jnp.bfloat16)
    query_s[...] = (query_rot.astype(jnp.float32) * (1.0 / math.sqrt(HD))).astype(jnp.bfloat16)
    key_rot = rotate(rows[:, PAIR : 2 * PAIR].astype(jnp.float32), cosine, sine)
    key_s[...] = key_rot.astype(jnp.bfloat16)
    value_s[...] = rows[:, 2 * PAIR :]


def forward_kernel(qkv_ref, cosine_ref, sine_ref, mixed_ref, query_s, key_s, value_s):
    load_heads(qkv_ref, cosine_ref, sine_ref, query_s, key_s, value_s)
    pieces, _, piece_len, _ = mixed_ref.shape
    masks = head_masks(1)

    def one_piece(piece, carry):
        start = pl.multiple_of(piece * piece_len, piece_len)
        query_rows = query_s[pl.ds(start, piece_len), :]
        mixed = jnp.zeros((piece_len, PAIR), jnp.float32)
        for mask in masks:
            own_query = query_rows * mask.astype(jnp.bfloat16)
            scores = times_transpose(own_query, key_s[...])
            weights_exp = jnp.exp(scores - jnp.max(scores, axis=-1, keepdims=True))
            inverse = 1.0 / jnp.sum(weights_exp, axis=-1, keepdims=True)
            probs_low = (weights_exp * inverse).astype(jnp.bfloat16)
            part = jnp.dot(probs_low, value_s[...], preferred_element_type=jnp.float32)
            mixed = mixed + part * mask
        mixed_ref[piece, 0] = mixed.astype(jnp.bfloat16)
        return carry

    lax.fori_loop(0, pieces, one_piece, 0)


def backward_kernel(
    qkv_ref, grad_ref, cosine_ref, sine_ref, out_ref,
    query_s, key_s, value_s, turned_s, key_grad_s, value_grad_s,
):
    load_heads(qkv_ref, cosine_ref, sine_ref, query_s, key_s, value_s)
    pieces, _, piece_len, _ = grad_ref.shape
    turned_s[...] = key_s[...].astype(jnp.float32).T.astype(jnp.bfloat16)
    key_grad_s[...] = jnp.zeros_like(key_grad_s)
    value_grad_s[...] = jnp.zeros_like(value_grad_s)
    row_masks = head_masks(1)
    column_masks = head_masks(0)

    def one_piece(piece, carry):
        start = pl.multiple_of(piece * piece_len, piece_len)
        rows = pl.ds(start, piece_len)
        query_rows = query_s[rows, :]
        grad_rows = grad_ref[piece, 0]
        query_grad = jnp.zeros((PAIR, piece_len), jnp.float32)
        for mask, column_mask in zip(row_masks, column_masks):
            own_query = query_rows * mask.astype(jnp.bfloat16)
            own_grad = grad_rows * mask.astype(jnp.bfloat16)
            scores = times_transpose(key_s[...], own_query)
            weights_exp = jnp.exp(scores - jnp.max(scores, axis=0, keepdims=True))
            probs = weights_exp * (1.0 / jnp.sum(weights_exp, axis=0, keepdims=True))
            grad_probs = times_transpose(value_s[...], own_grad)
            row_dot = jnp.sum(grad_probs * probs, axis=0, keepdims=True)
            grad_scores = (probs * (grad_probs - row_dot)).astype(jnp.bfloat16)
            value_grad_s[...] += jnp.dot(
                probs.astype(jnp.bfloat16), own_grad, preferred_element_type=jnp.float32
            )
            key_grad_s[...] += jnp.dot(grad_scores, own_query, preferred_element_type=jnp.float32)
            own_turned = turned_s[...] * column_mask.astype(jnp.bfloat16)
            query_grad = query_grad + jnp.dot(
                own_turned, grad_scores, preferred_element_type=jnp.float32
            )
        query_grad = query_grad.T * (1.0 / math.sqrt(HD))
        turned = rotate_back(query_grad, cosine_ref[rows, :], sine_ref[rows, :])
        out_ref[piece, 0, :, :PAIR] = turned.astype(jnp.bfloat16)
        return carry

    lax.fori_loop(0, pieces, one_piece, 0)
    piece_shape = (pieces, 1, piece_len, PAIR)
    key_grad = rotate_back(key_grad_s[...], cosine_ref[...], sine_ref[...])
    out_ref[:, :, :, PAIR : 2 * PAIR] = key_grad.astype(jnp.bfloat16).reshape(piece_shape)
    out_ref[:, :, :, 2 * PAIR :] = value_grad_s[...].astype(jnp.bfloat16).reshape(piece_shape)


def attention_call(kernel, name, qkv, extra, tables, out_lanes, more_scratch, products):
    pieces, seq_count, piece_len, lanes = qkv.shape
    pair_count = lanes // (3 * PAIR)
    length = pieces * piece_len

    def per_pair(wide):
        return pl.BlockSpec((pieces, 1, piece_len, wide), lambda seq, pair: (0, seq, 0, pair))

    table_spec = pl.BlockSpec((length, PAIR), lambda seq, pair: (0, 0))
    blocks = seq_count * pair_count
    return pl.pallas_call(
        kernel,
        name=name,
        grid=(seq_count, pair_count),
        in_specs=[per_pair(3 * PAIR)] + [per_pair(PAIR)] * len(extra) + [table_spec] * 2,
        out_specs=per_pair(out_lanes),
        out_shape=jax.ShapeDtypeStruct(
            (pieces, seq_count, piece_len, pair_count * out_lanes), jnp.bfloat16
        ),
        scratch_shapes=[pltpu.VMEM((length, PAIR), jnp.bfloat16)] * 3 + more_scratch,
        compiler_params=pltpu.CompilerParams(vmem_limit_bytes=48 << 20),
        cost_estimate=pl.CostEstimate(
            flops=blocks * products * 4 * length * length * PAIR,
            bytes_accessed=blocks * length * PAIR * 16,
            transcendentals=blocks * 2 * length * length,
        ),
    )(qkv, *extra, *tables)


def attend_forward(qkv, tables):
    return attention_call(forward_kernel, "attend_forward", qkv, (), tables, PAIR, [], 2)


def attend_backward(qkv, grad_mixed, tables):
    length = qkv.shape[0] * qkv.shape[2]
    more = [
        pltpu.VMEM((PAIR, length), jnp.bfloat16),
        pltpu.VMEM((length, PAIR), jnp.float32),
        pltpu.VMEM((length, PAIR), jnp.float32),
    ]
    return attention_call(
        backward_kernel, "attend_backward", qkv, (grad_mixed,), tables, 3 * PAIR, more, 5
    )


def hidden_forward(token_rows, gate_part, up_part, gate_shift, up_shift, unit_mask):
    gate_pre = jnp.dot(token_rows, gate_part, preferred_element_type=jnp.float32) + gate_shift
    up_pre = jnp.dot(token_rows, up_part, preferred_element_type=jnp.float32) + up_shift
    return (gate_pre, up_pre, jax.nn.silu(gate_pre) * up_pre * unit_mask)


def inner_normalize(hidden, first_sum, second_sum, inner_scale, inner_offset, unit_mask):
    unit_mean = first_sum[:, None] / FF_REAL
    unit_var = second_sum[:, None] / FF_REAL - unit_mean * unit_mean
    inv_std = lax.rsqrt(unit_var + norm_eps)
    unit_hidden = (hidden - unit_mean) * inv_std
    normed = ((unit_hidden * inner_scale + inner_offset) * unit_mask).astype(jnp.bfloat16)
    return (normed, unit_hidden, inv_std)


def hidden_backward_terms(grad_normed, unit_hidden, inner_scale, unit_mask):
    scaled = grad_normed * unit_mask * inner_scale
    return (scaled, jnp.sum(scaled, axis=-1), jnp.sum(scaled * unit_hidden, axis=-1))


def gate_grads(scaled, scaled_sum, cross_sum, unit_hidden, inv_std, gate_pre, up_pre, unit_mask):
    grad_hidden = (
        unit_mask
        * (scaled - scaled_sum[:, None] / FF_REAL - unit_hidden * cross_sum[:, None] / FF_REAL)
        * inv_std
    )
    sigmoid_gate = jax.nn.sigmoid(gate_pre)
    grad_gate = (
        grad_hidden * up_pre * sigmoid_gate * (1.0 + gate_pre * (1.0 - sigmoid_gate))
    ).astype(jnp.bfloat16)
    grad_up = (grad_hidden * gate_pre * sigmoid_gate).astype(jnp.bfloat16)
    return (grad_gate, grad_up)


def vector_sums(grad_gate, grad_up, grad_normed, unit_hidden, unit_mask):
    return (
        jnp.sum(grad_gate, axis=0, dtype=jnp.float32),
        jnp.sum(grad_up, axis=0, dtype=jnp.float32),
        jnp.sum(grad_normed * unit_mask * unit_hidden, axis=0),
        jnp.sum(grad_normed * unit_mask, axis=0),
    )


def on_device(
    inputs,
    slot_flag,
    cotangent,
    first_gain,
    first_shift,
    query_weight,
    query_bias,
    key_weight,
    value_weight,
    value_bias,
    out_weight,
    out_bias,
    second_gain,
    second_shift,
    gate_weight,
    gate_bias,
    up_weight,
    up_bias,
    inner_gain,
    inner_shift,
    down_weight,
    down_bias,
):
    seq_local, piece_len, width = inputs.shape
    head_ways = lax.axis_size("heads")
    seq_len = piece_len * head_ways
    group_width = width // head_ways
    group_pairs = group_width // PAIR
    token_count = seq_local * piece_len
    fsdp_ways, tensor_ways = lax.axis_size("fsdp"), lax.axis_size("tensor")
    row_part = query_weight.shape[0]
    group_index = lax.axis_index("heads")
    inputs_group = cube_gather(inputs, "heads")
    grad_flags = slot_flag.astype(jnp.float32)[:, None, None]
    grad_total = grad_flags * cotangent.astype(jnp.float32)
    grad_branch = grad_total.astype(jnp.bfloat16)
    stacked = jnp.stack(
        [
            member.reshape(row_part, head_ways, group_pairs, PAIR)
            for member in (query_weight, key_weight, value_weight)
        ],
        axis=3,
    ).reshape(row_part, head_ways, 3 * group_width)
    vectors = (
        first_gain,
        first_shift,
        query_bias,
        value_bias,
        out_bias,
        second_gain,
        second_shift,
        down_bias,
    )
    row_lanes = 3 * group_width
    vector_row = jnp.zeros((row_lanes,), jnp.float32)
    for place, member in enumerate(vectors):
        ahead = place * row_part
        vector_row = vector_row + jnp.pad(
            member.astype(jnp.float32), (ahead, row_lanes - ahead - row_part)
        )
    vector_row = vector_row.astype(jnp.bfloat16)
    sent_columns = jnp.concatenate(
        [
            stacked.transpose(1, 0, 2),
            jnp.broadcast_to(vector_row, (head_ways, 1, 3 * group_width)),
        ],
        axis=1,
    )
    own_columns = lax.all_to_all(
        sent_columns, "heads", split_axis=0, concat_axis=0, tiled=True
    )
    columns = lax.all_gather(
        own_columns.reshape(-1, 3 * group_width), ("fsdp", "tensor"), axis=0, tiled=True
    )
    group_f = inputs_group.reshape(-1, width).astype(jnp.float32)
    group_mean = jnp.mean(group_f, axis=-1, keepdims=True)
    group_var = jnp.mean(jnp.square(group_f - group_mean), axis=-1, keepdims=True)
    group_inv = lax.rsqrt(group_var + norm_eps)
    columns, group_mean, group_inv = lax.optimization_barrier((columns, group_mean, group_inv))
    columns = columns.reshape(
        fsdp_ways, tensor_ways, head_ways, row_part + 1, 3 * group_width
    ).transpose(0, 2, 1, 3, 4)
    qkv_part = columns[:, :, :, :row_part].reshape(width, 3 * group_width)
    gated_branch = after(grad_branch, columns)
    below, above = [gated_branch], [gated_branch]
    line_step(below, above, "tensor")
    gathered = (
        columns[:, :, :, row_part, : len(vectors) * row_part]
        .reshape(-1, 8, row_part)
        .transpose(1, 0, 2)
        .reshape(8, width)
    )
    out_full = lax.all_gather(
        lax.all_gather(out_weight, "tensor", axis=0, tiled=True),
        ("fsdp", "heads"),
        axis=0,
        tiled=True,
    )
    gain_one, shift_one, query_shift, value_shift, out_shift, gain_two, shift_two, down_shift = [
        member.astype(jnp.float32) for member in gathered
    ]
    gate_part, up_part, down_part = (
        lax.all_gather(gate_weight, ("fsdp", "heads"), axis=0, tiled=True),
        lax.all_gather(up_weight, ("fsdp", "heads"), axis=0, tiled=True),
        lax.all_gather(down_weight, ("fsdp", "heads"), axis=1, tiled=True),
    )
    inputs_f = inputs.astype(jnp.float32)
    _, unit_one, inv_one = layer_norm(inputs_f, gain_one, shift_one)
    unit_group = (group_f - group_mean) * group_inv
    low_one = (unit_group * gain_one + shift_one).astype(jnp.bfloat16)

    def group_lanes(full_vec):
        own = lax.dynamic_slice_in_dim(full_vec, group_index * group_width, group_width, 0)
        return own.reshape(group_pairs, PAIR)

    query_lanes, value_lanes = group_lanes(query_shift), group_lanes(value_shift)
    qkv_shift = jnp.stack([query_lanes, jnp.zeros_like(query_lanes), value_lanes], axis=1)
    qkv_lin = (
        (jnp.dot(low_one, qkv_part, preferred_element_type=jnp.float32) + qkv_shift.reshape(-1))
        .astype(jnp.bfloat16)
        .reshape(head_ways, seq_local, piece_len, 3 * group_width)
    )
    tables = tuple(jnp.tile(table, (1, PAIR // HD)) for table in rope_tables())
    attended = after(qkv_lin, below[-1], above[-1])
    for _ in range(tensor_ways - 3):
        line_step(below, above, "tensor")
    mixed_heads = attend_forward(attended, tables)
    mixed_heads, below[-1], above[-1] = lax.optimization_barrier(
        (mixed_heads, below[-1], above[-1])
    )
    line_step(below, above, "tensor")
    mixed_parts = lax.all_to_all(mixed_heads, "heads", split_axis=0, concat_axis=0, tiled=True)
    grad_rows = line_pick(below, above, "tensor").reshape(-1, width)
    mixed_flat = mixed_parts.transpose(1, 2, 0, 3).reshape(token_count, width)
    residual = inputs_f + (
        jnp.dot(mixed_flat, out_full, preferred_element_type=jnp.float32) + out_shift
    ).reshape(inputs.shape)
    normed_two, unit_two, inv_two = layer_norm(residual, gain_two, shift_two)
    low_two = normed_two.astype(jnp.bfloat16)
    flag_rows = slot_flag.astype(jnp.float32)[:, None, None]
    down_shift_grad = jnp.sum(grad_branch.reshape(token_count, width), axis=0, dtype=jnp.float32)
    ffn_local = gate_part.shape[1]
    token_rows3 = gather_rows(after(low_two, gate_part, up_part, below[-1], above[-1]))
    token_rows = token_rows3.reshape(-1, width)
    col_index = lax.axis_index("tensor") * ffn_local + jnp.arange(ffn_local, dtype=jnp.int32)
    unit_mask = (col_index < FF_REAL).astype(jnp.float32)
    gate_pre, up_pre, hidden = hidden_forward(
        token_rows,
        gate_part,
        up_part,
        gate_bias.astype(jnp.float32),
        up_bias.astype(jnp.float32),
        unit_mask,
    )
    first_sum, second_sum = tensor_sums(jnp.sum(hidden, axis=-1), jnp.sum(hidden * hidden, axis=-1))
    inner_scale = inner_gain.astype(jnp.float32)
    normed_hidden, unit_hidden, inv_hidden = inner_normalize(
        hidden, first_sum, second_sum, inner_scale, inner_shift.astype(jnp.float32), unit_mask
    )
    hidden_seqs = normed_hidden.reshape(token_rows3.shape[0], piece_len, ffn_local)

    def down_term(row_start, row_count):
        picked = hidden_seqs.reshape(-1, ffn_local)
        return jnp.dot(picked, down_part, preferred_element_type=jnp.float32).reshape(
            row_count, piece_len, width
        )

    down_grad = outer_product(normed_hidden, grad_rows)
    down_weight_grad = lax.psum_scatter(
        down_grad.astype(jnp.bfloat16), ("fsdp", "heads"), scatter_dimension=1, tiled=True
    )
    grad_normed = times_transpose(after(grad_rows, down_grad), down_part)
    scaled, scaled_sum, cross_sum = hidden_backward_terms(
        grad_normed, unit_hidden, inner_scale, unit_mask
    )
    scaled_sum, cross_sum = tensor_sums(scaled_sum, cross_sum)
    grad_gate, grad_up = gate_grads(
        scaled, scaled_sum, cross_sum, unit_hidden, inv_hidden, gate_pre, up_pre, unit_mask
    )
    gate_grad = outer_product(token_rows, grad_gate)
    up_grad = outer_product(token_rows, grad_up)
    vector_grads = vector_sums(grad_gate, grad_up, grad_normed, unit_hidden, unit_mask)
    gate_seqs = after(grad_gate, down_weight_grad).reshape(-1, piece_len, ffn_local)
    up_seqs = grad_up.reshape(-1, piece_len, ffn_local)

    def input_term(row_start, row_count):
        picked_gate = gate_seqs.reshape(-1, ffn_local)
        picked_up = up_seqs.reshape(-1, ffn_local)
        summed = times_transpose(picked_gate, gate_part) + times_transpose(picked_up, up_part)
        return summed.reshape(row_count, piece_len, width)

    grad_normed_two = scatter_rows(input_term, seq_local)
    gate_weight_grad, up_weight_grad = (
        lax.psum_scatter(
            gate_grad.astype(jnp.bfloat16), ("fsdp", "heads"), scatter_dimension=0, tiled=True
        ).astype(jnp.float32),
        lax.psum_scatter(
            up_grad.astype(jnp.bfloat16), ("fsdp", "heads"), scatter_dimension=0, tiled=True
        ).astype(jnp.float32),
    )
    down_weight_grad = down_weight_grad.astype(jnp.float32)
    gate_bias_grad, up_bias_grad, inner_gain_grad, inner_shift_grad = lax.psum(
        (vector_grads[0], vector_grads[1], vector_grads[2], vector_grads[3]), ("fsdp", "heads")
    )
    grad_normed_two = after(grad_normed_two, gate_bias_grad)
    grad_residual = grad_total + norm_backward(grad_normed_two, unit_two, inv_two, gain_two)
    gain_two_grad = jnp.sum((grad_normed_two * unit_two).reshape(token_count, width), axis=0)
    shift_two_grad = jnp.sum(grad_normed_two.reshape(token_count, width), axis=0)
    grad_attn = grad_residual.astype(jnp.bfloat16).reshape(token_count, width)
    out_weight_part = outer_product(mixed_flat, grad_attn)
    out_shift_grad = jnp.sum(grad_attn, axis=0, dtype=jnp.float32)
    grad_mixed = times_transpose(grad_attn, out_full).astype(jnp.bfloat16)
    grad_parts = grad_mixed.reshape(seq_local, piece_len, head_ways, group_width)
    grad_heads = lax.all_to_all(
        grad_parts.transpose(2, 0, 1, 3), "heads", split_axis=0, concat_axis=0, tiled=True
    )
    branch_terms = down_term(0, seq_local * tensor_ways).astype(jnp.bfloat16)
    branch_terms = branch_terms.reshape((tensor_ways,) + inputs.shape)
    running = line_scatter_step(branch_terms, None, tensor_ways - 1, "tensor", grad_mixed)
    qkv_grad = attend_backward(qkv_lin, grad_heads, tables)
    qkv_grad = after(qkv_grad, *running)
    for distance in range(tensor_ways - 2, 0, -1):
        running = line_scatter_step(branch_terms, running, distance, "tensor", qkv_grad)
    branch_out = (
        line_term(branch_terms, 0, "tensor")
        + running[0].astype(jnp.float32)
        + running[1].astype(jnp.float32)
    )
    output = (flag_rows * (residual + branch_out + down_shift)).astype(jnp.bfloat16)
    qkv_grad = qkv_grad.reshape(head_ways * token_count, 3 * group_width)
    group_grad = times_transpose(qkv_grad, qkv_part)
    gain_one_grad = jnp.sum(group_grad * unit_group, axis=0)
    shift_one_grad = jnp.sum(group_grad, axis=0)
    group_terms = group_grad.astype(jnp.bfloat16)
    grad_normed_one = cube_scatter(
        group_terms.reshape((head_ways,) + inputs.shape), "heads"
    )
    qkv_shift_grad = jnp.sum(qkv_grad, axis=0, dtype=jnp.float32).reshape(group_pairs, 3, PAIR)

    def place_lanes(own_lanes):
        return lax.dynamic_update_slice_in_dim(
            jnp.zeros((width,), jnp.float32), own_lanes.reshape(-1), group_index * group_width, 0
        )

    query_shift_grad = place_lanes(qkv_shift_grad[:, 0])
    value_shift_grad = place_lanes(qkv_shift_grad[:, 2])
    input_grad = (
        grad_residual + norm_backward(grad_normed_one, unit_one, inv_one, gain_one)
    ).astype(jnp.bfloat16)
    vector_terms = jnp.stack(
        [
            gain_one_grad,
            shift_one_grad,
            query_shift_grad,
            value_shift_grad,
            out_shift_grad,
            gain_two_grad,
            shift_two_grad,
            down_shift_grad,
        ]
    )
    vector_lanes = vector_terms.shape[0] * row_part
    vector_rows = (
        vector_terms.reshape(-1, fsdp_ways, head_ways, tensor_ways, row_part)
        .transpose(1, 3, 2, 0, 4)
        .reshape(fsdp_ways, tensor_ways, head_ways, 1, vector_lanes)
    )
    extra_rows = 1
    while head_ways * (row_part + extra_rows) % 16 != 0:
        extra_rows += 1
    vector_rows = jnp.pad(
        vector_rows,
        ((0, 0),) * 3 + ((0, extra_rows - 1), (0, 3 * group_width - vector_lanes)),
    )
    qkv_terms = outer_product(low_one, qkv_grad).astype(jnp.bfloat16)
    qkv_terms = qkv_terms.reshape(
        fsdp_ways, head_ways, tensor_ways, row_part, 3 * group_width
    ).transpose(0, 2, 1, 3, 4)
    qkv_terms = jnp.concatenate([qkv_terms, vector_rows.astype(jnp.bfloat16)], axis=3)
    qkv_half = cube_scatter(
        qkv_terms.reshape(fsdp_ways, -1, 3 * group_width), "fsdp"
    ).astype(jnp.bfloat16)
    qkv_rows = lax.psum_scatter(qkv_half, "tensor", scatter_dimension=0, tiled=True)
    qkv_columns = lax.all_to_all(
        qkv_rows, "heads", split_axis=0, concat_axis=0, tiled=True
    ).reshape(head_ways, row_part + extra_rows, 3 * group_width)
    qkv_weight_grads = (
        qkv_columns[:, :row_part]
        .reshape(head_ways, row_part, group_pairs, 3, PAIR)
        .transpose(3, 1, 0, 2, 4)
        .reshape(3, row_part, width)
        .astype(jnp.float32)
    )
    own_sums = jnp.sum(
        qkv_columns[:, row_part, :vector_lanes].astype(jnp.float32), axis=0
    ).reshape(-1, row_part)
    out_terms = out_weight_part.astype(jnp.bfloat16).reshape(fsdp_ways, -1, width)
    out_half = cube_scatter(out_terms, "fsdp").astype(jnp.bfloat16)
    out_eighth = cube_scatter(out_half.reshape(head_ways, -1, width), "heads")
    out_weight_grad = lax.psum_scatter(
        out_eighth.astype(jnp.bfloat16), "tensor", scatter_dimension=0, tiled=True
    ).astype(jnp.float32)
    attn_sums = tuple(qkv_weight_grads) + (out_weight_grad,) + tuple(own_sums)
    return (
        output,
        input_grad,
        attn_sums[4],
        attn_sums[5],
        attn_sums[0],
        attn_sums[6],
        attn_sums[1],
        attn_sums[2],
        attn_sums[7],
        attn_sums[3],
        attn_sums[8],
        attn_sums[9],
        attn_sums[10],
        gate_weight_grad,
        gate_bias_grad,
        up_weight_grad,
        up_bias_grad,
        inner_gain_grad,
        inner_shift_grad,
        down_weight_grad,
        attn_sums[11],
    )


def solution(mesh):
    return jax.shard_map(
        on_device,
        mesh=mesh,
        in_specs=(
            P(("fsdp", "tensor"), "heads", None),
            P(("fsdp", "tensor")),
            P(("fsdp", "tensor"), "heads", None),
            P(("fsdp", "heads", "tensor")),
            P(("fsdp", "heads", "tensor")),
            P(("fsdp", "heads", "tensor"), None),
            P(("fsdp", "heads", "tensor")),
            P(("fsdp", "heads", "tensor"), None),
            P(("fsdp", "heads", "tensor"), None),
            P(("fsdp", "heads", "tensor")),
            P(("fsdp", "heads", "tensor"), None),
            P(("fsdp", "heads", "tensor")),
            P(("fsdp", "heads", "tensor")),
            P(("fsdp", "heads", "tensor")),
            P(("fsdp", "heads"), "tensor"),
            P("tensor"),
            P(("fsdp", "heads"), "tensor"),
            P("tensor"),
            P("tensor"),
            P("tensor"),
            P("tensor", ("fsdp", "heads")),
            P(("fsdp", "heads", "tensor")),
        ),
        out_specs=(
            P(("fsdp", "tensor"), "heads", None),
            P(("fsdp", "tensor"), "heads", None),
            P(("fsdp", "heads", "tensor")),
            P(("fsdp", "heads", "tensor")),
            P(("fsdp", "heads", "tensor"), None),
            P(("fsdp", "heads", "tensor")),
            P(("fsdp", "heads", "tensor"), None),
            P(("fsdp", "heads", "tensor"), None),
            P(("fsdp", "heads", "tensor")),
            P(("fsdp", "heads", "tensor"), None),
            P(("fsdp", "heads", "tensor")),
            P(("fsdp", "heads", "tensor")),
            P(("fsdp", "heads", "tensor")),
            P(("fsdp", "heads"), "tensor"),
            P("tensor"),
            P(("fsdp", "heads"), "tensor"),
            P("tensor"),
            P("tensor"),
            P("tensor"),
            P("tensor", ("fsdp", "heads")),
            P(("fsdp", "heads", "tensor")),
        ),
        check_vma=False,
    )
```

```python
import math

import jax
import jax.numpy as jnp
from jax import lax
from jax.experimental import pallas as pl
from jax.experimental.pallas import tpu as pltpu
from jax.sharding import PartitionSpec as P

HD = 64
PAIR = 2 * HD
FF_REAL = 2730
GRID = 32


norm_eps = 1e-06


def layer_norm(values, gain_vec, shift_vec):
    row_mean = jnp.mean(values, axis=-1, keepdims=True)
    centered = values - row_mean
    row_var = jnp.mean(centered * centered, axis=-1, keepdims=True)
    inv_std = lax.rsqrt(row_var + norm_eps)
    unit_rows = centered * inv_std
    return (unit_rows * gain_vec + shift_vec, unit_rows, inv_std)


def norm_backward(grad_values, unit_rows, inv_std, gain_vec):
    scaled = grad_values * gain_vec
    centered = scaled - jnp.mean(scaled, axis=-1, keepdims=True)
    centered = centered - unit_rows * jnp.mean(scaled * unit_rows, axis=-1, keepdims=True)
    return centered * inv_std


def rope_tables():
    positions = jnp.arange(GRID * GRID, dtype=jnp.int32)
    row_place = (positions // GRID).astype(jnp.float32)
    col_place = (positions % GRID).astype(jnp.float32)
    quarter = HD // 4
    frequency = jnp.power(10000.0, -jnp.arange(quarter, dtype=jnp.float32) / quarter)
    angles = jnp.concatenate(
        [row_place[:, None] * frequency[None, :], col_place[:, None] * frequency[None, :]], axis=1
    )
    angles = jnp.repeat(angles, 2, axis=1)
    return (jnp.cos(angles), jnp.sin(angles))


def pair_swap(values):
    count = values.shape[-1]
    lanes = lax.broadcasted_iota(jnp.int32, values.shape, 1)
    following = pltpu.roll(values, count - 1, 1)
    preceding = pltpu.roll(values, 1, 1)
    return jnp.where(lanes % 2 == 0, -following, preceding)


def rotate(values, cosine_table, sine_table):
    return values * cosine_table + pair_swap(values) * sine_table


def rotate_back(grad_values, cosine_table, sine_table):
    return grad_values * cosine_table - pair_swap(grad_values * sine_table)


def outer_product(left_rows, right_rows):
    return lax.dot_general(
        left_rows, right_rows, (((0,), (0,)), ((), ())), preferred_element_type=jnp.float32
    )


def times_transpose(left_rows, right_rows):
    return lax.dot_general(
        left_rows, right_rows, (((1,), (1,)), ((), ())), preferred_element_type=jnp.float32
    )


def gather_rows(block_values):
    return lax.all_gather(block_values, "tensor", axis=0, tiled=True)


def tensor_sums(first_sum, second_sum):
    both = lax.psum(jnp.stack([first_sum, second_sum]).astype(jnp.bfloat16), "tensor")
    return (both[0].astype(jnp.float32), both[1].astype(jnp.float32))


def cube_pairs(ways, bit):
    return [(place, place ^ (1 << bit)) for place in range(ways)]


def cube_gather(block, axis_name):
    ways = lax.axis_size(axis_name)
    bits = ways.bit_length() - 1
    index = lax.axis_index(axis_name)
    held = block.reshape((1,) * bits + block.shape)
    for bit in reversed(range(bits)):
        place = bits - 1 - bit
        other = lax.ppermute(held, axis_name, cube_pairs(ways, bit))
        held = jnp.where(
            (index >> bit) % 2 == 0,
            jnp.concatenate([held, other], axis=place),
            jnp.concatenate([other, held], axis=place),
        )
    return held.reshape((ways * block.shape[0],) + block.shape[1:])


def cube_scatter(terms, axis_name):
    ways = lax.axis_size(axis_name)
    bits = ways.bit_length() - 1
    index = lax.axis_index(axis_name)
    held = terms.reshape((2,) * bits + terms.shape[1:])
    for bit in range(bits):
        place = bits - 1 - bit
        mine = (index >> bit) % 2
        kept = lax.dynamic_index_in_dim(held, mine, place, keepdims=False)
        sent = lax.dynamic_index_in_dim(held, 1 - mine, place, keepdims=False)
        other = lax.ppermute(sent.astype(jnp.bfloat16), axis_name, cube_pairs(ways, bit))
        held = kept.astype(jnp.float32) + other.astype(jnp.float32)
    return held


def line_pairs(ways):
    upward = [(place, place + 1) for place in range(ways - 1)]
    return (upward, [(target, source) for source, target in upward])


def line_step(below, above, axis_name):
    upward, downward = line_pairs(lax.axis_size(axis_name))
    below.append(lax.ppermute(below[-1], axis_name, upward))
    above.append(lax.ppermute(above[-1], axis_name, downward))


def line_pick(below, above, axis_name):
    ways = lax.axis_size(axis_name)
    block = below[0]
    around = jnp.stack(below[:0:-1] + [block] + above[1:])
    picked = lax.dynamic_slice_in_dim(around, ways - 1 - lax.axis_index(axis_name), ways, 0)
    return picked.reshape((ways * block.shape[0],) + block.shape[1:])


def after(value, *others):
    return lax.optimization_barrier((value,) + others)[0]


def line_term(terms, offset, axis_name):
    place = lax.axis_index(axis_name) + offset
    place = jnp.clip(place, 0, lax.axis_size(axis_name) - 1)
    return lax.dynamic_index_in_dim(terms, place, 0, keepdims=False).astype(jnp.float32)


def line_scatter_step(terms, running, distance, axis_name, gate):
    pairs = line_pairs(lax.axis_size(axis_name))
    passed = []
    for side, sign in ((0, 1), (1, -1)):
        total = line_term(terms, sign * distance, axis_name)
        if running is not None:
            total = total + running[side].astype(jnp.float32)
        gated = after(total.astype(jnp.bfloat16), gate)
        passed.append(lax.ppermute(gated, axis_name, pairs[side]))
    return passed


def scatter_rows(term_fn, row_total):
    return lax.psum_scatter(
        term_fn(jnp.int32(0), row_total * lax.axis_size("tensor")).astype(jnp.bfloat16),
        "tensor",
        scatter_dimension=0,
        tiled=True,
    ).astype(jnp.float32)


def head_masks(axis):
    shape = (1, PAIR) if axis == 1 else (PAIR, 1)
    place = lax.broadcasted_iota(jnp.int32, shape, axis)
    first = (place < HD).astype(jnp.float32)
    return (first, 1.0 - first)


def load_heads(qkv_ref, cosine_ref, sine_ref, query_s, key_s, value_s):
    rows = qkv_ref[...].reshape(query_s.shape[0], 3 * PAIR)
    cosine, sine = cosine_ref[...], sine_ref[...]
    query_rot = rotate(rows[:, :PAIR].astype(jnp.float32), cosine, sine).astype(jnp.bfloat16)
    query_s[...] = (query_rot.astype(jnp.float32) * (1.0 / math.sqrt(HD))).astype(jnp.bfloat16)
    key_rot = rotate(rows[:, PAIR : 2 * PAIR].astype(jnp.float32), cosine, sine)
    key_s[...] = key_rot.astype(jnp.bfloat16)
    value_s[...] = rows[:, 2 * PAIR :]


def forward_kernel(qkv_ref, cosine_ref, sine_ref, mixed_ref, query_s, key_s, value_s):
    load_heads(qkv_ref, cosine_ref, sine_ref, query_s, key_s, value_s)
    pieces, _, piece_len, _ = mixed_ref.shape
    masks = head_masks(1)

    def one_piece(piece, carry):
        start = pl.multiple_of(piece * piece_len, piece_len)
        query_rows = query_s[pl.ds(start, piece_len), :]
        mixed = jnp.zeros((piece_len, PAIR), jnp.float32)
        for mask in masks:
            own_query = query_rows * mask.astype(jnp.bfloat16)
            scores = times_transpose(own_query, key_s[...])
            weights_exp = jnp.exp(scores - jnp.max(scores, axis=-1, keepdims=True))
            inverse = 1.0 / jnp.sum(weights_exp, axis=-1, keepdims=True)
            probs_low = (weights_exp * inverse).astype(jnp.bfloat16)
            part = jnp.dot(probs_low, value_s[...], preferred_element_type=jnp.float32)
            mixed = mixed + part * mask
        mixed_ref[piece, 0] = mixed.astype(jnp.bfloat16)
        return carry

    lax.fori_loop(0, pieces, one_piece, 0)


def backward_kernel(
    qkv_ref, grad_ref, cosine_ref, sine_ref, out_ref,
    query_s, key_s, value_s, turned_s, key_grad_s, value_grad_s,
):
    load_heads(qkv_ref, cosine_ref, sine_ref, query_s, key_s, value_s)
    pieces, _, piece_len, _ = grad_ref.shape
    turned_s[...] = key_s[...].astype(jnp.float32).T.astype(jnp.bfloat16)
    key_grad_s[...] = jnp.zeros_like(key_grad_s)
    value_grad_s[...] = jnp.zeros_like(value_grad_s)
    row_masks = head_masks(1)
    column_masks = head_masks(0)

    def one_piece(piece, carry):
        start = pl.multiple_of(piece * piece_len, piece_len)
        rows = pl.ds(start, piece_len)
        query_rows = query_s[rows, :]
        grad_rows = grad_ref[piece, 0]
        query_grad = jnp.zeros((PAIR, piece_len), jnp.float32)
        for mask, column_mask in zip(row_masks, column_masks):
            own_query = query_rows * mask.astype(jnp.bfloat16)
            own_grad = grad_rows * mask.astype(jnp.bfloat16)
            scores = times_transpose(key_s[...], own_query)
            weights_exp = jnp.exp(scores - jnp.max(scores, axis=0, keepdims=True))
            probs = weights_exp * (1.0 / jnp.sum(weights_exp, axis=0, keepdims=True))
            grad_probs = times_transpose(value_s[...], own_grad)
            row_dot = jnp.sum(grad_probs * probs, axis=0, keepdims=True)
            grad_scores = (probs * (grad_probs - row_dot)).astype(jnp.bfloat16)
            value_grad_s[...] += jnp.dot(
                probs.astype(jnp.bfloat16), own_grad, preferred_element_type=jnp.float32
            )
            key_grad_s[...] += jnp.dot(grad_scores, own_query, preferred_element_type=jnp.float32)
            own_turned = turned_s[...] * column_mask.astype(jnp.bfloat16)
            query_grad = query_grad + jnp.dot(
                own_turned, grad_scores, preferred_element_type=jnp.float32
            )
        query_grad = query_grad.T * (1.0 / math.sqrt(HD))
        turned = rotate_back(query_grad, cosine_ref[rows, :], sine_ref[rows, :])
        out_ref[piece, 0, :, :PAIR] = turned.astype(jnp.bfloat16)
        return carry

    lax.fori_loop(0, pieces, one_piece, 0)
    piece_shape = (pieces, 1, piece_len, PAIR)
    key_grad = rotate_back(key_grad_s[...], cosine_ref[...], sine_ref[...])
    out_ref[:, :, :, PAIR : 2 * PAIR] = key_grad.astype(jnp.bfloat16).reshape(piece_shape)
    out_ref[:, :, :, 2 * PAIR :] = value_grad_s[...].astype(jnp.bfloat16).reshape(piece_shape)


def attention_call(kernel, name, qkv, extra, tables, out_lanes, more_scratch, products):
    pieces, seq_count, piece_len, lanes = qkv.shape
    pair_count = lanes // (3 * PAIR)
    length = pieces * piece_len

    def per_pair(wide):
        return pl.BlockSpec((pieces, 1, piece_len, wide), lambda seq, pair: (0, seq, 0, pair))

    table_spec = pl.BlockSpec((length, PAIR), lambda seq, pair: (0, 0))
    blocks = seq_count * pair_count
    return pl.pallas_call(
        kernel,
        name=name,
        grid=(seq_count, pair_count),
        in_specs=[per_pair(3 * PAIR)] + [per_pair(PAIR)] * len(extra) + [table_spec] * 2,
        out_specs=per_pair(out_lanes),
        out_shape=jax.ShapeDtypeStruct(
            (pieces, seq_count, piece_len, pair_count * out_lanes), jnp.bfloat16
        ),
        scratch_shapes=[pltpu.VMEM((length, PAIR), jnp.bfloat16)] * 3 + more_scratch,
        compiler_params=pltpu.CompilerParams(vmem_limit_bytes=48 << 20),
        cost_estimate=pl.CostEstimate(
            flops=blocks * products * 4 * length * length * PAIR,
            bytes_accessed=blocks * length * PAIR * 16,
            transcendentals=blocks * 2 * length * length,
        ),
    )(qkv, *extra, *tables)


def attend_forward(qkv, tables):
    return attention_call(forward_kernel, "attend_forward", qkv, (), tables, PAIR, [], 2)


def attend_backward(qkv, grad_mixed, tables):
    length = qkv.shape[0] * qkv.shape[2]
    more = [
        pltpu.VMEM((PAIR, length), jnp.bfloat16),
        pltpu.VMEM((length, PAIR), jnp.float32),
        pltpu.VMEM((length, PAIR), jnp.float32),
    ]
    return attention_call(
        backward_kernel, "attend_backward", qkv, (grad_mixed,), tables, 3 * PAIR, more, 5
    )


def hidden_forward(token_rows, gate_part, up_part, gate_shift, up_shift, unit_mask):
    gate_pre = jnp.dot(token_rows, gate_part, preferred_element_type=jnp.float32) + gate_shift
    up_pre = jnp.dot(token_rows, up_part, preferred_element_type=jnp.float32) + up_shift
    return (gate_pre, up_pre, jax.nn.silu(gate_pre) * up_pre * unit_mask)


def inner_normalize(hidden, first_sum, second_sum, inner_scale, inner_offset, unit_mask):
    unit_mean = first_sum[:, None] / FF_REAL
    unit_var = second_sum[:, None] / FF_REAL - unit_mean * unit_mean
    inv_std = lax.rsqrt(unit_var + norm_eps)
    unit_hidden = (hidden - unit_mean) * inv_std
    normed = ((unit_hidden * inner_scale + inner_offset) * unit_mask).astype(jnp.bfloat16)
    return (normed, unit_hidden, inv_std)


def hidden_backward_terms(grad_normed, unit_hidden, inner_scale, unit_mask):
    scaled = grad_normed * unit_mask * inner_scale
    return (scaled, jnp.sum(scaled, axis=-1), jnp.sum(scaled * unit_hidden, axis=-1))


def gate_grads(scaled, scaled_sum, cross_sum, unit_hidden, inv_std, gate_pre, up_pre, unit_mask):
    grad_hidden = (
        unit_mask
        * (scaled - scaled_sum[:, None] / FF_REAL - unit_hidden * cross_sum[:, None] / FF_REAL)
        * inv_std
    )
    sigmoid_gate = jax.nn.sigmoid(gate_pre)
    grad_gate = (
        grad_hidden * up_pre * sigmoid_gate * (1.0 + gate_pre * (1.0 - sigmoid_gate))
    ).astype(jnp.bfloat16)
    grad_up = (grad_hidden * gate_pre * sigmoid_gate).astype(jnp.bfloat16)
    return (grad_gate, grad_up)


def vector_sums(grad_gate, grad_up, grad_normed, unit_hidden, unit_mask):
    return (
        jnp.sum(grad_gate, axis=0, dtype=jnp.float32),
        jnp.sum(grad_up, axis=0, dtype=jnp.float32),
        jnp.sum(grad_normed * unit_mask * unit_hidden, axis=0),
        jnp.sum(grad_normed * unit_mask, axis=0),
    )


def on_device(
    inputs,
    slot_flag,
    cotangent,
    first_gain,
    first_shift,
    query_weight,
    query_bias,
    key_weight,
    value_weight,
    value_bias,
    out_weight,
    out_bias,
    second_gain,
    second_shift,
    gate_weight,
    gate_bias,
    up_weight,
    up_bias,
    inner_gain,
    inner_shift,
    down_weight,
    down_bias,
):
    seq_local, piece_len, width = inputs.shape
    head_ways = lax.axis_size("heads")
    seq_len = piece_len * head_ways
    group_width = width // head_ways
    group_pairs = group_width // PAIR
    token_count = seq_local * piece_len
    fsdp_ways, tensor_ways = lax.axis_size("fsdp"), lax.axis_size("tensor")
    row_part = query_weight.shape[0]
    group_index = lax.axis_index("heads")
    inputs_group = cube_gather(inputs, "heads")
    grad_flags = slot_flag.astype(jnp.float32)[:, None, None]
    grad_total = grad_flags * cotangent.astype(jnp.float32)
    grad_branch = grad_total.astype(jnp.bfloat16)
    below, above = [grad_branch], [grad_branch]
    line_step(below, above, "tensor")
    below[-1], above[-1] = after(below[-1], inputs_group), after(above[-1], inputs_group)
    line_step(below, above, "tensor")
    stacked = jnp.stack(
        [
            member.reshape(row_part, head_ways, group_pairs, PAIR)
            for member in (query_weight, key_weight, value_weight)
        ],
        axis=3,
    ).reshape(row_part, head_ways, 3 * group_width)
    vectors = (
        first_gain,
        first_shift,
        query_bias,
        value_bias,
        out_bias,
        second_gain,
        second_shift,
        down_bias,
    )
    row_lanes = 3 * group_width
    vector_row = jnp.zeros((row_lanes,), jnp.float32)
    for place, member in enumerate(vectors):
        ahead = place * row_part
        vector_row = vector_row + jnp.pad(
            member.astype(jnp.float32), (ahead, row_lanes - ahead - row_part)
        )
    vector_row = vector_row.astype(jnp.bfloat16)
    sent_columns = jnp.concatenate(
        [
            stacked.transpose(1, 0, 2),
            jnp.broadcast_to(vector_row, (head_ways, 1, 3 * group_width)),
        ],
        axis=1,
    )
    own_columns = lax.all_to_all(
        sent_columns, "heads", split_axis=0, concat_axis=0, tiled=True
    )
    columns = lax.all_gather(
        own_columns.reshape(-1, 3 * group_width), ("fsdp", "tensor"), axis=0, tiled=True
    )
    group_f = inputs_group.reshape(-1, width).astype(jnp.float32)
    group_mean = jnp.mean(group_f, axis=-1, keepdims=True)
    group_var = jnp.mean(jnp.square(group_f - group_mean), axis=-1, keepdims=True)
    group_inv = lax.rsqrt(group_var + norm_eps)
    columns, group_mean, group_inv = lax.optimization_barrier((columns, group_mean, group_inv))
    columns = columns.reshape(
        fsdp_ways, tensor_ways, head_ways, row_part + 1, 3 * group_width
    ).transpose(0, 2, 1, 3, 4)
    qkv_part = columns[:, :, :, :row_part].reshape(width, 3 * group_width)
    below[-1], above[-1] = after(below[-1], columns), after(above[-1], columns)
    line_step(below, above, "tensor")
    gathered = (
        columns[:, :, :, row_part, : len(vectors) * row_part]
        .reshape(-1, 8, row_part)
        .transpose(1, 0, 2)
        .reshape(8, width)
    )
    out_below, out_above = [out_weight], [out_weight]
    for _ in range(tensor_ways - 1):
        line_step(out_below, out_above, "tensor")
    out_full = lax.all_gather(
        line_pick(out_below, out_above, "tensor"),
        ("fsdp", "heads"),
        axis=0,
        tiled=True,
    )
    gain_one, shift_one, query_shift, value_shift, out_shift, gain_two, shift_two, down_shift = [
        member.astype(jnp.float32) for member in gathered
    ]
    gate_part, up_part, down_part = (
        lax.all_gather(gate_weight, ("fsdp", "heads"), axis=0, tiled=True),
        lax.all_gather(up_weight, ("fsdp", "heads"), axis=0, tiled=True),
        lax.all_gather(down_weight, ("fsdp", "heads"), axis=1, tiled=True),
    )
    inputs_f = inputs.astype(jnp.float32)
    _, unit_one, inv_one = layer_norm(inputs_f, gain_one, shift_one)
    unit_group = (group_f - group_mean) * group_inv
    low_one = (unit_group * gain_one + shift_one).astype(jnp.bfloat16)

    def group_lanes(full_vec):
        own = lax.dynamic_slice_in_dim(full_vec, group_index * group_width, group_width, 0)
        return own.reshape(group_pairs, PAIR)

    query_lanes, value_lanes = group_lanes(query_shift), group_lanes(value_shift)
    qkv_shift = jnp.stack([query_lanes, jnp.zeros_like(query_lanes), value_lanes], axis=1)
    qkv_lin = (
        (jnp.dot(low_one, qkv_part, preferred_element_type=jnp.float32) + qkv_shift.reshape(-1))
        .astype(jnp.bfloat16)
        .reshape(head_ways, seq_local, piece_len, 3 * group_width)
    )
    tables = tuple(jnp.tile(table, (1, PAIR // HD)) for table in rope_tables())
    mixed_heads = attend_forward(qkv_lin, tables)
    mixed_heads, below[-1], above[-1] = lax.optimization_barrier(
        (mixed_heads, below[-1], above[-1])
    )
    for _ in range(tensor_ways - 4):
        line_step(below, above, "tensor")
    mixed_parts = lax.all_to_all(mixed_heads, "heads", split_axis=0, concat_axis=0, tiled=True)
    grad_rows = line_pick(below, above, "tensor").reshape(-1, width)
    mixed_flat = mixed_parts.transpose(1, 2, 0, 3).reshape(token_count, width)
    residual = inputs_f + (
        jnp.dot(mixed_flat, out_full, preferred_element_type=jnp.float32) + out_shift
    ).reshape(inputs.shape)
    normed_two, unit_two, inv_two = layer_norm(residual, gain_two, shift_two)
    low_two = normed_two.astype(jnp.bfloat16)
    flag_rows = slot_flag.astype(jnp.float32)[:, None, None]
    down_shift_grad = jnp.sum(grad_branch.reshape(token_count, width), axis=0, dtype=jnp.float32)
    ffn_local = gate_part.shape[1]
    token_rows3 = gather_rows(after(low_two, gate_part, up_part, below[-1], above[-1]))
    token_rows = token_rows3.reshape(-1, width)
    col_index = lax.axis_index("tensor") * ffn_local + jnp.arange(ffn_local, dtype=jnp.int32)
    unit_mask = (col_index < FF_REAL).astype(jnp.float32)
    gate_pre, up_pre, hidden = hidden_forward(
        token_rows,
        gate_part,
        up_part,
        gate_bias.astype(jnp.float32),
        up_bias.astype(jnp.float32),
        unit_mask,
    )
    first_sum, second_sum = tensor_sums(jnp.sum(hidden, axis=-1), jnp.sum(hidden * hidden, axis=-1))
    inner_scale = inner_gain.astype(jnp.float32)
    normed_hidden, unit_hidden, inv_hidden = inner_normalize(
        hidden, first_sum, second_sum, inner_scale, inner_shift.astype(jnp.float32), unit_mask
    )
    hidden_seqs = normed_hidden.reshape(token_rows3.shape[0], piece_len, ffn_local)

    def down_term(row_start, row_count):
        picked = hidden_seqs.reshape(-1, ffn_local)
        return jnp.dot(picked, down_part, preferred_element_type=jnp.float32).reshape(
            row_count, piece_len, width
        )

    down_grad = outer_product(normed_hidden, grad_rows)
    down_weight_grad = lax.psum_scatter(
        down_grad.astype(jnp.bfloat16), ("fsdp", "heads"), scatter_dimension=1, tiled=True
    )
    grad_normed = times_transpose(after(grad_rows, down_grad), down_part)
    scaled, scaled_sum, cross_sum = hidden_backward_terms(
        grad_normed, unit_hidden, inner_scale, unit_mask
    )
    scaled_sum, cross_sum = tensor_sums(scaled_sum, cross_sum)
    grad_gate, grad_up = gate_grads(
        scaled, scaled_sum, cross_sum, unit_hidden, inv_hidden, gate_pre, up_pre, unit_mask
    )
    gate_grad = outer_product(token_rows, grad_gate)
    up_grad = outer_product(token_rows, grad_up)
    vector_grads = vector_sums(grad_gate, grad_up, grad_normed, unit_hidden, unit_mask)
    gate_seqs = after(grad_gate, down_weight_grad).reshape(-1, piece_len, ffn_local)
    up_seqs = grad_up.reshape(-1, piece_len, ffn_local)

    def input_term(row_start, row_count):
        picked_gate = gate_seqs.reshape(-1, ffn_local)
        picked_up = up_seqs.reshape(-1, ffn_local)
        summed = times_transpose(picked_gate, gate_part) + times_transpose(picked_up, up_part)
        return summed.reshape(row_count, piece_len, width)

    grad_normed_two = scatter_rows(input_term, seq_local)
    gate_weight_grad, up_weight_grad = (
        lax.psum_scatter(
            gate_grad.astype(jnp.bfloat16), ("fsdp", "heads"), scatter_dimension=0, tiled=True
        ).astype(jnp.float32),
        lax.psum_scatter(
            up_grad.astype(jnp.bfloat16), ("fsdp", "heads"), scatter_dimension=0, tiled=True
        ).astype(jnp.float32),
    )
    down_weight_grad = down_weight_grad.astype(jnp.float32)
    gate_bias_grad, up_bias_grad, inner_gain_grad, inner_shift_grad = lax.psum(
        (vector_grads[0], vector_grads[1], vector_grads[2], vector_grads[3]), ("fsdp", "heads")
    )
    grad_normed_two = after(grad_normed_two, gate_bias_grad)
    branch_terms = down_term(0, seq_local * tensor_ways).astype(jnp.bfloat16)
    branch_terms = branch_terms.reshape((tensor_ways,) + inputs.shape)
    running = line_scatter_step(branch_terms, None, tensor_ways - 1, "tensor", grad_normed_two)
    grad_residual = grad_total + norm_backward(grad_normed_two, unit_two, inv_two, gain_two)
    gain_two_grad = jnp.sum((grad_normed_two * unit_two).reshape(token_count, width), axis=0)
    shift_two_grad = jnp.sum(grad_normed_two.reshape(token_count, width), axis=0)
    grad_attn = grad_residual.astype(jnp.bfloat16).reshape(token_count, width)
    out_weight_part = outer_product(mixed_flat, grad_attn)
    out_shift_grad = jnp.sum(grad_attn, axis=0, dtype=jnp.float32)
    grad_mixed = times_transpose(grad_attn, out_full).astype(jnp.bfloat16)
    grad_parts = grad_mixed.reshape(seq_local, piece_len, head_ways, group_width)
    grad_heads = lax.all_to_all(
        grad_parts.transpose(2, 0, 1, 3), "heads", split_axis=0, concat_axis=0, tiled=True
    )
    grad_heads = after(grad_heads, *running)
    running = line_scatter_step(branch_terms, running, tensor_ways - 2, "tensor", grad_heads)
    qkv_grad = attend_backward(qkv_lin, grad_heads, tables)
    qkv_grad = after(qkv_grad, *running)
    for distance in range(tensor_ways - 3, 0, -1):
        running = line_scatter_step(branch_terms, running, distance, "tensor", qkv_grad)
    branch_out = (
        line_term(branch_terms, 0, "tensor")
        + running[0].astype(jnp.float32)
        + running[1].astype(jnp.float32)
    )
    output = (flag_rows * (residual + branch_out + down_shift)).astype(jnp.bfloat16)
    qkv_grad = qkv_grad.reshape(head_ways * token_count, 3 * group_width)
    group_grad = times_transpose(qkv_grad, qkv_part)
    gain_one_grad = jnp.sum(group_grad * unit_group, axis=0)
    shift_one_grad = jnp.sum(group_grad, axis=0)
    group_terms = group_grad.astype(jnp.bfloat16)
    grad_normed_one = cube_scatter(
        group_terms.reshape((head_ways,) + inputs.shape), "heads"
    )
    qkv_shift_grad = jnp.sum(qkv_grad, axis=0, dtype=jnp.float32).reshape(group_pairs, 3, PAIR)

    def place_lanes(own_lanes):
        return lax.dynamic_update_slice_in_dim(
            jnp.zeros((width,), jnp.float32), own_lanes.reshape(-1), group_index * group_width, 0
        )

    query_shift_grad = place_lanes(qkv_shift_grad[:, 0])
    value_shift_grad = place_lanes(qkv_shift_grad[:, 2])
    input_grad = (
        grad_residual + norm_backward(grad_normed_one, unit_one, inv_one, gain_one)
    ).astype(jnp.bfloat16)
    vector_terms = jnp.stack(
        [
            gain_one_grad,
            shift_one_grad,
            query_shift_grad,
            value_shift_grad,
            out_shift_grad,
            gain_two_grad,
            shift_two_grad,
            down_shift_grad,
        ]
    )
    vector_lanes = vector_terms.shape[0] * row_part
    vector_rows = (
        vector_terms.reshape(-1, fsdp_ways, head_ways, tensor_ways, row_part)
        .transpose(1, 3, 2, 0, 4)
        .reshape(fsdp_ways, tensor_ways, head_ways, 1, vector_lanes)
    )
    extra_rows = 1
    while head_ways * (row_part + extra_rows) % 16 != 0:
        extra_rows += 1
    vector_rows = jnp.pad(
        vector_rows,
        ((0, 0),) * 3 + ((0, extra_rows - 1), (0, 3 * group_width - vector_lanes)),
    )
    qkv_terms = outer_product(low_one, qkv_grad).astype(jnp.bfloat16)
    qkv_terms = qkv_terms.reshape(
        fsdp_ways, head_ways, tensor_ways, row_part, 3 * group_width
    ).transpose(0, 2, 1, 3, 4)
    qkv_terms = jnp.concatenate([qkv_terms, vector_rows.astype(jnp.bfloat16)], axis=3)
    qkv_half = cube_scatter(
        qkv_terms.reshape(fsdp_ways, -1, 3 * group_width), "fsdp"
    ).astype(jnp.bfloat16)
    qkv_rows = lax.psum_scatter(qkv_half, "tensor", scatter_dimension=0, tiled=True)
    qkv_columns = lax.all_to_all(
        qkv_rows, "heads", split_axis=0, concat_axis=0, tiled=True
    ).reshape(head_ways, row_part + extra_rows, 3 * group_width)
    qkv_weight_grads = (
        qkv_columns[:, :row_part]
        .reshape(head_ways, row_part, group_pairs, 3, PAIR)
        .transpose(3, 1, 0, 2, 4)
        .reshape(3, row_part, width)
        .astype(jnp.float32)
    )
    own_sums = jnp.sum(
        qkv_columns[:, row_part, :vector_lanes].astype(jnp.float32), axis=0
    ).reshape(-1, row_part)
    out_terms = out_weight_part.astype(jnp.bfloat16).reshape(fsdp_ways, -1, width)
    out_half = cube_scatter(out_terms, "fsdp").astype(jnp.bfloat16)
    out_eighth = cube_scatter(out_half.reshape(head_ways, -1, width), "heads")
    out_weight_grad = lax.psum_scatter(
        out_eighth.astype(jnp.bfloat16), "tensor", scatter_dimension=0, tiled=True
    ).astype(jnp.float32)
    attn_sums = tuple(qkv_weight_grads) + (out_weight_grad,) + tuple(own_sums)
    return (
        output,
        input_grad,
        attn_sums[4],
        attn_sums[5],
        attn_sums[0],
        attn_sums[6],
        attn_sums[1],
        attn_sums[2],
        attn_sums[7],
        attn_sums[3],
        attn_sums[8],
        attn_sums[9],
        attn_sums[10],
        gate_weight_grad,
        gate_bias_grad,
        up_weight_grad,
        up_bias_grad,
        inner_gain_grad,
        inner_shift_grad,
        down_weight_grad,
        attn_sums[11],
    )


def solution(mesh):
    return jax.shard_map(
        on_device,
        mesh=mesh,
        in_specs=(
            P(("fsdp", "tensor"), "heads", None),
            P(("fsdp", "tensor")),
            P(("fsdp", "tensor"), "heads", None),
            P(("fsdp", "heads", "tensor")),
            P(("fsdp", "heads", "tensor")),
            P(("fsdp", "heads", "tensor"), None),
            P(("fsdp", "heads", "tensor")),
            P(("fsdp", "heads", "tensor"), None),
            P(("fsdp", "heads", "tensor"), None),
            P(("fsdp", "heads", "tensor")),
            P(("fsdp", "heads", "tensor"), None),
            P(("fsdp", "heads", "tensor")),
            P(("fsdp", "heads", "tensor")),
            P(("fsdp", "heads", "tensor")),
            P(("fsdp", "heads"), "tensor"),
            P("tensor"),
            P(("fsdp", "heads"), "tensor"),
            P("tensor"),
            P("tensor"),
            P("tensor"),
            P("tensor", ("fsdp", "heads")),
            P(("fsdp", "heads", "tensor")),
        ),
        out_specs=(
            P(("fsdp", "tensor"), "heads", None),
            P(("fsdp", "tensor"), "heads", None),
            P(("fsdp", "heads", "tensor")),
            P(("fsdp", "heads", "tensor")),
            P(("fsdp", "heads", "tensor"), None),
            P(("fsdp", "heads", "tensor")),
            P(("fsdp", "heads", "tensor"), None),
            P(("fsdp", "heads", "tensor"), None),
            P(("fsdp", "heads", "tensor")),
            P(("fsdp", "heads", "tensor"), None),
            P(("fsdp", "heads", "tensor")),
            P(("fsdp", "heads", "tensor")),
            P(("fsdp", "heads", "tensor")),
            P(("fsdp", "heads"), "tensor"),
            P("tensor"),
            P(("fsdp", "heads"), "tensor"),
            P("tensor"),
            P("tensor"),
            P("tensor"),
            P("tensor", ("fsdp", "heads")),
            P(("fsdp", "heads", "tensor")),
        ),
        check_vma=False,
    )
```

```python
import math

import jax
import jax.numpy as jnp
from jax import lax
from jax.experimental import pallas as pl
from jax.experimental.pallas import tpu as pltpu
from jax.sharding import PartitionSpec as P


HD = 64
PAIR = 2 * HD
FF_REAL = 2730
GRID = 32


norm_eps = 1e-06


def layer_norm(values, gain_vec, shift_vec):
    row_mean = jnp.mean(values, axis=-1, keepdims=True)
    centered = values - row_mean
    row_var = jnp.mean(centered * centered, axis=-1, keepdims=True)
    inv_std = lax.rsqrt(row_var + norm_eps)
    unit_rows = centered * inv_std
    return (unit_rows * gain_vec + shift_vec, unit_rows, inv_std)


def norm_backward(grad_values, unit_rows, inv_std, gain_vec):
    scaled = grad_values * gain_vec
    centered = scaled - jnp.mean(scaled, axis=-1, keepdims=True)
    centered = centered - unit_rows * jnp.mean(scaled * unit_rows, axis=-1, keepdims=True)
    return centered * inv_std


def rope_tables():
    positions = jnp.arange(GRID * GRID, dtype=jnp.int32)
    row_place = (positions // GRID).astype(jnp.float32)
    col_place = (positions % GRID).astype(jnp.float32)
    quarter = HD // 4
    frequency = jnp.power(10000.0, -jnp.arange(quarter, dtype=jnp.float32) / quarter)
    angles = jnp.concatenate(
        [row_place[:, None] * frequency[None, :], col_place[:, None] * frequency[None, :]], axis=1
    )
    angles = jnp.repeat(angles, 2, axis=1)
    return (jnp.cos(angles), jnp.sin(angles))


def pair_swap(values):
    count = values.shape[-1]
    lanes = lax.broadcasted_iota(jnp.int32, values.shape, 1)
    following = pltpu.roll(values, count - 1, 1)
    preceding = pltpu.roll(values, 1, 1)
    return jnp.where(lanes % 2 == 0, -following, preceding)


def rotate(values, cosine_table, sine_table):
    return values * cosine_table + pair_swap(values) * sine_table


def rotate_back(grad_values, cosine_table, sine_table):
    return grad_values * cosine_table - pair_swap(grad_values * sine_table)


def outer_product(left_rows, right_rows):
    return lax.dot_general(
        left_rows, right_rows, (((0,), (0,)), ((), ())), preferred_element_type=jnp.float32
    )


def times_transpose(left_rows, right_rows):
    return lax.dot_general(
        left_rows, right_rows, (((1,), (1,)), ((), ())), preferred_element_type=jnp.float32
    )


def gather_rows(block_values):
    return lax.all_gather(block_values, "tensor", axis=0, tiled=True)


def tensor_sums(first_sum, second_sum):
    both = lax.psum(jnp.stack([first_sum, second_sum]).astype(jnp.bfloat16), "tensor")
    return (both[0].astype(jnp.float32), both[1].astype(jnp.float32))


def cube_pairs(ways, bit):
    return [(place, place ^ (1 << bit)) for place in range(ways)]


def cube_gather(block, axis_name):
    ways = lax.axis_size(axis_name)
    bits = ways.bit_length() - 1
    index = lax.axis_index(axis_name)
    held = block.reshape((1,) * bits + block.shape)
    for bit in reversed(range(bits)):
        place = bits - 1 - bit
        other = lax.ppermute(held, axis_name, cube_pairs(ways, bit))
        held = jnp.where(
            (index >> bit) % 2 == 0,
            jnp.concatenate([held, other], axis=place),
            jnp.concatenate([other, held], axis=place),
        )
    return held.reshape((ways * block.shape[0],) + block.shape[1:])


def cube_scatter(terms, axis_name):
    ways = lax.axis_size(axis_name)
    bits = ways.bit_length() - 1
    index = lax.axis_index(axis_name)
    held = terms.reshape((2,) * bits + terms.shape[1:])
    for bit in range(bits):
        place = bits - 1 - bit
        mine = (index >> bit) % 2
        kept = lax.dynamic_index_in_dim(held, mine, place, keepdims=False)
        sent = lax.dynamic_index_in_dim(held, 1 - mine, place, keepdims=False)
        other = lax.ppermute(sent.astype(jnp.bfloat16), axis_name, cube_pairs(ways, bit))
        held = kept.astype(jnp.float32) + other.astype(jnp.float32)
    return held


def line_pairs(ways):
    upward = [(place, place + 1) for place in range(ways - 1)]
    return (upward, [(target, source) for source, target in upward])


def line_step(below, above, axis_name):
    upward, downward = line_pairs(lax.axis_size(axis_name))
    below.append(lax.ppermute(below[-1], axis_name, upward))
    above.append(lax.ppermute(above[-1], axis_name, downward))


def line_pick(below, above, axis_name):
    ways = lax.axis_size(axis_name)
    block = below[0]
    around = jnp.stack(below[:0:-1] + [block] + above[1:])
    picked = lax.dynamic_slice_in_dim(around, ways - 1 - lax.axis_index(axis_name), ways, 0)
    return picked.reshape((ways * block.shape[0],) + block.shape[1:])


def after(value, *others):
    return lax.optimization_barrier((value,) + others)[0]


def line_term(terms, offset, axis_name):
    place = lax.axis_index(axis_name) + offset
    place = jnp.clip(place, 0, lax.axis_size(axis_name) - 1)
    return lax.dynamic_index_in_dim(terms, place, 0, keepdims=False).astype(jnp.float32)


def line_scatter_step(terms, running, distance, axis_name, gate):
    pairs = line_pairs(lax.axis_size(axis_name))
    passed = []
    for side, sign in ((0, 1), (1, -1)):
        total = line_term(terms, sign * distance, axis_name)
        if running is not None:
            total = total + running[side].astype(jnp.float32)
        gated = after(total.astype(jnp.bfloat16), gate)
        passed.append(lax.ppermute(gated, axis_name, pairs[side]))
    return passed


def scatter_rows(term_fn, row_total):
    return lax.psum_scatter(
        term_fn(jnp.int32(0), row_total * lax.axis_size("tensor")).astype(jnp.bfloat16),
        "tensor",
        scatter_dimension=0,
        tiled=True,
    ).astype(jnp.float32)


def head_masks(axis):
    shape = (1, PAIR) if axis == 1 else (PAIR, 1)
    place = lax.broadcasted_iota(jnp.int32, shape, axis)
    first = (place < HD).astype(jnp.float32)
    return (first, 1.0 - first)


def load_heads(qkv_ref, cosine_ref, sine_ref, query_s, key_s, value_s):
    rows = qkv_ref[...].reshape(query_s.shape[0], 3 * PAIR)
    cosine, sine = cosine_ref[...], sine_ref[...]
    query_rot = rotate(rows[:, :PAIR].astype(jnp.float32), cosine, sine).astype(jnp.bfloat16)
    query_s[...] = (query_rot.astype(jnp.float32) * (1.0 / math.sqrt(HD))).astype(jnp.bfloat16)
    key_rot = rotate(rows[:, PAIR : 2 * PAIR].astype(jnp.float32), cosine, sine)
    key_s[...] = key_rot.astype(jnp.bfloat16)
    value_s[...] = rows[:, 2 * PAIR :]


def forward_kernel(qkv_ref, cosine_ref, sine_ref, mixed_ref, query_s, key_s, value_s):
    load_heads(qkv_ref, cosine_ref, sine_ref, query_s, key_s, value_s)
    pieces, _, piece_len, _ = mixed_ref.shape
    masks = head_masks(1)

    def one_piece(piece, carry):
        start = pl.multiple_of(piece * piece_len, piece_len)
        query_rows = query_s[pl.ds(start, piece_len), :]
        mixed = jnp.zeros((piece_len, PAIR), jnp.float32)
        for mask in masks:
            own_query = query_rows * mask.astype(jnp.bfloat16)
            scores = times_transpose(own_query, key_s[...])
            weights_exp = jnp.exp(scores - jnp.max(scores, axis=-1, keepdims=True))
            inverse = 1.0 / jnp.sum(weights_exp, axis=-1, keepdims=True)
            probs_low = (weights_exp * inverse).astype(jnp.bfloat16)
            part = jnp.dot(probs_low, value_s[...], preferred_element_type=jnp.float32)
            mixed = mixed + part * mask
        mixed_ref[piece, 0] = mixed.astype(jnp.bfloat16)
        return carry

    lax.fori_loop(0, pieces, one_piece, 0)


def backward_kernel(
    qkv_ref, grad_ref, cosine_ref, sine_ref, out_ref,
    query_s, key_s, value_s, turned_s, key_grad_s, value_grad_s,
):
    load_heads(qkv_ref, cosine_ref, sine_ref, query_s, key_s, value_s)
    pieces, _, piece_len, _ = grad_ref.shape
    turned_s[...] = key_s[...].astype(jnp.float32).T.astype(jnp.bfloat16)
    key_grad_s[...] = jnp.zeros_like(key_grad_s)
    value_grad_s[...] = jnp.zeros_like(value_grad_s)
    row_masks = head_masks(1)
    column_masks = head_masks(0)

    def one_piece(piece, carry):
        start = pl.multiple_of(piece * piece_len, piece_len)
        rows = pl.ds(start, piece_len)
        query_rows = query_s[rows, :]
        grad_rows = grad_ref[piece, 0]
        query_grad = jnp.zeros((PAIR, piece_len), jnp.float32)
        for mask, column_mask in zip(row_masks, column_masks):
            own_query = query_rows * mask.astype(jnp.bfloat16)
            own_grad = grad_rows * mask.astype(jnp.bfloat16)
            scores = times_transpose(key_s[...], own_query)
            weights_exp = jnp.exp(scores - jnp.max(scores, axis=0, keepdims=True))
            probs = weights_exp * (1.0 / jnp.sum(weights_exp, axis=0, keepdims=True))
            grad_probs = times_transpose(value_s[...], own_grad)
            row_dot = jnp.sum(grad_probs * probs, axis=0, keepdims=True)
            grad_scores = (probs * (grad_probs - row_dot)).astype(jnp.bfloat16)
            value_grad_s[...] += jnp.dot(
                probs.astype(jnp.bfloat16), own_grad, preferred_element_type=jnp.float32
            )
            key_grad_s[...] += jnp.dot(grad_scores, own_query, preferred_element_type=jnp.float32)
            own_turned = turned_s[...] * column_mask.astype(jnp.bfloat16)
            query_grad = query_grad + jnp.dot(
                own_turned, grad_scores, preferred_element_type=jnp.float32
            )
        query_grad = query_grad.T * (1.0 / math.sqrt(HD))
        turned = rotate_back(query_grad, cosine_ref[rows, :], sine_ref[rows, :])
        out_ref[piece, 0, :, :PAIR] = turned.astype(jnp.bfloat16)
        return carry

    lax.fori_loop(0, pieces, one_piece, 0)
    piece_shape = (pieces, 1, piece_len, PAIR)
    key_grad = rotate_back(key_grad_s[...], cosine_ref[...], sine_ref[...])
    out_ref[:, :, :, PAIR : 2 * PAIR] = key_grad.astype(jnp.bfloat16).reshape(piece_shape)
    out_ref[:, :, :, 2 * PAIR :] = value_grad_s[...].astype(jnp.bfloat16).reshape(piece_shape)


def attention_call(kernel, qkv, extra, tables, out_lanes, more_scratch, products):
    pieces, seq_count, piece_len, lanes = qkv.shape
    pair_count = lanes // (3 * PAIR)
    length = pieces * piece_len

    def per_pair(wide):
        return pl.BlockSpec((pieces, 1, piece_len, wide), lambda seq, pair: (0, seq, 0, pair))

    table_spec = pl.BlockSpec((length, PAIR), lambda seq, pair: (0, 0))
    blocks = seq_count * pair_count
    return pl.pallas_call(
        kernel,
        grid=(seq_count, pair_count),
        in_specs=[per_pair(3 * PAIR)] + [per_pair(PAIR)] * len(extra) + [table_spec] * 2,
        out_specs=per_pair(out_lanes),
        out_shape=jax.ShapeDtypeStruct(
            (pieces, seq_count, piece_len, pair_count * out_lanes), jnp.bfloat16
        ),
        scratch_shapes=[pltpu.VMEM((length, PAIR), jnp.bfloat16)] * 3 + more_scratch,
        compiler_params=pltpu.CompilerParams(vmem_limit_bytes=48 << 20),
        cost_estimate=pl.CostEstimate(
            flops=blocks * products * 4 * length * length * PAIR,
            bytes_accessed=blocks * length * PAIR * 16,
            transcendentals=blocks * 2 * length * length,
        ),
    )(qkv, *extra, *tables)


def attend_forward(qkv, tables):
    return attention_call(forward_kernel, qkv, (), tables, PAIR, [], 2)


def attend_backward(qkv, grad_mixed, tables):
    length = qkv.shape[0] * qkv.shape[2]
    more = [
        pltpu.VMEM((PAIR, length), jnp.bfloat16),
        pltpu.VMEM((length, PAIR), jnp.float32),
        pltpu.VMEM((length, PAIR), jnp.float32),
    ]
    return attention_call(backward_kernel, qkv, (grad_mixed,), tables, 3 * PAIR, more, 5)


def hidden_forward(token_rows, gate_part, up_part, gate_shift, up_shift, unit_mask):
    gate_pre = jnp.dot(token_rows, gate_part, preferred_element_type=jnp.float32) + gate_shift
    up_pre = jnp.dot(token_rows, up_part, preferred_element_type=jnp.float32) + up_shift
    return (gate_pre, up_pre, jax.nn.silu(gate_pre) * up_pre * unit_mask)


def inner_normalize(hidden, first_sum, second_sum, inner_scale, inner_offset, unit_mask):
    unit_mean = first_sum[:, None] / FF_REAL
    unit_var = second_sum[:, None] / FF_REAL - unit_mean * unit_mean
    inv_std = lax.rsqrt(unit_var + norm_eps)
    unit_hidden = (hidden - unit_mean) * inv_std
    normed = ((unit_hidden * inner_scale + inner_offset) * unit_mask).astype(jnp.bfloat16)
    return (normed, unit_hidden, inv_std)


def hidden_backward_terms(grad_normed, unit_hidden, inner_scale, unit_mask):
    scaled = grad_normed * unit_mask * inner_scale
    return (scaled, jnp.sum(scaled, axis=-1), jnp.sum(scaled * unit_hidden, axis=-1))


def gate_grads(scaled, scaled_sum, cross_sum, unit_hidden, inv_std, gate_pre, up_pre, unit_mask):
    grad_hidden = (
        unit_mask
        * (scaled - scaled_sum[:, None] / FF_REAL - unit_hidden * cross_sum[:, None] / FF_REAL)
        * inv_std
    )
    sigmoid_gate = jax.nn.sigmoid(gate_pre)
    grad_gate = (
        grad_hidden * up_pre * sigmoid_gate * (1.0 + gate_pre * (1.0 - sigmoid_gate))
    ).astype(jnp.bfloat16)
    grad_up = (grad_hidden * gate_pre * sigmoid_gate).astype(jnp.bfloat16)
    return (grad_gate, grad_up)


def vector_sums(grad_gate, grad_up, grad_normed, unit_hidden, unit_mask):
    return (
        jnp.sum(grad_gate, axis=0, dtype=jnp.float32),
        jnp.sum(grad_up, axis=0, dtype=jnp.float32),
        jnp.sum(grad_normed * unit_mask * unit_hidden, axis=0),
        jnp.sum(grad_normed * unit_mask, axis=0),
    )


def on_device(
    inputs,
    slot_flag,
    cotangent,
    first_gain,
    first_shift,
    query_weight,
    query_bias,
    key_weight,
    value_weight,
    value_bias,
    out_weight,
    out_bias,
    second_gain,
    second_shift,
    gate_weight,
    gate_bias,
    up_weight,
    up_bias,
    inner_gain,
    inner_shift,
    down_weight,
    down_bias,
):
    seq_local, piece_len, width = inputs.shape
    head_ways = lax.axis_size("heads")
    group_width = width // head_ways
    group_pairs = group_width // PAIR
    token_count = seq_local * piece_len
    fsdp_ways, tensor_ways = lax.axis_size("fsdp"), lax.axis_size("tensor")
    row_part = query_weight.shape[0]
    group_index = lax.axis_index("heads")
    inputs_group = cube_gather(inputs, "heads")
    grad_flags = slot_flag.astype(jnp.float32)[:, None, None]
    grad_total = grad_flags * cotangent.astype(jnp.float32)
    grad_branch = grad_total.astype(jnp.bfloat16)
    below, above = [grad_branch], [grad_branch]
    line_step(below, above, "tensor")
    below[-1], above[-1] = after(below[-1], inputs_group), after(above[-1], inputs_group)
    line_step(below, above, "tensor")
    stacked = jnp.stack(
        [
            member.reshape(row_part, head_ways, group_pairs, PAIR)
            for member in (query_weight, key_weight, value_weight)
        ],
        axis=3,
    ).reshape(row_part, head_ways, 3 * group_width)
    vectors = (
        first_gain,
        first_shift,
        query_bias,
        value_bias,
        out_bias,
        second_gain,
        second_shift,
        down_bias,
    )
    row_lanes = 3 * group_width
    vector_row = jnp.zeros((row_lanes,), jnp.float32)
    for place, member in enumerate(vectors):
        ahead = place * row_part
        vector_row = vector_row + jnp.pad(
            member.astype(jnp.float32), (ahead, row_lanes - ahead - row_part)
        )
    vector_row = vector_row.astype(jnp.bfloat16)
    sent_columns = jnp.concatenate(
        [
            stacked.transpose(1, 0, 2),
            jnp.broadcast_to(vector_row, (head_ways, 1, 3 * group_width)),
        ],
        axis=1,
    )
    own_columns = lax.all_to_all(
        sent_columns, "heads", split_axis=0, concat_axis=0, tiled=True
    )
    columns = lax.all_gather(
        own_columns.reshape(-1, 3 * group_width), ("fsdp", "tensor"), axis=0, tiled=True
    )
    group_f = inputs_group.reshape(-1, width).astype(jnp.float32)
    group_mean = jnp.mean(group_f, axis=-1, keepdims=True)
    group_var = jnp.mean(jnp.square(group_f - group_mean), axis=-1, keepdims=True)
    group_inv = lax.rsqrt(group_var + norm_eps)
    columns, group_mean, group_inv = lax.optimization_barrier((columns, group_mean, group_inv))
    columns = columns.reshape(
        fsdp_ways, tensor_ways, head_ways, row_part + 1, 3 * group_width
    ).transpose(0, 2, 1, 3, 4)
    qkv_part = columns[:, :, :, :row_part].reshape(width, 3 * group_width)
    below[-1], above[-1] = after(below[-1], columns), after(above[-1], columns)
    line_step(below, above, "tensor")
    gathered = (
        columns[:, :, :, row_part, : len(vectors) * row_part]
        .reshape(-1, 8, row_part)
        .transpose(1, 0, 2)
        .reshape(8, width)
    )
    out_below, out_above = [out_weight], [out_weight]
    for _ in range(tensor_ways - 1):
        line_step(out_below, out_above, "tensor")
    out_full = lax.all_gather(
        line_pick(out_below, out_above, "tensor"),
        ("fsdp", "heads"),
        axis=0,
        tiled=True,
    )
    gain_one, shift_one, query_shift, value_shift, out_shift, gain_two, shift_two, down_shift = [
        member.astype(jnp.float32) for member in gathered
    ]
    gate_part, up_part, down_part = (
        lax.all_gather(gate_weight, ("fsdp", "heads"), axis=0, tiled=True),
        lax.all_gather(up_weight, ("fsdp", "heads"), axis=0, tiled=True),
        lax.all_gather(down_weight, ("fsdp", "heads"), axis=1, tiled=True),
    )
    inputs_f = inputs.astype(jnp.float32)
    _, unit_one, inv_one = layer_norm(inputs_f, gain_one, shift_one)
    unit_group = (group_f - group_mean) * group_inv
    low_one = (unit_group * gain_one + shift_one).astype(jnp.bfloat16)

    def group_lanes(full_vec):
        own = lax.dynamic_slice_in_dim(full_vec, group_index * group_width, group_width, 0)
        return own.reshape(group_pairs, PAIR)

    query_lanes, value_lanes = group_lanes(query_shift), group_lanes(value_shift)
    qkv_shift = jnp.stack([query_lanes, jnp.zeros_like(query_lanes), value_lanes], axis=1)
    qkv_lin = (
        (jnp.dot(low_one, qkv_part, preferred_element_type=jnp.float32) + qkv_shift.reshape(-1))
        .astype(jnp.bfloat16)
        .reshape(head_ways, seq_local, piece_len, 3 * group_width)
    )
    tables = tuple(jnp.tile(table, (1, PAIR // HD)) for table in rope_tables())
    mixed_heads = attend_forward(qkv_lin, tables)
    mixed_heads, below[-1], above[-1] = lax.optimization_barrier(
        (mixed_heads, below[-1], above[-1])
    )
    for _ in range(tensor_ways - 4):
        line_step(below, above, "tensor")
    mixed_parts = lax.all_to_all(mixed_heads, "heads", split_axis=0, concat_axis=0, tiled=True)
    grad_rows = line_pick(below, above, "tensor").reshape(-1, width)
    mixed_flat = mixed_parts.transpose(1, 2, 0, 3).reshape(token_count, width)
    residual = inputs_f + (
        jnp.dot(mixed_flat, out_full, preferred_element_type=jnp.float32) + out_shift
    ).reshape(inputs.shape)
    normed_two, unit_two, inv_two = layer_norm(residual, gain_two, shift_two)
    low_two = normed_two.astype(jnp.bfloat16)
    flag_rows = slot_flag.astype(jnp.float32)[:, None, None]
    down_shift_grad = jnp.sum(grad_branch.reshape(token_count, width), axis=0, dtype=jnp.float32)
    ffn_local = gate_part.shape[1]
    token_rows3 = gather_rows(after(low_two, gate_part, up_part, below[-1], above[-1]))
    token_rows = token_rows3.reshape(-1, width)
    col_index = lax.axis_index("tensor") * ffn_local + jnp.arange(ffn_local, dtype=jnp.int32)
    unit_mask = (col_index < FF_REAL).astype(jnp.float32)
    gate_pre, up_pre, hidden = hidden_forward(
        token_rows,
        gate_part,
        up_part,
        gate_bias.astype(jnp.float32),
        up_bias.astype(jnp.float32),
        unit_mask,
    )
    first_sum, second_sum = tensor_sums(jnp.sum(hidden, axis=-1), jnp.sum(hidden * hidden, axis=-1))
    inner_scale = inner_gain.astype(jnp.float32)
    normed_hidden, unit_hidden, inv_hidden = inner_normalize(
        hidden, first_sum, second_sum, inner_scale, inner_shift.astype(jnp.float32), unit_mask
    )
    hidden_seqs = normed_hidden.reshape(token_rows3.shape[0], piece_len, ffn_local)

    def down_term(row_count):
        picked = hidden_seqs.reshape(-1, ffn_local)
        return jnp.dot(picked, down_part, preferred_element_type=jnp.float32).reshape(
            row_count, piece_len, width
        )

    down_grad = outer_product(normed_hidden, grad_rows)
    down_weight_grad = lax.psum_scatter(
        down_grad.astype(jnp.bfloat16), ("fsdp", "heads"), scatter_dimension=1, tiled=True
    )
    grad_normed = times_transpose(after(grad_rows, down_grad), down_part)
    scaled, scaled_sum, cross_sum = hidden_backward_terms(
        grad_normed, unit_hidden, inner_scale, unit_mask
    )
    scaled_sum, cross_sum = tensor_sums(scaled_sum, cross_sum)
    grad_gate, grad_up = gate_grads(
        scaled, scaled_sum, cross_sum, unit_hidden, inv_hidden, gate_pre, up_pre, unit_mask
    )
    gate_grad = outer_product(token_rows, grad_gate)
    up_grad = outer_product(token_rows, grad_up)
    vector_grads = vector_sums(grad_gate, grad_up, grad_normed, unit_hidden, unit_mask)
    gate_seqs = after(grad_gate, down_weight_grad).reshape(-1, piece_len, ffn_local)
    up_seqs = grad_up.reshape(-1, piece_len, ffn_local)

    def input_term(row_start, row_count):
        picked_gate = gate_seqs.reshape(-1, ffn_local)
        picked_up = up_seqs.reshape(-1, ffn_local)
        summed = times_transpose(picked_gate, gate_part) + times_transpose(picked_up, up_part)
        return summed.reshape(row_count, piece_len, width)

    grad_normed_two = scatter_rows(input_term, seq_local)
    gate_weight_grad, up_weight_grad = (
        lax.psum_scatter(
            gate_grad.astype(jnp.bfloat16), ("fsdp", "heads"), scatter_dimension=0, tiled=True
        ).astype(jnp.float32),
        lax.psum_scatter(
            up_grad.astype(jnp.bfloat16), ("fsdp", "heads"), scatter_dimension=0, tiled=True
        ).astype(jnp.float32),
    )
    down_weight_grad = down_weight_grad.astype(jnp.float32)
    gate_bias_grad, up_bias_grad, inner_gain_grad, inner_shift_grad = lax.psum(
        (vector_grads[0], vector_grads[1], vector_grads[2], vector_grads[3]), ("fsdp", "heads")
    )
    grad_normed_two = after(grad_normed_two, gate_bias_grad)
    grad_residual = grad_total + norm_backward(grad_normed_two, unit_two, inv_two, gain_two)
    gain_two_grad = jnp.sum((grad_normed_two * unit_two).reshape(token_count, width), axis=0)
    shift_two_grad = jnp.sum(grad_normed_two.reshape(token_count, width), axis=0)
    grad_attn = grad_residual.astype(jnp.bfloat16).reshape(token_count, width)
    out_weight_part = outer_product(mixed_flat, grad_attn)
    out_shift_grad = jnp.sum(grad_attn, axis=0, dtype=jnp.float32)
    grad_mixed = times_transpose(grad_attn, out_full).astype(jnp.bfloat16)
    grad_parts = grad_mixed.reshape(seq_local, piece_len, head_ways, group_width)
    grad_heads = lax.all_to_all(
        grad_parts.transpose(2, 0, 1, 3), "heads", split_axis=0, concat_axis=0, tiled=True
    )
    branch_terms = down_term(seq_local * tensor_ways).astype(jnp.bfloat16)
    branch_terms = branch_terms.reshape((tensor_ways,) + inputs.shape)
    running = line_scatter_step(branch_terms, None, tensor_ways - 1, "tensor", grad_mixed)
    qkv_grad = attend_backward(qkv_lin, grad_heads, tables)
    qkv_grad = after(qkv_grad, *running)
    for distance in range(tensor_ways - 2, 0, -1):
        running = line_scatter_step(branch_terms, running, distance, "tensor", qkv_grad)
    branch_out = (
        line_term(branch_terms, 0, "tensor")
        + running[0].astype(jnp.float32)
        + running[1].astype(jnp.float32)
    )
    output = (flag_rows * (residual + branch_out + down_shift)).astype(jnp.bfloat16)
    qkv_grad = qkv_grad.reshape(head_ways * token_count, 3 * group_width)
    group_grad = times_transpose(qkv_grad, qkv_part)
    gain_one_grad = jnp.sum(group_grad * unit_group, axis=0)
    shift_one_grad = jnp.sum(group_grad, axis=0)
    group_terms = group_grad.astype(jnp.bfloat16)
    grad_normed_one = cube_scatter(
        group_terms.reshape((head_ways,) + inputs.shape), "heads"
    )
    qkv_shift_grad = jnp.sum(qkv_grad, axis=0, dtype=jnp.float32).reshape(group_pairs, 3, PAIR)

    def place_lanes(own_lanes):
        return lax.dynamic_update_slice_in_dim(
            jnp.zeros((width,), jnp.float32), own_lanes.reshape(-1), group_index * group_width, 0
        )

    query_shift_grad = place_lanes(qkv_shift_grad[:, 0])
    value_shift_grad = place_lanes(qkv_shift_grad[:, 2])
    input_grad = (
        grad_residual + norm_backward(grad_normed_one, unit_one, inv_one, gain_one)
    ).astype(jnp.bfloat16)
    vector_terms = jnp.stack(
        [
            gain_one_grad,
            shift_one_grad,
            query_shift_grad,
            value_shift_grad,
            out_shift_grad,
            gain_two_grad,
            shift_two_grad,
            down_shift_grad,
        ]
    )
    vector_lanes = vector_terms.shape[0] * row_part
    vector_rows = (
        vector_terms.reshape(-1, fsdp_ways, head_ways, tensor_ways, row_part)
        .transpose(1, 3, 2, 0, 4)
        .reshape(fsdp_ways, tensor_ways, head_ways, 1, vector_lanes)
    )
    extra_rows = 1
    while head_ways * (row_part + extra_rows) % 16 != 0:
        extra_rows += 1
    vector_rows = jnp.pad(
        vector_rows,
        ((0, 0),) * 3 + ((0, extra_rows - 1), (0, 3 * group_width - vector_lanes)),
    )
    qkv_terms = outer_product(low_one, qkv_grad).astype(jnp.bfloat16)
    qkv_terms = qkv_terms.reshape(
        fsdp_ways, head_ways, tensor_ways, row_part, 3 * group_width
    ).transpose(0, 2, 1, 3, 4)
    qkv_terms = jnp.concatenate([qkv_terms, vector_rows.astype(jnp.bfloat16)], axis=3)
    qkv_half = cube_scatter(
        qkv_terms.reshape(fsdp_ways, -1, 3 * group_width), "fsdp"
    ).astype(jnp.bfloat16)
    qkv_rows = lax.psum_scatter(qkv_half, "tensor", scatter_dimension=0, tiled=True)
    qkv_columns = lax.all_to_all(
        qkv_rows, "heads", split_axis=0, concat_axis=0, tiled=True
    ).reshape(head_ways, row_part + extra_rows, 3 * group_width)
    qkv_weight_grads = (
        qkv_columns[:, :row_part]
        .reshape(head_ways, row_part, group_pairs, 3, PAIR)
        .transpose(3, 1, 0, 2, 4)
        .reshape(3, row_part, width)
        .astype(jnp.float32)
    )
    own_sums = jnp.sum(
        qkv_columns[:, row_part, :vector_lanes].astype(jnp.float32), axis=0
    ).reshape(-1, row_part)
    out_terms = out_weight_part.astype(jnp.bfloat16).reshape(fsdp_ways, -1, width)
    out_half = cube_scatter(out_terms, "fsdp").astype(jnp.bfloat16)
    out_eighth = cube_scatter(out_half.reshape(head_ways, -1, width), "heads")
    out_weight_grad = lax.psum_scatter(
        out_eighth.astype(jnp.bfloat16), "tensor", scatter_dimension=0, tiled=True
    ).astype(jnp.float32)
    attn_sums = tuple(qkv_weight_grads) + (out_weight_grad,) + tuple(own_sums)
    return (
        output,
        input_grad,
        attn_sums[4],
        attn_sums[5],
        attn_sums[0],
        attn_sums[6],
        attn_sums[1],
        attn_sums[2],
        attn_sums[7],
        attn_sums[3],
        attn_sums[8],
        attn_sums[9],
        attn_sums[10],
        gate_weight_grad,
        gate_bias_grad,
        up_weight_grad,
        up_bias_grad,
        inner_gain_grad,
        inner_shift_grad,
        down_weight_grad,
        attn_sums[11],
    )


def solution(mesh):
    return jax.shard_map(
        on_device,
        mesh=mesh,
        in_specs=(
            P(("fsdp", "tensor"), "heads", None),
            P(("fsdp", "tensor")),
            P(("fsdp", "tensor"), "heads", None),
            P(("fsdp", "heads", "tensor")),
            P(("fsdp", "heads", "tensor")),
            P(("fsdp", "heads", "tensor"), None),
            P(("fsdp", "heads", "tensor")),
            P(("fsdp", "heads", "tensor"), None),
            P(("fsdp", "heads", "tensor"), None),
            P(("fsdp", "heads", "tensor")),
            P(("fsdp", "heads", "tensor"), None),
            P(("fsdp", "heads", "tensor")),
            P(("fsdp", "heads", "tensor")),
            P(("fsdp", "heads", "tensor")),
            P(("fsdp", "heads"), "tensor"),
            P("tensor"),
            P(("fsdp", "heads"), "tensor"),
            P("tensor"),
            P("tensor"),
            P("tensor"),
            P("tensor", ("fsdp", "heads")),
            P(("fsdp", "heads", "tensor")),
        ),
        out_specs=(
            P(("fsdp", "tensor"), "heads", None),
            P(("fsdp", "tensor"), "heads", None),
            P(("fsdp", "heads", "tensor")),
            P(("fsdp", "heads", "tensor")),
            P(("fsdp", "heads", "tensor"), None),
            P(("fsdp", "heads", "tensor")),
            P(("fsdp", "heads", "tensor"), None),
            P(("fsdp", "heads", "tensor"), None),
            P(("fsdp", "heads", "tensor")),
            P(("fsdp", "heads", "tensor"), None),
            P(("fsdp", "heads", "tensor")),
            P(("fsdp", "heads", "tensor")),
            P(("fsdp", "heads", "tensor")),
            P(("fsdp", "heads"), "tensor"),
            P("tensor"),
            P(("fsdp", "heads"), "tensor"),
            P("tensor"),
            P("tensor"),
            P("tensor"),
            P("tensor", ("fsdp", "heads")),
            P(("fsdp", "heads", "tensor")),
        ),
        check_vma=False,
    )
```

```python
import math

import jax
import jax.numpy as jnp
from jax import lax
from jax.experimental import pallas as pl
from jax.experimental.pallas import tpu as pltpu
from jax.sharding import PartitionSpec as P


FSDP, HEADS, TENSOR = "fsdp", "heads", "tensor"
HD = 64
PAIR = 2 * HD
FF_REAL = 2730
GRID = 32


norm_eps = 1e-06


def layer_norm(values, gain_vec, shift_vec):
    row_mean = jnp.mean(values, axis=-1, keepdims=True)
    centered = values - row_mean
    row_var = jnp.mean(centered * centered, axis=-1, keepdims=True)
    inv_std = lax.rsqrt(row_var + norm_eps)
    unit_rows = centered * inv_std
    return (unit_rows * gain_vec + shift_vec, unit_rows, inv_std)


def norm_backward(grad_values, unit_rows, inv_std, gain_vec):
    scaled = grad_values * gain_vec
    centered = scaled - jnp.mean(scaled, axis=-1, keepdims=True)
    centered = centered - unit_rows * jnp.mean(scaled * unit_rows, axis=-1, keepdims=True)
    return centered * inv_std


def rope_tables():
    positions = jnp.arange(GRID * GRID, dtype=jnp.int32)
    row_place = (positions // GRID).astype(jnp.float32)
    col_place = (positions % GRID).astype(jnp.float32)
    quarter = HD // 4
    frequency = jnp.power(10000.0, -jnp.arange(quarter, dtype=jnp.float32) / quarter)
    angles = jnp.concatenate(
        [row_place[:, None] * frequency[None, :], col_place[:, None] * frequency[None, :]], axis=1
    )
    angles = jnp.repeat(angles, 2, axis=1)
    return (jnp.cos(angles), jnp.sin(angles))


def pair_swap(values):
    count = values.shape[-1]
    lanes = lax.broadcasted_iota(jnp.int32, values.shape, 1)
    following = pltpu.roll(values, count - 1, 1)
    preceding = pltpu.roll(values, 1, 1)
    return jnp.where(lanes % 2 == 0, -following, preceding)


def rotate(values, cosine_table, sine_table):
    return values * cosine_table + pair_swap(values) * sine_table


def rotate_back(grad_values, cosine_table, sine_table):
    return grad_values * cosine_table - pair_swap(grad_values * sine_table)


def outer_product(left_rows, right_rows):
    return lax.dot_general(
        left_rows, right_rows, (((0,), (0,)), ((), ())), preferred_element_type=jnp.float32
    )


def times_transpose(left_rows, right_rows):
    return lax.dot_general(
        left_rows, right_rows, (((1,), (1,)), ((), ())), preferred_element_type=jnp.float32
    )


def gather_rows(block_values):
    return lax.all_gather(block_values, TENSOR, axis=0, tiled=True)


def tensor_sums(first_sum, second_sum):
    both = lax.psum(jnp.stack([first_sum, second_sum]).astype(jnp.bfloat16), TENSOR)
    return (both[0].astype(jnp.float32), both[1].astype(jnp.float32))


def cube_pairs(ways, bit):
    return [(place, place ^ (1 << bit)) for place in range(ways)]


def cube_gather(block, axis_name):
    ways = lax.axis_size(axis_name)
    bits = ways.bit_length() - 1
    index = lax.axis_index(axis_name)
    held = block.reshape((1,) * bits + block.shape)
    for bit in reversed(range(bits)):
        place = bits - 1 - bit
        other = lax.ppermute(held, axis_name, cube_pairs(ways, bit))
        held = jnp.where(
            (index >> bit) % 2 == 0,
            jnp.concatenate([held, other], axis=place),
            jnp.concatenate([other, held], axis=place),
        )
    return held.reshape((ways * block.shape[0],) + block.shape[1:])


def cube_scatter(terms, axis_name):
    ways = lax.axis_size(axis_name)
    bits = ways.bit_length() - 1
    index = lax.axis_index(axis_name)
    held = terms.reshape((2,) * bits + terms.shape[1:])
    for bit in range(bits):
        place = bits - 1 - bit
        mine = (index >> bit) % 2
        kept = lax.dynamic_index_in_dim(held, mine, place, keepdims=False)
        sent = lax.dynamic_index_in_dim(held, 1 - mine, place, keepdims=False)
        other = lax.ppermute(sent.astype(jnp.bfloat16), axis_name, cube_pairs(ways, bit))
        held = kept.astype(jnp.float32) + other.astype(jnp.float32)
    return held


def line_pairs(ways):
    upward = [(place, place + 1) for place in range(ways - 1)]
    return (upward, [(target, source) for source, target in upward])


def line_step(below, above, axis_name):
    upward, downward = line_pairs(lax.axis_size(axis_name))
    below.append(lax.ppermute(below[-1], axis_name, upward))
    above.append(lax.ppermute(above[-1], axis_name, downward))


def line_pick(below, above, axis_name):
    ways = lax.axis_size(axis_name)
    block = below[0]
    around = jnp.stack(below[:0:-1] + [block] + above[1:])
    picked = lax.dynamic_slice_in_dim(around, ways - 1 - lax.axis_index(axis_name), ways, 0)
    return picked.reshape((ways * block.shape[0],) + block.shape[1:])


def after(value, *others):
    return lax.optimization_barrier((value,) + others)[0]


def line_term(terms, offset, axis_name):
    place = lax.axis_index(axis_name) + offset
    place = jnp.clip(place, 0, lax.axis_size(axis_name) - 1)
    return lax.dynamic_index_in_dim(terms, place, 0, keepdims=False).astype(jnp.float32)


def line_scatter_step(terms, running, distance, axis_name, gate):
    pairs = line_pairs(lax.axis_size(axis_name))
    passed = []
    for side, sign in ((0, 1), (1, -1)):
        total = line_term(terms, sign * distance, axis_name)
        if running is not None:
            total = total + running[side].astype(jnp.float32)
        gated = after(total.astype(jnp.bfloat16), gate)
        passed.append(lax.ppermute(gated, axis_name, pairs[side]))
    return passed


def scatter_rows(term_fn, row_total):
    return lax.psum_scatter(
        term_fn(jnp.int32(0), row_total * lax.axis_size(TENSOR)).astype(jnp.bfloat16),
        TENSOR,
        scatter_dimension=0,
        tiled=True,
    ).astype(jnp.float32)


def head_masks(axis):
    shape = (1, PAIR) if axis == 1 else (PAIR, 1)
    place = lax.broadcasted_iota(jnp.int32, shape, axis)
    first = (place < HD).astype(jnp.float32)
    return (first, 1.0 - first)


def load_heads(qkv_ref, cosine_ref, sine_ref, query_s, key_s, value_s):
    rows = qkv_ref[...].reshape(query_s.shape[0], 3 * PAIR)
    cosine, sine = cosine_ref[...], sine_ref[...]
    query_rot = rotate(rows[:, :PAIR].astype(jnp.float32), cosine, sine).astype(jnp.bfloat16)
    query_s[...] = (query_rot.astype(jnp.float32) * (1.0 / math.sqrt(HD))).astype(jnp.bfloat16)
    key_rot = rotate(rows[:, PAIR : 2 * PAIR].astype(jnp.float32), cosine, sine)
    key_s[...] = key_rot.astype(jnp.bfloat16)
    value_s[...] = rows[:, 2 * PAIR :]


def forward_kernel(qkv_ref, cosine_ref, sine_ref, mixed_ref, query_s, key_s, value_s):
    load_heads(qkv_ref, cosine_ref, sine_ref, query_s, key_s, value_s)
    pieces, _, piece_len, _ = mixed_ref.shape
    masks = head_masks(1)

    def one_piece(piece, carry):
        start = pl.multiple_of(piece * piece_len, piece_len)
        query_rows = query_s[pl.ds(start, piece_len), :]
        mixed = jnp.zeros((piece_len, PAIR), jnp.float32)
        for mask in masks:
            own_query = query_rows * mask.astype(jnp.bfloat16)
            scores = times_transpose(own_query, key_s[...])
            weights_exp = jnp.exp(scores - jnp.max(scores, axis=-1, keepdims=True))
            inverse = 1.0 / jnp.sum(weights_exp, axis=-1, keepdims=True)
            probs_low = (weights_exp * inverse).astype(jnp.bfloat16)
            part = jnp.dot(probs_low, value_s[...], preferred_element_type=jnp.float32)
            mixed = mixed + part * mask
        mixed_ref[piece, 0] = mixed.astype(jnp.bfloat16)
        return carry

    lax.fori_loop(0, pieces, one_piece, 0)


def backward_kernel(
    qkv_ref, grad_ref, cosine_ref, sine_ref, out_ref,
    query_s, key_s, value_s, turned_s, key_grad_s, value_grad_s,
):
    load_heads(qkv_ref, cosine_ref, sine_ref, query_s, key_s, value_s)
    pieces, _, piece_len, _ = grad_ref.shape
    turned_s[...] = key_s[...].astype(jnp.float32).T.astype(jnp.bfloat16)
    key_grad_s[...] = jnp.zeros_like(key_grad_s)
    value_grad_s[...] = jnp.zeros_like(value_grad_s)
    row_masks = head_masks(1)
    column_masks = head_masks(0)

    def one_piece(piece, carry):
        start = pl.multiple_of(piece * piece_len, piece_len)
        rows = pl.ds(start, piece_len)
        query_rows = query_s[rows, :]
        grad_rows = grad_ref[piece, 0]
        query_grad = jnp.zeros((PAIR, piece_len), jnp.float32)
        for mask, column_mask in zip(row_masks, column_masks):
            own_query = query_rows * mask.astype(jnp.bfloat16)
            own_grad = grad_rows * mask.astype(jnp.bfloat16)
            scores = times_transpose(key_s[...], own_query)
            weights_exp = jnp.exp(scores - jnp.max(scores, axis=0, keepdims=True))
            probs = weights_exp * (1.0 / jnp.sum(weights_exp, axis=0, keepdims=True))
            grad_probs = times_transpose(value_s[...], own_grad)
            row_dot = jnp.sum(grad_probs * probs, axis=0, keepdims=True)
            grad_scores = (probs * (grad_probs - row_dot)).astype(jnp.bfloat16)
            value_grad_s[...] += jnp.dot(
                probs.astype(jnp.bfloat16), own_grad, preferred_element_type=jnp.float32
            )
            key_grad_s[...] += jnp.dot(grad_scores, own_query, preferred_element_type=jnp.float32)
            own_turned = turned_s[...] * column_mask.astype(jnp.bfloat16)
            query_grad = query_grad + jnp.dot(
                own_turned, grad_scores, preferred_element_type=jnp.float32
            )
        query_grad = query_grad.T * (1.0 / math.sqrt(HD))
        turned = rotate_back(query_grad, cosine_ref[rows, :], sine_ref[rows, :])
        out_ref[piece, 0, :, :PAIR] = turned.astype(jnp.bfloat16)
        return carry

    lax.fori_loop(0, pieces, one_piece, 0)
    piece_shape = (pieces, 1, piece_len, PAIR)
    key_grad = rotate_back(key_grad_s[...], cosine_ref[...], sine_ref[...])
    out_ref[:, :, :, PAIR : 2 * PAIR] = key_grad.astype(jnp.bfloat16).reshape(piece_shape)
    out_ref[:, :, :, 2 * PAIR :] = value_grad_s[...].astype(jnp.bfloat16).reshape(piece_shape)


def attention_call(kernel, qkv, extra, tables, out_lanes, more_scratch, products):
    pieces, seq_count, piece_len, lanes = qkv.shape
    pair_count = lanes // (3 * PAIR)
    length = pieces * piece_len

    def per_pair(wide):
        return pl.BlockSpec((pieces, 1, piece_len, wide), lambda seq, pair: (0, seq, 0, pair))

    table_spec = pl.BlockSpec((length, PAIR), lambda seq, pair: (0, 0))
    blocks = seq_count * pair_count
    return pl.pallas_call(
        kernel,
        grid=(seq_count, pair_count),
        in_specs=[per_pair(3 * PAIR)] + [per_pair(PAIR)] * len(extra) + [table_spec] * 2,
        out_specs=per_pair(out_lanes),
        out_shape=jax.ShapeDtypeStruct(
            (pieces, seq_count, piece_len, pair_count * out_lanes), jnp.bfloat16
        ),
        scratch_shapes=[pltpu.VMEM((length, PAIR), jnp.bfloat16)] * 3 + more_scratch,
        compiler_params=pltpu.CompilerParams(vmem_limit_bytes=48 << 20),
        cost_estimate=pl.CostEstimate(
            flops=blocks * products * 4 * length * length * PAIR,
            bytes_accessed=blocks * length * PAIR * 16,
            transcendentals=blocks * 2 * length * length,
        ),
    )(qkv, *extra, *tables)


def attend_forward(qkv, tables):
    return attention_call(forward_kernel, qkv, (), tables, PAIR, [], 2)


def attend_backward(qkv, grad_mixed, tables):
    length = qkv.shape[0] * qkv.shape[2]
    more = [
        pltpu.VMEM((PAIR, length), jnp.bfloat16),
        pltpu.VMEM((length, PAIR), jnp.float32),
        pltpu.VMEM((length, PAIR), jnp.float32),
    ]
    return attention_call(backward_kernel, qkv, (grad_mixed,), tables, 3 * PAIR, more, 5)


def hidden_forward(token_rows, gate_part, up_part, gate_shift, up_shift, unit_mask):
    gate_pre = jnp.dot(token_rows, gate_part, preferred_element_type=jnp.float32) + gate_shift
    up_pre = jnp.dot(token_rows, up_part, preferred_element_type=jnp.float32) + up_shift
    return (gate_pre, up_pre, jax.nn.silu(gate_pre) * up_pre * unit_mask)


def inner_normalize(hidden, first_sum, second_sum, inner_scale, inner_offset, unit_mask):
    unit_mean = first_sum[:, None] / FF_REAL
    unit_var = second_sum[:, None] / FF_REAL - unit_mean * unit_mean
    inv_std = lax.rsqrt(unit_var + norm_eps)
    unit_hidden = (hidden - unit_mean) * inv_std
    normed = ((unit_hidden * inner_scale + inner_offset) * unit_mask).astype(jnp.bfloat16)
    return (normed, unit_hidden, inv_std)


def hidden_backward_terms(grad_normed, unit_hidden, inner_scale, unit_mask):
    scaled = grad_normed * unit_mask * inner_scale
    return (scaled, jnp.sum(scaled, axis=-1), jnp.sum(scaled * unit_hidden, axis=-1))


def gate_grads(scaled, scaled_sum, cross_sum, unit_hidden, inv_std, gate_pre, up_pre, unit_mask):
    grad_hidden = (
        unit_mask
        * (scaled - scaled_sum[:, None] / FF_REAL - unit_hidden * cross_sum[:, None] / FF_REAL)
        * inv_std
    )
    sigmoid_gate = jax.nn.sigmoid(gate_pre)
    grad_gate = (
        grad_hidden * up_pre * sigmoid_gate * (1.0 + gate_pre * (1.0 - sigmoid_gate))
    ).astype(jnp.bfloat16)
    grad_up = (grad_hidden * gate_pre * sigmoid_gate).astype(jnp.bfloat16)
    return (grad_gate, grad_up)


def vector_sums(grad_gate, grad_up, grad_normed, unit_hidden, unit_mask):
    return (
        jnp.sum(grad_gate, axis=0, dtype=jnp.float32),
        jnp.sum(grad_up, axis=0, dtype=jnp.float32),
        jnp.sum(grad_normed * unit_mask * unit_hidden, axis=0),
        jnp.sum(grad_normed * unit_mask, axis=0),
    )


def on_device(
    inputs,
    slot_flag,
    cotangent,
    first_gain,
    first_shift,
    query_weight,
    query_bias,
    key_weight,
    value_weight,
    value_bias,
    out_weight,
    out_bias,
    second_gain,
    second_shift,
    gate_weight,
    gate_bias,
    up_weight,
    up_bias,
    inner_gain,
    inner_shift,
    down_weight,
    down_bias,
):
    seq_local, piece_len, width = inputs.shape
    head_ways = lax.axis_size(HEADS)
    group_width = width // head_ways
    group_pairs = group_width // PAIR
    token_count = seq_local * piece_len
    fsdp_ways, tensor_ways = lax.axis_size(FSDP), lax.axis_size(TENSOR)
    row_part = query_weight.shape[0]
    group_index = lax.axis_index(HEADS)
    inputs_group = cube_gather(inputs, HEADS)
    grad_flags = slot_flag.astype(jnp.float32)[:, None, None]
    grad_total = grad_flags * cotangent.astype(jnp.float32)
    grad_branch = grad_total.astype(jnp.bfloat16)
    below, above = [grad_branch], [grad_branch]
    line_step(below, above, TENSOR)
    below[-1], above[-1] = after(below[-1], inputs_group), after(above[-1], inputs_group)
    line_step(below, above, TENSOR)
    stacked = jnp.stack(
        [
            member.reshape(row_part, head_ways, group_pairs, PAIR)
            for member in (query_weight, key_weight, value_weight)
        ],
        axis=3,
    ).reshape(row_part, head_ways, 3 * group_width)
    vectors = (
        first_gain,
        first_shift,
        query_bias,
        value_bias,
        out_bias,
        second_gain,
        second_shift,
        down_bias,
    )
    row_lanes = 3 * group_width
    vector_row = jnp.zeros((row_lanes,), jnp.float32)
    for place, member in enumerate(vectors):
        ahead = place * row_part
        vector_row = vector_row + jnp.pad(
            member.astype(jnp.float32), (ahead, row_lanes - ahead - row_part)
        )
    vector_row = vector_row.astype(jnp.bfloat16)
    sent_columns = jnp.concatenate(
        [
            stacked.transpose(1, 0, 2),
            jnp.broadcast_to(vector_row, (head_ways, 1, 3 * group_width)),
        ],
        axis=1,
    )
    own_columns = lax.all_to_all(
        sent_columns, HEADS, split_axis=0, concat_axis=0, tiled=True
    )
    columns = lax.all_gather(
        own_columns.reshape(-1, 3 * group_width), (FSDP, TENSOR), axis=0, tiled=True
    )
    group_f = inputs_group.reshape(-1, width).astype(jnp.float32)
    group_mean = jnp.mean(group_f, axis=-1, keepdims=True)
    group_var = jnp.mean(jnp.square(group_f - group_mean), axis=-1, keepdims=True)
    group_inv = lax.rsqrt(group_var + norm_eps)
    columns, group_mean, group_inv = lax.optimization_barrier((columns, group_mean, group_inv))
    columns = columns.reshape(
        fsdp_ways, tensor_ways, head_ways, row_part + 1, 3 * group_width
    ).transpose(0, 2, 1, 3, 4)
    qkv_part = columns[:, :, :, :row_part].reshape(width, 3 * group_width)
    below[-1], above[-1] = after(below[-1], columns), after(above[-1], columns)
    line_step(below, above, TENSOR)
    gathered = (
        columns[:, :, :, row_part, : len(vectors) * row_part]
        .reshape(-1, 8, row_part)
        .transpose(1, 0, 2)
        .reshape(8, width)
    )
    out_below, out_above = [out_weight], [out_weight]
    for _ in range(tensor_ways - 1):
        line_step(out_below, out_above, TENSOR)
    out_full = lax.all_gather(
        line_pick(out_below, out_above, TENSOR),
        (FSDP, HEADS),
        axis=0,
        tiled=True,
    )
    gain_one, shift_one, query_shift, value_shift, out_shift, gain_two, shift_two, down_shift = [
        member.astype(jnp.float32) for member in gathered
    ]
    gate_part, up_part, down_part = (
        lax.all_gather(gate_weight, (FSDP, HEADS), axis=0, tiled=True),
        lax.all_gather(up_weight, (FSDP, HEADS), axis=0, tiled=True),
        lax.all_gather(down_weight, (FSDP, HEADS), axis=1, tiled=True),
    )
    inputs_f = inputs.astype(jnp.float32)
    _, unit_one, inv_one = layer_norm(inputs_f, gain_one, shift_one)
    unit_group = (group_f - group_mean) * group_inv
    low_one = (unit_group * gain_one + shift_one).astype(jnp.bfloat16)

    def group_lanes(full_vec):
        own = lax.dynamic_slice_in_dim(full_vec, group_index * group_width, group_width, 0)
        return own.reshape(group_pairs, PAIR)

    query_lanes, value_lanes = group_lanes(query_shift), group_lanes(value_shift)
    qkv_shift = jnp.stack([query_lanes, jnp.zeros_like(query_lanes), value_lanes], axis=1)
    qkv_lin = (
        (jnp.dot(low_one, qkv_part, preferred_element_type=jnp.float32) + qkv_shift.reshape(-1))
        .astype(jnp.bfloat16)
        .reshape(head_ways, seq_local, piece_len, 3 * group_width)
    )
    tables = tuple(jnp.tile(table, (1, PAIR // HD)) for table in rope_tables())
    mixed_heads = attend_forward(qkv_lin, tables)
    mixed_heads, below[-1], above[-1] = lax.optimization_barrier(
        (mixed_heads, below[-1], above[-1])
    )
    for _ in range(tensor_ways - 4):
        line_step(below, above, TENSOR)
    mixed_parts = lax.all_to_all(mixed_heads, HEADS, split_axis=0, concat_axis=0, tiled=True)
    grad_rows = line_pick(below, above, TENSOR).reshape(-1, width)
    mixed_flat = mixed_parts.transpose(1, 2, 0, 3).reshape(token_count, width)
    residual = inputs_f + (
        jnp.dot(mixed_flat, out_full, preferred_element_type=jnp.float32) + out_shift
    ).reshape(inputs.shape)
    normed_two, unit_two, inv_two = layer_norm(residual, gain_two, shift_two)
    low_two = normed_two.astype(jnp.bfloat16)
    flag_rows = slot_flag.astype(jnp.float32)[:, None, None]
    down_shift_grad = jnp.sum(grad_branch.reshape(token_count, width), axis=0, dtype=jnp.float32)
    ffn_local = gate_part.shape[1]
    token_rows3 = gather_rows(after(low_two, gate_part, up_part, below[-1], above[-1]))
    token_rows = token_rows3.reshape(-1, width)
    col_index = lax.axis_index(TENSOR) * ffn_local + jnp.arange(ffn_local, dtype=jnp.int32)
    unit_mask = (col_index < FF_REAL).astype(jnp.float32)
    gate_pre, up_pre, hidden = hidden_forward(
        token_rows,
        gate_part,
        up_part,
        gate_bias.astype(jnp.float32),
        up_bias.astype(jnp.float32),
        unit_mask,
    )
    first_sum, second_sum = tensor_sums(jnp.sum(hidden, axis=-1), jnp.sum(hidden * hidden, axis=-1))
    inner_scale = inner_gain.astype(jnp.float32)
    normed_hidden, unit_hidden, inv_hidden = inner_normalize(
        hidden, first_sum, second_sum, inner_scale, inner_shift.astype(jnp.float32), unit_mask
    )
    hidden_seqs = normed_hidden.reshape(token_rows3.shape[0], piece_len, ffn_local)

    def down_term(row_count):
        picked = hidden_seqs.reshape(-1, ffn_local)
        return jnp.dot(picked, down_part, preferred_element_type=jnp.float32).reshape(
            row_count, piece_len, width
        )

    down_grad = outer_product(normed_hidden, grad_rows)
    down_weight_grad = lax.psum_scatter(
        down_grad.astype(jnp.bfloat16), (FSDP, HEADS), scatter_dimension=1, tiled=True
    )
    grad_normed = times_transpose(after(grad_rows, down_grad), down_part)
    scaled, scaled_sum, cross_sum = hidden_backward_terms(
        grad_normed, unit_hidden, inner_scale, unit_mask
    )
    scaled_sum, cross_sum = tensor_sums(scaled_sum, cross_sum)
    grad_gate, grad_up = gate_grads(
        scaled, scaled_sum, cross_sum, unit_hidden, inv_hidden, gate_pre, up_pre, unit_mask
    )
    gate_grad = outer_product(token_rows, grad_gate)
    up_grad = outer_product(token_rows, grad_up)
    vector_grads = vector_sums(grad_gate, grad_up, grad_normed, unit_hidden, unit_mask)
    gate_seqs = after(grad_gate, down_weight_grad).reshape(-1, piece_len, ffn_local)
    up_seqs = grad_up.reshape(-1, piece_len, ffn_local)

    def input_term(row_start, row_count):
        picked_gate = gate_seqs.reshape(-1, ffn_local)
        picked_up = up_seqs.reshape(-1, ffn_local)
        summed = times_transpose(picked_gate, gate_part) + times_transpose(picked_up, up_part)
        return summed.reshape(row_count, piece_len, width)

    grad_normed_two = scatter_rows(input_term, seq_local)
    gate_weight_grad, up_weight_grad = (
        lax.psum_scatter(
            gate_grad.astype(jnp.bfloat16), (FSDP, HEADS), scatter_dimension=0, tiled=True
        ).astype(jnp.float32),
        lax.psum_scatter(
            up_grad.astype(jnp.bfloat16), (FSDP, HEADS), scatter_dimension=0, tiled=True
        ).astype(jnp.float32),
    )
    down_weight_grad = down_weight_grad.astype(jnp.float32)
    gate_bias_grad, up_bias_grad, inner_gain_grad, inner_shift_grad = lax.psum(
        (vector_grads[0], vector_grads[1], vector_grads[2], vector_grads[3]), (FSDP, HEADS)
    )
    grad_normed_two = after(grad_normed_two, gate_bias_grad)
    grad_residual = grad_total + norm_backward(grad_normed_two, unit_two, inv_two, gain_two)
    gain_two_grad = jnp.sum((grad_normed_two * unit_two).reshape(token_count, width), axis=0)
    shift_two_grad = jnp.sum(grad_normed_two.reshape(token_count, width), axis=0)
    grad_attn = grad_residual.astype(jnp.bfloat16).reshape(token_count, width)
    out_weight_part = outer_product(mixed_flat, grad_attn)
    out_shift_grad = jnp.sum(grad_attn, axis=0, dtype=jnp.float32)
    grad_mixed = times_transpose(grad_attn, out_full).astype(jnp.bfloat16)
    grad_parts = grad_mixed.reshape(seq_local, piece_len, head_ways, group_width)
    grad_heads = lax.all_to_all(
        grad_parts.transpose(2, 0, 1, 3), HEADS, split_axis=0, concat_axis=0, tiled=True
    )
    branch_terms = down_term(seq_local * tensor_ways).astype(jnp.bfloat16)
    branch_terms = branch_terms.reshape((tensor_ways,) + inputs.shape)
    running = line_scatter_step(branch_terms, None, tensor_ways - 1, TENSOR, grad_mixed)
    qkv_grad = attend_backward(qkv_lin, grad_heads, tables)
    qkv_grad = after(qkv_grad, *running)
    running = line_scatter_step(branch_terms, running, tensor_ways - 2, TENSOR, qkv_grad)
    for distance in range(tensor_ways - 3, 0, -1):
        running = line_scatter_step(branch_terms, running, distance, TENSOR, qkv_grad)
    branch_out = (
        line_term(branch_terms, 0, TENSOR)
        + running[0].astype(jnp.float32)
        + running[1].astype(jnp.float32)
    )
    output = (flag_rows * (residual + branch_out + down_shift)).astype(jnp.bfloat16)
    qkv_grad = qkv_grad.reshape(head_ways * token_count, 3 * group_width)
    group_grad = times_transpose(qkv_grad, qkv_part)
    gain_one_grad = jnp.sum(group_grad * unit_group, axis=0)
    shift_one_grad = jnp.sum(group_grad, axis=0)
    group_terms = group_grad.astype(jnp.bfloat16)
    grad_normed_one = cube_scatter(
        group_terms.reshape((head_ways,) + inputs.shape), HEADS
    )
    qkv_shift_grad = jnp.sum(qkv_grad, axis=0, dtype=jnp.float32).reshape(group_pairs, 3, PAIR)

    def place_lanes(own_lanes):
        return lax.dynamic_update_slice_in_dim(
            jnp.zeros((width,), jnp.float32), own_lanes.reshape(-1), group_index * group_width, 0
        )

    query_shift_grad = place_lanes(qkv_shift_grad[:, 0])
    value_shift_grad = place_lanes(qkv_shift_grad[:, 2])
    input_grad = (
        grad_residual + norm_backward(grad_normed_one, unit_one, inv_one, gain_one)
    ).astype(jnp.bfloat16)
    vector_terms = jnp.stack(
        [
            gain_one_grad,
            shift_one_grad,
            query_shift_grad,
            value_shift_grad,
            out_shift_grad,
            gain_two_grad,
            shift_two_grad,
            down_shift_grad,
        ]
    )
    vector_lanes = vector_terms.shape[0] * row_part
    vector_rows = (
        vector_terms.reshape(-1, fsdp_ways, head_ways, tensor_ways, row_part)
        .transpose(1, 3, 2, 0, 4)
        .reshape(fsdp_ways, tensor_ways, head_ways, 1, vector_lanes)
    )
    extra_rows = 1
    while head_ways * (row_part + extra_rows) % 16 != 0:
        extra_rows += 1
    vector_rows = jnp.pad(
        vector_rows,
        ((0, 0),) * 3 + ((0, extra_rows - 1), (0, 3 * group_width - vector_lanes)),
    )
    qkv_terms = outer_product(low_one, qkv_grad).astype(jnp.bfloat16)
    qkv_terms = qkv_terms.reshape(
        fsdp_ways, head_ways, tensor_ways, row_part, 3 * group_width
    ).transpose(0, 2, 1, 3, 4)
    qkv_terms = jnp.concatenate([qkv_terms, vector_rows.astype(jnp.bfloat16)], axis=3)
    qkv_half = cube_scatter(
        qkv_terms.reshape(fsdp_ways, -1, 3 * group_width), FSDP
    ).astype(jnp.bfloat16)
    qkv_rows = lax.psum_scatter(qkv_half, TENSOR, scatter_dimension=0, tiled=True)
    qkv_columns = lax.all_to_all(
        qkv_rows, HEADS, split_axis=0, concat_axis=0, tiled=True
    ).reshape(head_ways, row_part + extra_rows, 3 * group_width)
    qkv_weight_grads = (
        qkv_columns[:, :row_part]
        .reshape(head_ways, row_part, group_pairs, 3, PAIR)
        .transpose(3, 1, 0, 2, 4)
        .reshape(3, row_part, width)
        .astype(jnp.float32)
    )
    own_sums = jnp.sum(
        qkv_columns[:, row_part, :vector_lanes].astype(jnp.float32), axis=0
    ).reshape(-1, row_part)
    out_terms = out_weight_part.astype(jnp.bfloat16).reshape(fsdp_ways, -1, width)
    out_half = cube_scatter(out_terms, FSDP).astype(jnp.bfloat16)
    out_eighth = cube_scatter(out_half.reshape(head_ways, -1, width), HEADS)
    out_weight_grad = lax.psum_scatter(
        out_eighth.astype(jnp.bfloat16), TENSOR, scatter_dimension=0, tiled=True
    ).astype(jnp.float32)
    attn_sums = tuple(qkv_weight_grads) + (out_weight_grad,) + tuple(own_sums)
    return (
        output,
        input_grad,
        attn_sums[4],
        attn_sums[5],
        attn_sums[0],
        attn_sums[6],
        attn_sums[1],
        attn_sums[2],
        attn_sums[7],
        attn_sums[3],
        attn_sums[8],
        attn_sums[9],
        attn_sums[10],
        gate_weight_grad,
        gate_bias_grad,
        up_weight_grad,
        up_bias_grad,
        inner_gain_grad,
        inner_shift_grad,
        down_weight_grad,
        attn_sums[11],
    )


def solution(mesh):
    return jax.shard_map(
        on_device,
        mesh=mesh,
        in_specs=(
            P((FSDP, TENSOR), HEADS, None),
            P((FSDP, TENSOR)),
            P((FSDP, TENSOR), HEADS, None),
            P((FSDP, HEADS, TENSOR)),
            P((FSDP, HEADS, TENSOR)),
            P((FSDP, HEADS, TENSOR), None),
            P((FSDP, HEADS, TENSOR)),
            P((FSDP, HEADS, TENSOR), None),
            P((FSDP, HEADS, TENSOR), None),
            P((FSDP, HEADS, TENSOR)),
            P((FSDP, HEADS, TENSOR), None),
            P((FSDP, HEADS, TENSOR)),
            P((FSDP, HEADS, TENSOR)),
            P((FSDP, HEADS, TENSOR)),
            P((FSDP, HEADS), TENSOR),
            P(TENSOR),
            P((FSDP, HEADS), TENSOR),
            P(TENSOR),
            P(TENSOR),
            P(TENSOR),
            P(TENSOR, (FSDP, HEADS)),
            P((FSDP, HEADS, TENSOR)),
        ),
        out_specs=(
            P((FSDP, TENSOR), HEADS, None),
            P((FSDP, TENSOR), HEADS, None),
            P((FSDP, HEADS, TENSOR)),
            P((FSDP, HEADS, TENSOR)),
            P((FSDP, HEADS, TENSOR), None),
            P((FSDP, HEADS, TENSOR)),
            P((FSDP, HEADS, TENSOR), None),
            P((FSDP, HEADS, TENSOR), None),
            P((FSDP, HEADS, TENSOR)),
            P((FSDP, HEADS, TENSOR), None),
            P((FSDP, HEADS, TENSOR)),
            P((FSDP, HEADS, TENSOR)),
            P((FSDP, HEADS, TENSOR)),
            P((FSDP, HEADS), TENSOR),
            P(TENSOR),
            P((FSDP, HEADS), TENSOR),
            P(TENSOR),
            P(TENSOR),
            P(TENSOR),
            P(TENSOR, (FSDP, HEADS)),
            P((FSDP, HEADS, TENSOR)),
        ),
        check_vma=False,
    )
```
